32 devices in a mesh: dp: 8 (over z, x), fsdp: 4 (over y, core).
Axes of the slice: x: 2, y: 2, z: 4, core: 2. Of those that a mesh axis runs over, the one named last changes fastest.
Arguments:
- tokens: bfloat16 [8192, 768], P(('dp', 'fsdp')), may hold values from -18 to 18, as said below
- cotangent: bfloat16 [8192, 768], P(('dp', 'fsdp')), may hold values from -6 to 6
- segment_ids: int32 [8192], P('dp'), may hold values from 0 to 239, as said below
- valid_mask: int32 [8192], P(('dp', 'fsdp')), may hold values from 0 to 1, as said below
- ln1_gain: bfloat16 [768], P('fsdp'), may hold values from 0.5 to 1.5
- ln1_bias: bfloat16 [768], P('fsdp'), may hold values from -1.1953125 to 1.1953125
- qkv_weight: bfloat16 [768, 2304], P('fsdp'), may hold values from -0.21875 to 0.21875
- qkv_bias: bfloat16 [2304], P('fsdp'), may hold values from -1.1953125 to 1.1953125
- query_gain: bfloat16 [64], P('fsdp'), may hold values from 0.5 to 1.5
- query_bias: bfloat16 [64], P('fsdp'), may hold values from -1.796875 to 1.796875
- key_gain: bfloat16 [64], P('fsdp'), may hold values from 0.5 to 1.5
- proj_weight: bfloat16 [768, 768], P('fsdp'), may hold values from -0.875 to 0.875
- proj_bias: bfloat16 [768], P('fsdp'), may hold values from -1.1953125 to 1.1953125
- ln2_gain: bfloat16 [768], P('fsdp'), may hold values from 0.5 to 1.5
- ln2_bias: bfloat16 [768], P('fsdp'), may hold values from -1.1953125 to 1.1953125
- fc1_weight: bfloat16 [768, 3072], P('fsdp'), may hold values from -0.21875 to 0.21875
- fc1_bias: bfloat16 [3072], P('fsdp'), may hold values from -1.1953125 to 1.1953125
- fc2_weight: bfloat16 [3072, 768], P('fsdp'), may hold values from -0.109375 to 0.109375
- fc2_bias: bfloat16 [768], P('fsdp'), may hold values from -1.1953125 to 1.1953125
Outputs:
- block_out: bfloat16 [8192, 768], P(('dp', 'fsdp'))
- tokens_grad: float32 [8192, 768], P(('dp', 'fsdp'))
- ln1_gain_grad: float32 [768], P('fsdp')
- ln1_bias_grad: float32 [768], P('fsdp')
- qkv_weight_grad: float32 [768, 2304], P('fsdp')
- qkv_bias_grad: float32 [2304], P('fsdp')
- query_gain_grad: float32 [64], P('fsdp')
- query_bias_grad: float32 [64], P('fsdp')
- key_gain_grad: float32 [64], P('fsdp')
- proj_weight_grad: float32 [768, 768], P('fsdp')
- proj_bias_grad: float32 [768], P('fsdp')
- ln2_gain_grad: float32 [768], P('fsdp')
- ln2_bias_grad: float32 [768], P('fsdp')
- fc1_weight_grad: float32 [768, 3072], P('fsdp')
- fc1_bias_grad: float32 [3072], P('fsdp')
- fc2_weight_grad: float32 [3072, 768], P('fsdp')
- fc2_bias_grad: float32 [768], P('fsdp')
- rms_values: float32 [3], replicated
The draws below stay inside these ranges and needn't reach their ends.
Inputs may be any that keep to these rules, and one draw needn't show every extreme that they name: `segment_ids`: in each aligned block of 1024 slots (block b) either one image of 576 patches with id 32 b, then padding with id 32 b + 1, or 16 images of 64 patches with ids 32 b + 0, 1, ...; block 0 holds a large image, block 1 and the last block small ones. `valid_mask`: 1 exactly on the slots of images, 0 on padding. `tokens`: row scales differ along the slots.
All inputs are finite; a program needn't handle non-finite values.
Results may differ from the reference program's by a relative error of at most 0.015.
Values may be sent and summed in bfloat16 or wider, within the bound.
A program may use at most 192 MiB of HBM per device.

```python
import jax
import jax.numpy as jnp
from jax import lax

D = 768
HEADS = 12
HEAD_DIM = 64
FF = 3072
SEQ = 1024
IMG = 64
BIG = 576
TOKENS = 8192
BLOCK_ROWS = 4096


def layout(key):
    slot_total = TOKENS // SEQ
    kinds = jax.random.randint(jax.random.fold_in(key, 7), (slot_total,), 0, 2)
    kinds = kinds.at[0].set(1).at[1].set(0).at[slot_total - 1].set(0)
    place = jnp.arange(SEQ, dtype=jnp.int32)
    long_local = jnp.where(place < BIG, 0, 1)
    short_local = place // IMG
    local = jnp.where(kinds[:, None] == 1, long_local[None, :], short_local[None, :])
    segment = jnp.arange(slot_total, dtype=jnp.int32)[:, None] * 32 + local
    padding = (kinds[:, None] == 1) & (place[None, :] >= BIG)
    valid = jnp.where(padding, 0, 1)
    return (segment.reshape(-1).astype(jnp.int32), valid.reshape(-1).astype(jnp.int32))


def draw_segment_ids(key, part):
    return layout(key)[0]


def draw_valid_mask(key, part):
    return layout(key)[1]


def draw_tokens(key, part):
    position = jnp.arange(TOKENS, dtype=jnp.float32) / (TOKENS - 1)
    scale = 1.0 + 2.0 * position
    values = jnp.clip(jax.random.normal(key, (TOKENS, D), jnp.float32), -6.0, 6.0)
    return (values * scale[:, None]).astype(jnp.bfloat16)


def block_levels(stream_key, extent, cuts, low, high):
    def one(axis_at, parts):
        draws = jax.random.uniform(jax.random.fold_in(jax.random.fold_in(stream_key, 6), axis_at), (parts,), jnp.float32, low / len(cuts), high / len(cuts))
        return jnp.repeat(jnp.exp(draws), extent[axis_at] // parts).reshape((-1,) + (1,) * (len(extent) - axis_at - 1))

    loudness = one(*cuts[0])
    for cut in cuts[1:]:
        loudness = loudness * one(*cut)
    return loudness


def noise(rng, shape, deviation, most, cuts=(), kind=jnp.bfloat16):
    array = jax.random.normal(rng, shape, jnp.float32) * deviation
    if len(cuts) > 0:
        array = block_levels(rng, shape, cuts, -0.22, 0.18) * array
    return jnp.clip(array, min=-most, max=most).astype(kind)


def setup_inputs(seed: int = 0) -> dict:
    key_of = jax.random.split(jax.random.key(seed), 20)
    return {
        "tokens": draw_tokens(jax.random.fold_in(key_of[19], 71), 0),
        "cotangent": noise(key_of[1], (TOKENS, D), 1.0, 6.0, ((0, 32),)),
        "segment_ids": draw_segment_ids(jax.random.fold_in(key_of[19], 71), 0),
        "valid_mask": draw_valid_mask(jax.random.fold_in(key_of[19], 71), 0),
        "ln1_gain": jnp.clip(1.0 + 0.1 * jax.random.normal(key_of[4], (D,), jnp.float32), 0.5, 1.5).astype(jnp.bfloat16),
        "ln1_bias": noise(key_of[5], (D,), 0.2, 1.1953125, ((0, 4),)),
        "qkv_weight": noise(key_of[6], (D, 3 * D), D ** -0.5, 0.21875, ((0, 4),)),
        "qkv_bias": noise(key_of[7], (3 * D,), 0.2, 1.1953125, ((0, 4),)),
        "query_gain": jnp.clip(1.0 + 0.1 * jax.random.normal(key_of[8], (HEAD_DIM,), jnp.float32), 0.5, 1.5).astype(jnp.bfloat16),
        "query_bias": noise(key_of[9], (HEAD_DIM,), 0.3, 1.796875, ((0, 4),)),
        "key_gain": jnp.clip(1.0 + 0.1 * jax.random.normal(key_of[10], (HEAD_DIM,), jnp.float32), 0.5, 1.5).astype(jnp.bfloat16),
        "proj_weight": noise(key_of[11], (D, D), (D // 16) ** -0.5, 0.875, ((0, 4),)),
        "proj_bias": noise(key_of[12], (D,), 0.2, 1.1953125, ((0, 4),)),
        "ln2_gain": jnp.clip(1.0 + 0.1 * jax.random.normal(key_of[13], (D,), jnp.float32), 0.5, 1.5).astype(jnp.bfloat16),
        "ln2_bias": noise(key_of[14], (D,), 0.2, 1.1953125, ((0, 4),)),
        "fc1_weight": noise(key_of[15], (D, FF), D ** -0.5, 0.21875, ((0, 4),)),
        "fc1_bias": noise(key_of[16], (FF,), 0.2, 1.1953125, ((0, 4),)),
        "fc2_weight": noise(key_of[17], (FF, D), FF ** -0.5, 0.109375, ((0, 4),)),
        "fc2_bias": noise(key_of[18], (D,), 0.2, 1.1953125, ((0, 4),)),
    }


EPS = 1e-06
MASKED = -1e+30

@jax.custom_vjp
def low(v):
    return lax.optimization_barrier(v.astype(jnp.bfloat16)).astype(jnp.float32)

@jax.custom_vjp
def low_back(v):
    return v

def low_keep(v):
    return (low(v), None)

def low_pass(kept, grad):
    return (grad,)

def back_keep(v):
    return (v, None)

def back_low(kept, grad):
    return (low(grad),)
low.defvjp(low_keep, low_pass)
low_back.defvjp(back_keep, back_low)

def exact_dot(first, second):
    return jnp.dot(first, second, precision=lax.Precision.HIGHEST, preferred_element_type=jnp.float32)

def layer_norm(values, gain, shift):
    average = lax.optimization_barrier(jnp.mean(values, axis=-1, keepdims=True))
    centred = values - average
    spread = lax.optimization_barrier(jnp.mean(centred * centred, axis=-1, keepdims=True))
    return centred * lax.rsqrt(spread + EPS) * gain + shift

def gelu_tanh(values):
    return jax.nn.gelu(values, approximate=True)

def block(params, inputs, seg_rows, valid_rows):
    gain_one, shift_one, w_qkv, b_qkv, gain_query, shift_query, gain_key, w_proj, b_proj, gain_two, shift_two, w_up, b_up, w_down, b_down = params
    row_count = inputs.shape[0]
    slot_count = row_count // SEQ
    normed = low(layer_norm(inputs, gain_one, shift_one))
    projected = low_back(exact_dot(normed, w_qkv) + b_qkv)
    raw_query = projected[:, :D].reshape(row_count, HEADS, HEAD_DIM)
    raw_key = projected[:, D:2 * D].reshape(row_count, HEADS, HEAD_DIM)
    values = low(projected[:, 2 * D:].reshape(row_count, HEADS, HEAD_DIM))
    queries = low(layer_norm(raw_query, gain_query, shift_query) * HEAD_DIM ** (-0.5))
    keys = low(layer_norm(raw_key, gain_key, 0.0))
    q_slots = queries.reshape(slot_count, SEQ, HEADS, HEAD_DIM)
    k_slots = keys.reshape(slot_count, SEQ, HEADS, HEAD_DIM)
    v_slots = values.reshape(slot_count, SEQ, HEADS, HEAD_DIM)
    scores = low_back(jnp.einsum('sqhd,skhd->shqk', q_slots, k_slots, precision=lax.Precision.HIGHEST))
    ids = seg_rows.reshape(slot_count, SEQ)
    allowed = ids[:, :, None] == ids[:, None, :]
    scores = jnp.where(allowed[:, None], scores, MASKED)
    probs = jax.nn.softmax(scores, axis=-1)
    mixed = jnp.einsum('shqk,skhd->sqhd', low(probs), v_slots, precision=lax.Precision.HIGHEST)
    mixed = low(low_back(mixed.reshape(row_count, D)))
    branch_attn = low_back(exact_dot(mixed, w_proj) + b_proj)
    hidden_one = inputs + branch_attn
    normed_two = low(layer_norm(hidden_one, gain_two, shift_two))
    inner = low_back(exact_dot(normed_two, w_up) + b_up)
    activated = low(gelu_tanh(inner))
    branch_mlp = low_back(exact_dot(activated, w_down) + b_down)
    result = hidden_one + branch_mlp
    weights_valid = valid_rows.astype(jnp.float32)[:, None]
    sums = jnp.stack([jnp.sum(weights_valid * result * result), jnp.sum(weights_valid * branch_attn * branch_attn), jnp.sum(weights_valid * branch_mlp * branch_mlp)])
    return (result, sums)

def forward(inputs, params, segment_ids, valid_mask):
    block_count = TOKENS // BLOCK_ROWS
    stacked = (inputs.reshape(block_count, BLOCK_ROWS, D), segment_ids.reshape(block_count, BLOCK_ROWS), valid_mask.reshape(block_count, BLOCK_ROWS))
    checked = jax.checkpoint(block)

    def step(carry, pieces):
        result, sums = checked(params, pieces[0], pieces[1], pieces[2])
        return (carry + sums, result)
    totals, results = lax.scan(step, jnp.zeros((3,), jnp.float32), stacked)
    return (results.reshape(TOKENS, D), totals)

def reference(tokens, cotangent, segment_ids, valid_mask, ln1_gain, ln1_bias, qkv_weight, qkv_bias, query_gain, query_bias, key_gain, proj_weight, proj_bias, ln2_gain, ln2_bias, fc1_weight, fc1_bias, fc2_weight, fc2_bias):
    params = tuple((p.astype(jnp.float32) for p in (ln1_gain, ln1_bias, qkv_weight, qkv_bias, query_gain, query_bias, key_gain, proj_weight, proj_bias, ln2_gain, ln2_bias, fc1_weight, fc1_bias, fc2_weight, fc2_bias)))
    inputs = tokens.astype(jnp.float32)

    def primal(inputs_now, params_now):
        return forward(inputs_now, params_now, segment_ids, valid_mask)
    result, pullback, totals = jax.vjp(primal, inputs, params, has_aux=True)
    grad_out = cotangent.astype(jnp.float32) * valid_mask.astype(jnp.float32)[:, None]
    inputs_grad, params_grad = pullback(grad_out)
    count = jnp.sum(valid_mask.astype(jnp.float32))
    rms_values = jnp.sqrt(totals / count)
    return (result.astype(jnp.bfloat16), inputs_grad, params_grad[0], params_grad[1], params_grad[2], params_grad[3], params_grad[4], params_grad[5], params_grad[6], params_grad[7], params_grad[8], params_grad[9], params_grad[10], params_grad[11], params_grad[12], params_grad[13], params_grad[14], rms_values)
```

```python
import functools

import jax
import jax.numpy as jnp
from jax import lax
from jax.experimental import pallas as pl
from jax.experimental.pallas import tpu as pltpu
from jax.sharding import PartitionSpec as P

HEADS = 12
HEAD_DIM = 64
EPS = 1e-06
MASKED = -1e30
F32 = jnp.float32
BF16 = jnp.bfloat16


def swap(value, axis, size, bit):
    return lax.ppermute(value, axis, [(i, i ^ bit) for i in range(size)])


def dot(first, second):
    return jnp.dot(first, second, preferred_element_type=F32)


def left_cross(first, second):
    return lax.dot_general(first, second, (((0,), (0,)), ((), ())), preferred_element_type=F32)


def right_cross(first, second):
    return lax.dot_general(first, second, (((1,), (1,)), ((), ())), preferred_element_type=F32)


def norm_parts(values):
    average = jnp.mean(values, axis=-1, keepdims=True)
    centred = values - average
    spread = jnp.mean(centred * centred, axis=-1, keepdims=True)
    scale = lax.rsqrt(spread + EPS)
    return centred * scale, scale


def norm_back(grad, unit, scale):
    return scale * (
        grad
        - jnp.mean(grad, axis=-1, keepdims=True)
        - unit * jnp.mean(grad * unit, axis=-1, keepdims=True)
    )


def attend_body(q_ref, k_ref, v_ref, rows_ref, cols_ref, o_ref, p_ref):
    scores = right_cross(q_ref[0], k_ref[0])
    scores = jnp.where(rows_ref[...] == cols_ref[...], scores, MASKED)
    top = jnp.max(scores, axis=-1, keepdims=True)
    raised = jnp.exp(scores - top)
    total = jnp.sum(raised, axis=-1, keepdims=True)
    probs = (raised * (1.0 / total)).astype(BF16)
    p_ref[0] = probs
    o_ref[0] = dot(probs, v_ref[0]).astype(BF16)


def attend(queries, keys, values, ids):
    heads, rows, width = queries.shape
    block = min(256, rows)
    return pl.pallas_call(
        attend_body,
        grid=(heads, rows // block),
        in_specs=[
            pl.BlockSpec((1, block, width), lambda h, i: (h, i, 0)),
            pl.BlockSpec((1, rows, width), lambda h, i: (h, 0, 0)),
            pl.BlockSpec((1, rows, width), lambda h, i: (h, 0, 0)),
            pl.BlockSpec((block, 1), lambda h, i: (i, 0)),
            pl.BlockSpec((1, rows), lambda h, i: (0, 0)),
        ],
        out_specs=[
            pl.BlockSpec((1, block, width), lambda h, i: (h, i, 0)),
            pl.BlockSpec((1, block, rows), lambda h, i: (h, i, 0)),
        ],
        out_shape=[
            jax.ShapeDtypeStruct((heads, rows, width), BF16),
            jax.ShapeDtypeStruct((heads, rows, rows), BF16),
        ],
        cost_estimate=pl.CostEstimate(
            flops=4 * heads * rows * rows * width,
            bytes_accessed=2 * heads * rows * (rows + 4 * width),
            transcendentals=heads * rows * rows,
        ),
        name="attend",
    )(queries, keys, values, ids[:, None], ids[None, :])


def attend_back_body(q_ref, k_ref, v_ref, p_ref, g_ref, dq_ref, dk_ref, dv_ref):
    @pl.when(pl.program_id(1) == 0)
    def _():
        dk_ref[...] = jnp.zeros_like(dk_ref)
        dv_ref[...] = jnp.zeros_like(dv_ref)

    grad = g_ref[0]
    low = p_ref[0]
    probs = low.astype(F32)
    grad_probs = right_cross(grad, v_ref[0])
    delta = jnp.sum(probs * grad_probs, axis=-1, keepdims=True)
    grad_scores = (probs * (grad_probs - delta)).astype(BF16)
    dq_ref[0] = dot(grad_scores, k_ref[0])
    dk_ref[0] += left_cross(grad_scores, q_ref[0])
    dv_ref[0] += left_cross(low, grad)


def attend_back(queries, keys, values, probs, grads):
    heads, rows, width = queries.shape
    block = min(256, rows)
    part = pl.BlockSpec((1, block, width), lambda h, i: (h, i, 0))
    whole = pl.BlockSpec((1, rows, width), lambda h, i: (h, 0, 0))
    return pl.pallas_call(
        attend_back_body,
        grid=(heads, rows // block),
        in_specs=[part, whole, whole, pl.BlockSpec((1, block, rows), lambda h, i: (h, i, 0)), part],
        out_specs=[part, whole, whole],
        out_shape=[jax.ShapeDtypeStruct((heads, rows, width), F32)] * 3,
        cost_estimate=pl.CostEstimate(
            flops=8 * heads * rows * rows * width,
            bytes_accessed=2 * heads * rows * (rows + 10 * width),
            transcendentals=0,
        ),
        name="attend_back",
    )(queries, keys, values, probs, grads)


def on_device(
    dp_size,
    fs_size,
    tokens,
    cotangent,
    segment_ids,
    valid_mask,
    ln1_gain,
    ln1_bias,
    qkv_weight,
    qkv_bias,
    query_gain,
    query_bias,
    key_gain,
    proj_weight,
    proj_bias,
    ln2_gain,
    ln2_bias,
    fc1_weight,
    fc1_bias,
    fc2_weight,
    fc2_bias,
):
    count, width = tokens.shape
    rank = lax.axis_index("fsdp")
    place = lax.axis_index("dp")
    near = functools.partial(swap, axis="fsdp", size=fs_size, bit=1)
    far = functools.partial(swap, axis="fsdp", size=fs_size, bit=2)
    own_heads = HEADS // fs_size
    part = own_heads * HEAD_DIM
    hidden = fc1_weight.shape[1]
    hidden_own = hidden // fs_size
    rows_own = qkv_weight.shape[0]
    rounds = [1 << i for i in range(dp_size.bit_length() - 1)]

    def gather(value):
        second = far(value)
        return [value, near(value), second, near(second)]

    def spread(pieces):
        return [pieces[0], near(pieces[1]), far(pieces[2]), swap(pieces[3], "fsdp", fs_size, 3)]

    def collect(total):
        low = [total[r * count : (r + 1) * count] for r in range(4)]
        other = near(jnp.concatenate([low[1], low[3]], axis=0).astype(BF16)).astype(F32)
        first = low[0] + other[:count]
        second = far((low[2] + other[count:]).astype(BF16))
        return first + second.astype(F32)

    def at(r):
        return rank ^ r

    small = jnp.concatenate(
        [
            ln1_gain, ln1_bias, ln2_gain, ln2_bias, proj_bias, fc2_bias,
            query_gain, query_bias, key_gain, qkv_bias,
        ]
    )
    small = jnp.pad(small, (0, -small.shape[0] % 128))
    small_all = jnp.zeros((fs_size, small.shape[0]), BF16)
    for r, piece in enumerate(gather(small)):
        small_all = lax.dynamic_update_slice(small_all, piece[None], (at(r), 0))
    small_all = small_all.astype(F32)
    sizes = [v.shape[0] for v in (ln1_gain, ln1_bias, ln2_gain, ln2_bias, proj_bias, fc2_bias)]
    sizes += [v.shape[0] for v in (query_gain, query_bias, key_gain, qkv_bias)]
    vectors = []
    start = 0
    for size in sizes:
        vectors.append(small_all[:, start : start + size].reshape(-1))
        start += size
    gain_one, shift_one, gain_two, shift_two, b_proj, b_down = vectors[:6]
    gain_query, shift_query, gain_key, b_qkv_all = vectors[6:]

    def own_columns(matrix, owner):
        return [
            lax.dynamic_slice_in_dim(matrix, block * width + owner * part, part, matrix.ndim - 1)
            for block in range(3)
        ]

    tokens_all = jnp.concatenate(gather(tokens), axis=0)
    w_qkv = jnp.zeros((width, 3 * part), BF16)
    for r, piece in enumerate(
        spread([jnp.concatenate(own_columns(qkv_weight, at(r)), axis=1) for r in range(4)])
    ):
        w_qkv = lax.dynamic_update_slice(w_qkv, piece, (at(r) * rows_own, 0))
    w_proj_rel = jnp.concatenate(gather(proj_weight), axis=0)
    w_up = jnp.zeros((width, hidden_own), BF16)
    for r, piece in enumerate(
        spread(
            [lax.dynamic_slice_in_dim(fc1_weight, at(r) * hidden_own, hidden_own, 1) for r in range(4)]
        )
    ):
        w_up = lax.dynamic_update_slice(w_up, piece, (at(r) * rows_own, 0))
    weights_valid = valid_mask.astype(F32)[:, None]
    grad_mlp_own = (cotangent.astype(F32) * weights_valid).astype(BF16)
    grad_mlp_low = jnp.concatenate(gather(grad_mlp_own), axis=0)
    ids = jnp.concatenate(
        [lax.dynamic_slice_in_dim(segment_ids, at(r) * count, count) for r in range(4)]
    )
    rows_all = 4 * count

    inputs = tokens_all.astype(F32)
    unit_one, scale_one = norm_parts(inputs)
    normed_low = (unit_one * gain_one + shift_one).astype(BF16)
    b_qkv = jnp.concatenate(own_columns(b_qkv_all, rank))
    projected = (dot(normed_low, w_qkv) + b_qkv).reshape(rows_all, 3 * own_heads, HEAD_DIM)
    projected = projected.transpose(1, 0, 2)
    unit_query, scale_query = norm_parts(projected[:own_heads])
    unit_key, scale_key = norm_parts(projected[own_heads : 2 * own_heads])
    queries = ((unit_query * gain_query + shift_query) * HEAD_DIM**-0.5).astype(BF16)
    keys = (unit_key * gain_key).astype(BF16)
    values = projected[2 * own_heads :].astype(BF16)
    mixed_heads, probs = attend(queries, keys, values, ids)
    mixed_own = mixed_heads.transpose(1, 0, 2).reshape(rows_all, part)
    columns = []
    for r, piece in enumerate(gather(mixed_own)):
        columns.append(
            jnp.concatenate([piece[(r ^ i) * count : ((r ^ i) + 1) * count] for i in range(4)], axis=0)
        )
    mixed_all = jnp.concatenate(columns, axis=1)
    branch_attn = dot(mixed_all, w_proj_rel) + b_proj
    hidden_one = inputs + branch_attn
    unit_two, scale_two = norm_parts(hidden_one)
    normed_two_low = (unit_two * gain_two + shift_two).astype(BF16)
    inner = dot(normed_two_low, w_up) + fc1_bias.astype(F32)
    activated, back_gelu = jax.vjp(lambda v: jax.nn.gelu(v, approximate=True), inner)
    activated_low = activated.astype(BF16)
    grad_activated = right_cross(grad_mlp_low, fc2_weight)
    grad_inner_low = back_gelu(grad_activated)[0].astype(BF16)

    def halve(total):
        for bit in rounds:
            size = total.shape[1] // 2
            low, high = total[:, :size], total[:, size:]
            upper = (place & bit) != 0
            sent = jnp.where(upper, low, high).astype(BF16)
            total = jnp.where(upper, high, low).astype(F32) + swap(sent, "dp", dp_size, bit).astype(F32)
        return total

    def unite(share):
        share = share.astype(BF16)
        for bit in reversed(rounds):
            other = swap(share, "dp", dp_size, bit)
            upper = (place & bit) != 0
            share = jnp.where(
                upper,
                jnp.concatenate([other, share], axis=0),
                jnp.concatenate([share, other], axis=0),
            )
        return share.astype(F32)

    grad_down = unite(halve(left_cross(activated_low, grad_mlp_low)[None])[0])
    grad_normed_two_part = right_cross(grad_inner_low, w_up)
    grad_normed_two = collect(grad_normed_two_part)
    share_up = halve(left_cross(normed_two_low, grad_inner_low).reshape(4, rows_own, hidden_own))

    def to_rows(share):
        share = share.astype(BF16)
        return spread([lax.dynamic_index_in_dim(share, at(r), 0, False) for r in range(4)])

    pieces_up = to_rows(share_up)
    rows_up = jnp.zeros((pieces_up[0].shape[0], hidden), BF16)
    for r, piece in enumerate(pieces_up):
        rows_up = lax.dynamic_update_slice(rows_up, piece, (0, at(r) * hidden_own))
    grad_up = unite(rows_up)

    grad_out = grad_mlp_own.astype(F32)
    grad_hidden = grad_out + norm_back(grad_normed_two * gain_two, unit_two[:count], scale_two[:count])
    grad_branch_own = grad_hidden.astype(BF16)
    grad_branch_low = jnp.concatenate(gather(grad_branch_own), axis=0)
    grad_mixed = right_cross(grad_branch_low, proj_weight).astype(BF16)
    grad_mixed = grad_mixed.reshape(rows_all, own_heads, HEAD_DIM).transpose(1, 0, 2)
    grad_proj = unite(halve(left_cross(mixed_own, grad_branch_low)[None])[0])
    grad_queries, grad_keys, grad_values = attend_back(queries, keys, values, probs, grad_mixed)
    grad_queries = grad_queries * HEAD_DIM**-0.5
    grad_gain_query = jnp.sum(grad_queries * unit_query, axis=(0, 1))
    grad_shift_query = jnp.sum(grad_queries, axis=(0, 1))
    grad_gain_key = jnp.sum(grad_keys * unit_key, axis=(0, 1))
    grad_projected = jnp.concatenate(
        [
            norm_back(grad_queries * gain_query, unit_query, scale_query).astype(BF16),
            norm_back(grad_keys * gain_key, unit_key, scale_key).astype(BF16),
            grad_values.astype(BF16),
        ],
        axis=0,
    )
    grad_projected = grad_projected.transpose(1, 0, 2).reshape(rows_all, 3 * part)
    share_qkv = halve(left_cross(normed_low, grad_projected).reshape(4, rows_own, 3 * part))
    pieces_qkv = to_rows(share_qkv)
    rows_qkv = jnp.zeros((pieces_qkv[0].shape[0], 3 * width), BF16)
    for r, piece in enumerate(pieces_qkv):
        for block in range(3):
            rows_qkv = lax.dynamic_update_slice(
                rows_qkv,
                piece[:, block * part : (block + 1) * part],
                (0, block * width + at(r) * part),
            )
    grad_qkv = unite(rows_qkv)
    grad_normed_one_part = right_cross(grad_projected, w_qkv)
    grad_normed_one = collect(grad_normed_one_part)
    tokens_grad = grad_hidden + norm_back(
        grad_normed_one * gain_one, unit_one[:count], scale_one[:count]
    )

    branch_mlp = collect(dot(activated_low, fc2_weight)) + b_down
    result = hidden_one[:count] + branch_mlp
    branch_own = branch_attn[:count]
    rms_sums = jnp.stack(
        [
            jnp.sum(weights_valid * result * result),
            jnp.sum(weights_valid * branch_own * branch_own),
            jnp.sum(weights_valid * branch_mlp * branch_mlp),
            jnp.sum(weights_valid),
        ]
    )

    bias_qkv = jnp.sum(grad_projected.astype(F32), axis=0)
    bias_qkv_all = jnp.zeros((3 * width,), F32)
    for block in range(3):
        bias_qkv_all = lax.dynamic_update_slice(
            bias_qkv_all, bias_qkv[block * part : (block + 1) * part], (block * width + rank * part,)
        )
    bias_up_all = lax.dynamic_update_slice(
        jnp.zeros((hidden,), F32),
        jnp.sum(grad_inner_low.astype(F32), axis=0),
        (rank * hidden_own,),
    )
    packed = [
        jnp.sum(grad_normed_one_part * unit_one, axis=0),
        jnp.sum(grad_normed_one_part, axis=0),
        bias_qkv_all,
        grad_gain_query,
        grad_shift_query,
        grad_gain_key,
        jnp.sum(grad_branch_own.astype(F32), axis=0),
        jnp.sum(grad_normed_two_part * unit_two, axis=0),
        jnp.sum(grad_normed_two_part, axis=0),
        bias_up_all,
        jnp.sum(grad_out, axis=0),
        rms_sums,
    ]
    lengths = [v.shape[0] for v in packed]
    vector = jnp.concatenate(packed)
    vector = jnp.pad(vector, (0, -vector.shape[0] % 1024)).reshape(-1, 128)
    for bit in (1, 2):
        vector = vector + swap(vector, "fsdp", fs_size, bit)
    for bit in rounds:
        vector = vector + swap(vector, "dp", dp_size, bit)
    vector = vector.reshape(-1)
    finals = []
    start = 0
    for length in lengths:
        whole = vector[start : start + length]
        start += length
        size = length // fs_size
        finals.append(whole if length == 4 else lax.dynamic_slice_in_dim(whole, rank * size, size))
    sums = finals.pop()
    return (
        result.astype(BF16),
        tokens_grad,
        finals[0],
        finals[1],
        grad_qkv,
        finals[2],
        finals[3],
        finals[4],
        finals[5],
        grad_proj,
        finals[6],
        finals[7],
        finals[8],
        grad_up,
        finals[9],
        grad_down,
        finals[10],
        jnp.sqrt(sums[:3] / sums[3]),
    )


def solution(mesh):
    rows = P(("dp", "fsdp"), None)
    vector = P("fsdp")
    matrix = P("fsdp", None)
    return jax.shard_map(
        functools.partial(on_device, mesh.shape["dp"], mesh.shape["fsdp"]),
        mesh=mesh,
        in_specs=(
            rows, rows, P("dp"), P(("dp", "fsdp")), vector, vector, matrix, vector, vector, vector,
            vector, matrix, vector, vector, vector, matrix, vector, matrix, vector,
        ),
        out_specs=(
            rows, rows, vector, vector, matrix, vector, vector, vector, vector, matrix, vector,
            vector, vector, matrix, vector, matrix, vector, P(),
        ),
        check_vma=False,
    )
```

```python
import functools

import jax
import jax.numpy as jnp
from jax import lax
from jax.experimental import pallas as pl
from jax.experimental.pallas import tpu as pltpu
from jax.sharding import PartitionSpec as P

HEADS = 12
HEAD_DIM = 64
EPS = 1e-06
MASKED = -1e30
F32 = jnp.float32
BF16 = jnp.bfloat16


def swap(value, axis, size, bit):
    return lax.ppermute(value, axis, [(i, i ^ bit) for i in range(size)])


def dot(first, second):
    return jnp.dot(first, second, preferred_element_type=F32)


def left_cross(first, second):
    return lax.dot_general(first, second, (((0,), (0,)), ((), ())), preferred_element_type=F32)


def right_cross(first, second):
    return lax.dot_general(first, second, (((1,), (1,)), ((), ())), preferred_element_type=F32)


def norm_parts(values):
    average = jnp.mean(values, axis=-1, keepdims=True)
    centred = values - average
    spread = jnp.mean(centred * centred, axis=-1, keepdims=True)
    scale = lax.rsqrt(spread + EPS)
    return centred * scale, scale


def norm_back(grad, unit, scale):
    return scale * (
        grad
        - jnp.mean(grad, axis=-1, keepdims=True)
        - unit * jnp.mean(grad * unit, axis=-1, keepdims=True)
    )


def attend_body(q_ref, k_ref, v_ref, rows_ref, cols_ref, o_ref, p_ref):
    scores = right_cross(q_ref[0], k_ref[0])
    scores = jnp.where(rows_ref[...] == cols_ref[...], scores, MASKED)
    top = jnp.max(scores, axis=-1, keepdims=True)
    raised = jnp.exp(scores - top)
    total = jnp.sum(raised, axis=-1, keepdims=True)
    probs = (raised * (1.0 / total)).astype(BF16)
    p_ref[0] = probs
    o_ref[0] = dot(probs, v_ref[0]).astype(BF16)


def attend(queries, keys, values, ids):
    heads, rows, width = queries.shape
    block = min(256, rows)
    return pl.pallas_call(
        attend_body,
        grid=(heads, rows // block),
        in_specs=[
            pl.BlockSpec((1, block, width), lambda h, i: (h, i, 0)),
            pl.BlockSpec((1, rows, width), lambda h, i: (h, 0, 0)),
            pl.BlockSpec((1, rows, width), lambda h, i: (h, 0, 0)),
            pl.BlockSpec((block, 1), lambda h, i: (i, 0)),
            pl.BlockSpec((1, rows), lambda h, i: (0, 0)),
        ],
        out_specs=[
            pl.BlockSpec((1, block, width), lambda h, i: (h, i, 0)),
            pl.BlockSpec((1, block, rows), lambda h, i: (h, i, 0)),
        ],
        out_shape=[
            jax.ShapeDtypeStruct((heads, rows, width), BF16),
            jax.ShapeDtypeStruct((heads, rows, rows), BF16),
        ],
        cost_estimate=pl.CostEstimate(
            flops=4 * heads * rows * rows * width,
            bytes_accessed=2 * heads * rows * (rows + 4 * width),
            transcendentals=heads * rows * rows,
        ),
        name="attend",
    )(queries, keys, values, ids[:, None], ids[None, :])


def attend_back_body(q_ref, k_ref, v_ref, p_ref, g_ref, dq_ref, dk_ref, dv_ref):
    @pl.when(pl.program_id(1) == 0)
    def _():
        dk_ref[...] = jnp.zeros_like(dk_ref)
        dv_ref[...] = jnp.zeros_like(dv_ref)

    grad = g_ref[0]
    low = p_ref[0]
    probs = low.astype(F32)
    grad_probs = right_cross(grad, v_ref[0])
    delta = jnp.sum(probs * grad_probs, axis=-1, keepdims=True)
    grad_scores = (probs * (grad_probs - delta)).astype(BF16)
    dq_ref[0] = dot(grad_scores, k_ref[0])
    dk_ref[0] += left_cross(grad_scores, q_ref[0])
    dv_ref[0] += left_cross(low, grad)


def attend_back(queries, keys, values, probs, grads):
    heads, rows, width = queries.shape
    block = min(256, rows)
    part = pl.BlockSpec((1, block, width), lambda h, i: (h, i, 0))
    whole = pl.BlockSpec((1, rows, width), lambda h, i: (h, 0, 0))
    return pl.pallas_call(
        attend_back_body,
        grid=(heads, rows // block),
        in_specs=[part, whole, whole, pl.BlockSpec((1, block, rows), lambda h, i: (h, i, 0)), part],
        out_specs=[part, whole, whole],
        out_shape=[jax.ShapeDtypeStruct((heads, rows, width), F32)] * 3,
        cost_estimate=pl.CostEstimate(
            flops=8 * heads * rows * rows * width,
            bytes_accessed=2 * heads * rows * (rows + 10 * width),
            transcendentals=0,
        ),
        name="attend_back",
    )(queries, keys, values, probs, grads)


def pack_body(*refs):
    out = refs[-1]
    columns = out.shape[1]
    rows = []
    for ref in refs[:-1]:
        value = ref[...].astype(F32)
        size = value.shape[1]
        if size < columns:
            rows.append(jnp.concatenate([value, jnp.zeros((1, columns - size), F32)], axis=1))
        else:
            rows += [value[:, i : i + columns] for i in range(0, size, columns)]
    rows.append(jnp.zeros((out.shape[0] - len(rows), columns), F32))
    out[...] = jnp.concatenate(rows, axis=0).astype(BF16)


def pack(vectors, columns):
    return pl.pallas_call(
        pack_body, out_shape=jax.ShapeDtypeStruct((16, columns), BF16), name="pack"
    )(*[v[None] for v in vectors])


GELU_SCALE = 0.7978845608028654
GELU_CUBE = 0.044715


def middle_body(
    m0, m1, m2, m3, x_ref, g_ref, wp_ref, wu_ref, wd_ref, vec_ref, bias_ref,
    z_ref, m_ref, dc_ref, dd_ref, du_ref, sum_ref,
):
    step = pl.program_id(0)

    @pl.when(step == 0)
    def _():
        dd_ref[...] = jnp.zeros_like(dd_ref)
        du_ref[...] = jnp.zeros_like(du_ref)
        sum_ref[...] = jnp.zeros_like(sum_ref)

    part = m0.shape[1]
    branch = vec_ref[0:1]
    for r, piece in enumerate((m0, m1, m2, m3)):
        branch = branch + dot(piece[...], wp_ref[r * part : (r + 1) * part])

    @pl.when(step == 0)
    def _():
        z_ref[...] = branch

    unit, _ = norm_parts(x_ref[...].astype(F32) + branch)
    normed = (unit * vec_ref[1:2] + vec_ref[2:3]).astype(BF16)
    inner = dot(normed, wu_ref[...]) + bias_ref[...]
    square = inner * inner
    bent = jnp.tanh(GELU_SCALE * (inner + GELU_CUBE * inner * square))
    half = 0.5 * (1.0 + bent)
    active = (inner * half).astype(BF16)
    slope = half + 0.5 * inner * (1.0 - bent * bent) * (
        GELU_SCALE * (1.0 + 3.0 * GELU_CUBE * square)
    )
    grad = g_ref[...]
    m_ref[...] = dot(active, wd_ref[...]).astype(BF16)
    dd_ref[...] += left_cross(active, grad)
    grad_inner = right_cross(grad, wd_ref[...]) * slope
    grad_low = grad_inner.astype(BF16)
    du_ref[...] += left_cross(normed, grad_low)
    grad_normed = right_cross(grad_low, wu_ref[...])
    dc_ref[...] = grad_normed.astype(BF16)
    sum_ref[0:1] += jnp.sum(grad_low.astype(F32), axis=0, keepdims=True)
    sum_ref[1:2] += jnp.sum(grad_normed * unit, axis=0, keepdims=True)
    sum_ref[2:3] += jnp.sum(grad_normed, axis=0, keepdims=True)


def middle(count, pieces, tokens_all, grads, w_proj, w_up, w_down, vectors, bias):
    rows, width = tokens_all.shape
    part = pieces[0].shape[1]
    hidden = w_up.shape[1]
    steps = rows // count

    def held(shape):
        return pl.BlockSpec(shape, lambda i: (0, 0))

    def shifted(r):
        return pl.BlockSpec((count, part), lambda i: (jnp.bitwise_xor(i, r), 0))

    block = pl.BlockSpec((count, width), lambda i: (i, 0))
    return pl.pallas_call(
        middle_body,
        grid=(steps,),
        in_specs=[shifted(r) for r in range(4)]
        + [block, block, held(w_proj.shape), held(w_up.shape), held(w_down.shape)]
        + [held(vectors.shape), held(bias.shape)],
        out_specs=[
            held((count, width)),
            block,
            block,
            held((hidden, width)),
            held((width, hidden)),
            held((8, width)),
        ],
        out_shape=[
            jax.ShapeDtypeStruct((count, width), F32),
            jax.ShapeDtypeStruct((rows, width), BF16),
            jax.ShapeDtypeStruct((rows, width), BF16),
            jax.ShapeDtypeStruct((hidden, width), F32),
            jax.ShapeDtypeStruct((width, hidden), F32),
            jax.ShapeDtypeStruct((8, width), F32),
        ],
        cost_estimate=pl.CostEstimate(
            flops=14 * rows * width * hidden,
            bytes_accessed=10 * rows * width + 14 * width * hidden,
            transcendentals=rows * hidden,
        ),
        name="middle",
    )(*pieces, tokens_all, grads, w_proj, w_up, w_down, vectors, bias)


def on_device(
    dp_size,
    fs_size,
    tokens,
    cotangent,
    segment_ids,
    valid_mask,
    ln1_gain,
    ln1_bias,
    qkv_weight,
    qkv_bias,
    query_gain,
    query_bias,
    key_gain,
    proj_weight,
    proj_bias,
    ln2_gain,
    ln2_bias,
    fc1_weight,
    fc1_bias,
    fc2_weight,
    fc2_bias,
):
    count, width = tokens.shape
    rank = lax.axis_index("fsdp")
    place = lax.axis_index("dp")
    near = functools.partial(swap, axis="fsdp", size=fs_size, bit=1)
    far = functools.partial(swap, axis="fsdp", size=fs_size, bit=2)
    own_heads = HEADS // fs_size
    part = own_heads * HEAD_DIM
    hidden = fc1_weight.shape[1]
    hidden_own = hidden // fs_size
    rows_own = qkv_weight.shape[0]
    rounds = [1 << i for i in range(dp_size.bit_length() - 1)]

    def gather(value):
        second = far(value)
        return [value, near(value), second, near(second)]

    def spread(pieces):
        return [pieces[0], near(pieces[1]), far(pieces[2]), swap(pieces[3], "fsdp", fs_size, 3)]

    def collect(low):
        low = [low[r * count : (r + 1) * count] for r in range(4)]
        other = near(jnp.concatenate([low[1], low[3]], axis=0)).astype(F32)
        first = low[0].astype(F32) + other[:count]
        second = far((low[2].astype(F32) + other[count:]).astype(BF16))
        return first + second.astype(F32)

    def at(r):
        return rank ^ r

    def ordered(pieces, axis):
        chosen = [lax.select_n(at(i), *[pieces[j] for j in range(4)]) for i in range(4)]
        return jnp.concatenate(chosen, axis=axis)

    small = pack(
        (ln1_gain, ln1_bias, ln2_gain, ln2_bias, proj_bias, fc2_bias, qkv_bias)
        + (query_gain, query_bias, key_gain),
        rows_own,
    )
    small_all = ordered([p[:, None] for p in gather(small)], 1).astype(F32)
    wide = small_all[:6].reshape(6, width)
    gain_one, shift_one, gain_two, shift_two, b_proj, b_down = [wide[i] for i in range(6)]
    narrow = query_gain.shape[0]
    gain_query, shift_query, gain_key = [
        small_all[i, :, :narrow].reshape(-1) for i in (9, 10, 11)
    ]
    b_qkv_all = small_all[6:9].transpose(1, 0, 2).reshape(-1)

    def own_columns(matrix, owner):
        return [
            lax.dynamic_slice_in_dim(matrix, block * width + owner * part, part, matrix.ndim - 1)
            for block in range(3)
        ]

    tokens_all = jnp.concatenate(gather(tokens), axis=0)
    w_qkv = ordered(
        spread([jnp.concatenate(own_columns(qkv_weight, at(r)), axis=1) for r in range(4)]), 0
    )
    w_proj_rel = jnp.concatenate(gather(proj_weight), axis=0)
    w_up = ordered(
        spread(
            [lax.dynamic_slice_in_dim(fc1_weight, at(r) * hidden_own, hidden_own, 1) for r in range(4)]
        ),
        0,
    )
    weights_valid = valid_mask.astype(F32)[:, None]
    grad_mlp_own = (cotangent.astype(F32) * weights_valid).astype(BF16)
    grad_mlp_low = jnp.concatenate(gather(grad_mlp_own), axis=0)
    ids = jnp.concatenate(
        [lax.dynamic_slice_in_dim(segment_ids, at(r) * count, count) for r in range(4)]
    )
    rows_all = 4 * count

    inputs = tokens_all.astype(F32)
    unit_one, scale_one = norm_parts(inputs)
    normed_low = (unit_one * gain_one + shift_one).astype(BF16)
    b_qkv = jnp.concatenate(own_columns(b_qkv_all, rank))
    projected = (dot(normed_low, w_qkv) + b_qkv).reshape(rows_all, 3 * own_heads, HEAD_DIM)
    projected = projected.transpose(1, 0, 2)
    unit_query, scale_query = norm_parts(projected[:own_heads])
    unit_key, scale_key = norm_parts(projected[own_heads : 2 * own_heads])
    queries = ((unit_query * gain_query + shift_query) * HEAD_DIM**-0.5).astype(BF16)
    keys = (unit_key * gain_key).astype(BF16)
    values = projected[2 * own_heads :].astype(BF16)
    mixed_heads, probs = attend(queries, keys, values, ids)
    mixed_own = mixed_heads.transpose(1, 0, 2).reshape(rows_all, part)
    vectors = jnp.concatenate([b_proj[None], gain_two[None], shift_two[None]])
    branch_own, mlp_part, grad_two_part, total_down, total_up, sums_middle = middle(
        count, gather(mixed_own), tokens_all, grad_mlp_low, w_proj_rel, w_up, fc2_weight, vectors,
        fc1_bias.astype(F32)[None],
    )
    hidden_one = inputs[:count] + branch_own

    def halve(total):
        for bit in rounds:
            size = total.shape[1] // 2
            low, high = total[:, :size], total[:, size:]
            upper = (place & bit) != 0
            sent = jnp.where(upper, low, high).astype(BF16)
            total = jnp.where(upper, high, low).astype(F32) + swap(sent, "dp", dp_size, bit).astype(F32)
        return total

    def halve_last(total):
        first, second = total[:, :rows_own], total[:, rows_own:]
        for bit in rounds:
            size = first.shape[1] // 2
            some = second.shape[1] // 2
            upper = (place & bit) != 0
            low = jnp.concatenate([first[:, :size], second[:, :some]], axis=1)
            high = jnp.concatenate([first[:, size:], second[:, some:]], axis=1)
            sent = jnp.where(upper, low, high).astype(BF16)
            total = jnp.where(upper, high, low).astype(F32)
            total = total + swap(sent, "dp", dp_size, bit).astype(F32)
            first, second = total[:, :size], total[:, size:]
        return total

    def unite_blocks(share):
        share = share[None]
        for bit in reversed(rounds):
            other = swap(share, "dp", dp_size, bit)
            upper = (place & bit) != 0
            share = jnp.where(
                upper,
                jnp.concatenate([other, share], axis=0),
                jnp.concatenate([share, other], axis=0),
            )
        return share.astype(F32)

    def unite(share):
        share = share.astype(BF16)
        for bit in reversed(rounds):
            other = swap(share, "dp", dp_size, bit)
            upper = (place & bit) != 0
            share = jnp.where(
                upper,
                jnp.concatenate([other, share], axis=0),
                jnp.concatenate([share, other], axis=0),
            )
        return share.astype(F32)

    def after(value, other):
        return lax.optimization_barrier((value, other))[0]

    def to_rows(share):
        share = share.astype(BF16)
        return spread([lax.dynamic_index_in_dim(share, at(r), 0, False) for r in range(4)])

    grad_normed_two = collect(grad_two_part)
    grad_out = grad_mlp_own.astype(F32)
    unit_two, scale_two = norm_parts(hidden_one)
    grad_hidden = grad_out + norm_back(grad_normed_two * gain_two, unit_two, scale_two)
    grad_branch_own = grad_hidden.astype(BF16)
    grad_branch_low = jnp.concatenate(gather(grad_branch_own), axis=0)
    grad_mixed = right_cross(grad_branch_low, proj_weight).astype(BF16)
    grad_mixed = grad_mixed.reshape(rows_all, own_heads, HEAD_DIM).transpose(1, 0, 2)
    total_proj = left_cross(mixed_own, grad_branch_low)
    grad_queries, grad_keys, grad_values = attend_back(queries, keys, values, probs, grad_mixed)
    grad_queries = grad_queries * HEAD_DIM**-0.5
    grad_gain_query = jnp.sum(grad_queries * unit_query, axis=(0, 1))
    grad_shift_query = jnp.sum(grad_queries, axis=(0, 1))
    grad_gain_key = jnp.sum(grad_keys * unit_key, axis=(0, 1))
    grad_projected = jnp.concatenate(
        [
            norm_back(grad_queries * gain_query, unit_query, scale_query).astype(BF16),
            norm_back(grad_keys * gain_key, unit_key, scale_key).astype(BF16),
            grad_values.astype(BF16),
        ],
        axis=0,
    )
    grad_projected = grad_projected.transpose(1, 0, 2).reshape(rows_all, 3 * part)
    total_qkv = left_cross(normed_low, grad_projected)
    grad_normed_one_part = right_cross(grad_projected, w_qkv)
    grad_normed_one = collect(grad_normed_one_part.astype(BF16))
    tokens_grad = grad_hidden + norm_back(
        grad_normed_one * gain_one, unit_one[:count], scale_one[:count]
    )

    branch_mlp = collect(mlp_part) + b_down
    result = hidden_one + branch_mlp
    rms_sums = jnp.stack(
        [
            jnp.sum(weights_valid * result * result),
            jnp.sum(weights_valid * branch_own * branch_own),
            jnp.sum(weights_valid * branch_mlp * branch_mlp),
            jnp.sum(weights_valid),
        ]
    )

    bias_qkv = jnp.sum(grad_projected.astype(F32), axis=0)
    bias_qkv_all = jnp.zeros((3 * width,), F32)
    for block in range(3):
        bias_qkv_all = lax.dynamic_update_slice(
            bias_qkv_all, bias_qkv[block * part : (block + 1) * part], (block * width + rank * part,)
        )
    bias_up_all = lax.dynamic_update_slice(jnp.zeros((hidden,), F32), sums_middle[0], (rank * hidden_own,))
    packed = [
        jnp.sum(grad_normed_one_part * unit_one, axis=0),
        jnp.sum(grad_normed_one_part, axis=0),
        bias_qkv_all,
        grad_gain_query,
        grad_shift_query,
        grad_gain_key,
        jnp.sum(grad_branch_own.astype(F32), axis=0),
        sums_middle[1],
        sums_middle[2],
        bias_up_all,
        jnp.sum(grad_out, axis=0),
    ]
    lengths = [v.shape[0] // fs_size for v in packed] + [4]
    vector = jnp.concatenate(
        [v.reshape(fs_size, -1) for v in packed] + [jnp.broadcast_to(rms_sums[None], (fs_size, 4))],
        axis=1,
    )
    vector = jnp.pad(vector, ((0, 0), (0, dp_size * 3 * part - vector.shape[1])))
    vector = vector.reshape(fs_size, dp_size, 3 * part)

    share_down = halve(total_down[None])[0]
    grad_down = unite(share_down)
    share_up = halve(
        jnp.concatenate(
            [total_up.reshape(fs_size, rows_own, hidden_own), total_proj[None]], axis=0
        )
    )
    grad_up_proj = unite(
        jnp.concatenate(
            [ordered(to_rows(share_up[:fs_size]), 1), share_up[fs_size].astype(BF16)], axis=1
        )
    )
    grad_up, grad_proj = grad_up_proj[:, :hidden], grad_up_proj[:, hidden:]
    total_last = jnp.concatenate([total_qkv.reshape(fs_size, rows_own, 3 * part), vector], axis=1)
    pieces_last = to_rows(halve_last(total_last))
    share_rows = rows_own // dp_size
    rows_qkv = ordered([p[:share_rows].reshape(share_rows, 3, 1, part) for p in pieces_last], 2)
    rows_qkv = rows_qkv.reshape(share_rows, 3 * width)
    rows_sum = [p[share_rows:].astype(F32) for p in pieces_last]
    rows_sum = ((rows_sum[0] + rows_sum[1]) + (rows_sum[2] + rows_sum[3])).astype(BF16)
    last = jnp.concatenate(
        [rows_qkv, jnp.pad(rows_sum, ((0, 0), (0, 3 * width - 3 * part)))], axis=0
    )
    last = unite_blocks(last)
    grad_qkv = last[:, :share_rows].reshape(rows_own, 3 * width)
    vector = last[:, share_rows, : 3 * part].reshape(-1)
    finals = []
    start = 0
    for length in lengths:
        finals.append(vector[start : start + length])
        start += length
    sums = finals.pop()
    return (
        result.astype(BF16),
        tokens_grad,
        finals[0],
        finals[1],
        grad_qkv,
        finals[2],
        finals[3],
        finals[4],
        finals[5],
        grad_proj,
        finals[6],
        finals[7],
        finals[8],
        grad_up,
        finals[9],
        grad_down,
        finals[10],
        jnp.sqrt(sums[:3] / sums[3]),
    )


def solution(mesh):
    rows = P(("dp", "fsdp"), None)
    vector = P("fsdp")
    matrix = P("fsdp", None)
    return jax.shard_map(
        functools.partial(on_device, mesh.shape["dp"], mesh.shape["fsdp"]),
        mesh=mesh,
        in_specs=(
            rows, rows, P("dp"), P(("dp", "fsdp")), vector, vector, matrix, vector, vector, vector,
            vector, matrix, vector, vector, vector, matrix, vector, matrix, vector,
        ),
        out_specs=(
            rows, rows, vector, vector, matrix, vector, vector, vector, vector, matrix, vector,
            vector, vector, matrix, vector, matrix, vector, P(),
        ),
        check_vma=False,
    )
```

```python
import functools

import jax
import jax.numpy as jnp
from jax import lax
from jax.experimental import pallas as pl
from jax.experimental.pallas import tpu as pltpu
from jax.sharding import PartitionSpec as P

HEADS = 12
HEAD_DIM = 64
EPS = 1e-06
MASKED = -1e30
F32 = jnp.float32
BF16 = jnp.bfloat16


def swap(value, axis, size, bit):
    return lax.ppermute(value, axis, [(i, i ^ bit) for i in range(size)])


def dot(first, second):
    return jnp.dot(first, second, preferred_element_type=F32)


def left_cross(first, second):
    return lax.dot_general(first, second, (((0,), (0,)), ((), ())), preferred_element_type=F32)


def right_cross(first, second):
    return lax.dot_general(first, second, (((1,), (1,)), ((), ())), preferred_element_type=F32)


def norm_parts(values):
    average = jnp.mean(values, axis=-1, keepdims=True)
    centred = values - average
    spread = jnp.mean(centred * centred, axis=-1, keepdims=True)
    scale = lax.rsqrt(spread + EPS)
    return centred * scale, scale


def norm_back(grad, unit, scale):
    return scale * (
        grad
        - jnp.mean(grad, axis=-1, keepdims=True)
        - unit * jnp.mean(grad * unit, axis=-1, keepdims=True)
    )


def block_of(step, count):
    return pl.ds(pl.multiple_of(step * count, count), count)


def front_body(
    count, x_ref, w_ref, vec_ref, bias_ref, head_ref, rows_ref, cols_ref,
    o_ref, p_ref, raw_ref, q_ref, k_ref, v_ref,
):
    heads, rows, size = q_ref.shape
    scaling = size**-0.5

    @pl.loop(0, rows // count)
    def _(step):
        at = block_of(step, count)
        unit, _ = norm_parts(x_ref[at].astype(F32))
        normed = (unit * vec_ref[0:1] + vec_ref[1:2]).astype(BF16)
        projected = dot(normed, w_ref[...]) + bias_ref[...]
        for h in range(heads):
            query, key, value = [
                projected[:, (j * heads + h) * size : (j * heads + h + 1) * size] for j in range(3)
            ]
            raw_ref[h, at] = query
            raw_ref[heads + h, at] = key
            unit, _ = norm_parts(query)
            q_ref[h, at] = ((unit * head_ref[0:1] + head_ref[1:2]) * scaling).astype(BF16)
            unit, _ = norm_parts(key)
            k_ref[h, at] = (unit * head_ref[2:3]).astype(BF16)
            v_ref[h, at] = value.astype(BF16)

    for h in range(heads):

        @pl.loop(0, rows // count)
        def _(step):
            at = block_of(step, count)
            scores = right_cross(q_ref[h, at], k_ref[h])
            scores = jnp.where(rows_ref[at] == cols_ref[...], scores, MASKED)
            top = jnp.max(scores, axis=-1, keepdims=True)
            raised = jnp.exp(scores - top)
            total = jnp.sum(raised, axis=-1, keepdims=True)
            probs = (raised * (1.0 / total)).astype(BF16)
            p_ref[h, at] = probs
            o_ref[at, h * size : (h + 1) * size] = dot(probs, v_ref[h]).astype(BF16)


def front(count, tokens_all, w_qkv, vectors, bias, head_vectors, ids):
    rows, width = tokens_all.shape
    size = head_vectors.shape[1]
    part = w_qkv.shape[1] // 3
    heads = part // size
    return pl.pallas_call(
        functools.partial(front_body, count),
        out_shape=[
            jax.ShapeDtypeStruct((rows, part), BF16),
            jax.ShapeDtypeStruct((heads, rows, rows), BF16),
            jax.ShapeDtypeStruct((2 * heads, rows, size), F32),
            jax.ShapeDtypeStruct((heads, rows, size), BF16),
            jax.ShapeDtypeStruct((heads, rows, size), BF16),
            jax.ShapeDtypeStruct((heads, rows, size), BF16),
        ],
        cost_estimate=pl.CostEstimate(
            flops=6 * rows * width * part + 4 * heads * rows * rows * size,
            bytes_accessed=2 * rows * (width + heads * rows + 8 * part) + 6 * width * part,
            transcendentals=heads * rows * rows,
        ),
        name="front",
    )(tokens_all, w_qkv, vectors, bias, head_vectors, ids[:, None], ids[None, :])


def back_body(
    count, z_ref, wp_ref, p_ref, raw_ref, q_ref, k_ref, v_ref, x_ref, w_ref, vec_ref, head_ref,
    dw_ref, da_ref, sum_ref, bias_ref, heads_ref, g_ref, dk_ref, dv_ref, dq_ref,
):
    heads, rows, size = q_ref.shape
    scaling = size**-0.5
    steps = rows // count
    sum_ref[...] = jnp.zeros_like(sum_ref)
    bias_ref[...] = jnp.zeros_like(bias_ref)
    heads_ref[...] = jnp.zeros_like(heads_ref)
    dw_ref[...] = jnp.zeros_like(dw_ref)
    for h in range(heads):
        dk_ref[...] = jnp.zeros_like(dk_ref)
        dv_ref[...] = jnp.zeros_like(dv_ref)

        @pl.loop(0, steps)
        def _(step):
            at = block_of(step, count)
            grad = right_cross(z_ref[at], wp_ref[h * size : (h + 1) * size]).astype(BF16)
            low = p_ref[h, at]
            probs = low.astype(F32)
            grad_probs = right_cross(grad, v_ref[h])
            delta = jnp.sum(probs * grad_probs, axis=-1, keepdims=True)
            grad_scores = (probs * (grad_probs - delta)).astype(BF16)
            dq_ref[at] = dot(grad_scores, k_ref[h])
            dk_ref[...] += left_cross(grad_scores, q_ref[h, at])
            dv_ref[...] += left_cross(low, grad)

        @pl.loop(0, steps)
        def _(step):
            at = block_of(step, count)
            grad = dq_ref[at] * scaling
            unit, scale = norm_parts(raw_ref[h, at])
            heads_ref[0:1] += jnp.sum(grad * unit, axis=0, keepdims=True)
            heads_ref[1:2] += jnp.sum(grad, axis=0, keepdims=True)
            g_ref[at, h * size : (h + 1) * size] = norm_back(
                grad * head_ref[0:1], unit, scale
            ).astype(BF16)
            grad = dk_ref[at]
            unit, scale = norm_parts(raw_ref[heads + h, at])
            heads_ref[2:3] += jnp.sum(grad * unit, axis=0, keepdims=True)
            first = (heads + h) * size
            g_ref[at, first : first + size] = norm_back(grad * head_ref[2:3], unit, scale).astype(
                BF16
            )
            first = (2 * heads + h) * size
            g_ref[at, first : first + size] = dv_ref[at].astype(BF16)

    @pl.loop(0, steps)
    def _(step):
        at = block_of(step, count)
        unit, _ = norm_parts(x_ref[at].astype(F32))
        normed = (unit * vec_ref[0:1] + vec_ref[1:2]).astype(BF16)
        grad = g_ref[at]
        dw_ref[...] += left_cross(normed, grad)
        bias_ref[0:1] += jnp.sum(grad.astype(F32), axis=0, keepdims=True)
        grad_normed = right_cross(grad, w_ref[...])
        da_ref[at] = grad_normed.astype(BF16)
        sum_ref[0:1] += jnp.sum(grad_normed * unit, axis=0, keepdims=True)
        sum_ref[1:2] += jnp.sum(grad_normed, axis=0, keepdims=True)


def back(count, z_all, w_proj, probs, raw, queries, keys, values, tokens_all, w_qkv, vectors, head_vectors):
    rows, width = tokens_all.shape
    heads, _, size = queries.shape
    part = heads * size
    return pl.pallas_call(
        functools.partial(back_body, count),
        out_shape=[
            jax.ShapeDtypeStruct((width, 3 * part), F32),
            jax.ShapeDtypeStruct((rows, width), BF16),
            jax.ShapeDtypeStruct((8, width), F32),
            jax.ShapeDtypeStruct((8, 3 * part), F32),
            jax.ShapeDtypeStruct((8, size), F32),
        ],
        scratch_shapes=[
            pltpu.VMEM((rows, 3 * part), BF16),
            pltpu.VMEM((rows, size), F32),
            pltpu.VMEM((rows, size), F32),
            pltpu.VMEM((rows, size), F32),
        ],
        cost_estimate=pl.CostEstimate(
            flops=14 * rows * width * part + 8 * heads * rows * rows * size,
            bytes_accessed=2 * rows * (3 * width + heads * rows + 12 * part) + 18 * width * part,
            transcendentals=0,
        ),
        name="back",
    )(z_all, w_proj, probs, raw, queries, keys, values, tokens_all, w_qkv, vectors, head_vectors)


def pack_body(*refs):
    out = refs[-1]
    columns = out.shape[1]
    rows = []
    for ref in refs[:-1]:
        value = ref[...].astype(F32)[None]
        size = value.shape[1]
        if size < columns:
            rows.append(jnp.concatenate([value, jnp.zeros((1, columns - size), F32)], axis=1))
        else:
            rows += [value[:, i : i + columns] for i in range(0, size, columns)]
    rows.append(jnp.zeros((out.shape[0] - len(rows), columns), F32))
    out[...] = jnp.concatenate(rows, axis=0).astype(BF16)


def pack(vectors, columns):
    return pl.pallas_call(
        pack_body, out_shape=jax.ShapeDtypeStruct((16, columns), BF16), name="pack"
    )(*vectors)


GELU_SCALE = 0.7978845608028654
GELU_CUBE = 0.044715


def middle_body(
    m0, m1, m2, m3, x_ref, g0, g1, g2, g3, w0, w1, w2, w3, wu_ref, wd_ref, vec_ref, bias_ref,
    z_ref, m_ref, dc_ref, dd_ref, du_ref, sum_ref, g_ref,
):
    step = pl.program_id(0)

    @pl.when(step == 0)
    def _():
        dd_ref[...] = jnp.zeros_like(dd_ref)
        du_ref[...] = jnp.zeros_like(du_ref)
        sum_ref[...] = jnp.zeros_like(sum_ref)

    for r, piece in enumerate((g0, g1, g2, g3)):

        @pl.when(step == r)
        def _(piece=piece):
            g_ref[...] = piece[...]

    branch = vec_ref[0:1]
    for piece, weight in zip((m0, m1, m2, m3), (w0, w1, w2, w3)):
        branch = branch + dot(piece[...], weight[...])

    @pl.when(step == 0)
    def _():
        z_ref[...] = branch

    unit, _ = norm_parts(x_ref[...].astype(F32) + branch)
    normed = (unit * vec_ref[1:2] + vec_ref[2:3]).astype(BF16)
    inner = dot(normed, wu_ref[...]) + bias_ref[...]
    square = inner * inner
    bent = jnp.tanh(GELU_SCALE * (inner + GELU_CUBE * inner * square))
    half = 0.5 * (1.0 + bent)
    active = (inner * half).astype(BF16)
    slope = half + 0.5 * inner * (1.0 - bent * bent) * (
        GELU_SCALE * (1.0 + 3.0 * GELU_CUBE * square)
    )
    grad = g_ref[...]
    m_ref[...] = dot(active, wd_ref[...]).astype(BF16)
    dd_ref[...] += left_cross(active, grad)
    grad_inner = right_cross(grad, wd_ref[...]) * slope
    grad_low = grad_inner.astype(BF16)
    du_ref[...] += left_cross(normed, grad_low)
    grad_normed = right_cross(grad_low, wu_ref[...])
    dc_ref[...] = grad_normed.astype(BF16)
    sum_ref[0:1] += jnp.sum(grad_low.astype(F32), axis=0, keepdims=True)
    sum_ref[1:2] += jnp.sum(grad_normed * unit, axis=0, keepdims=True)
    sum_ref[2:3] += jnp.sum(grad_normed, axis=0, keepdims=True)


def middle(count, pieces, tokens_all, grads, w_proj, w_up, w_down, vectors, bias):
    rows, width = tokens_all.shape
    part = pieces[0].shape[1]
    hidden = w_up.shape[1]
    steps = rows // count

    def held(shape):
        return pl.BlockSpec(shape, lambda i: (0, 0))

    def shifted(r):
        return pl.BlockSpec((count, part), lambda i: (jnp.bitwise_xor(i, r), 0))

    block = pl.BlockSpec((count, width), lambda i: (i, 0))
    return pl.pallas_call(
        middle_body,
        grid=(steps,),
        in_specs=[shifted(r) for r in range(4)]
        + [block]
        + [held(v.shape) for v in (*grads, *w_proj, w_up, w_down)]
        + [held(vectors.shape), held(bias.shape)],
        out_specs=[
            held((count, width)),
            block,
            block,
            held((hidden, width)),
            held((width, hidden)),
            held((8, width)),
        ],
        out_shape=[
            jax.ShapeDtypeStruct((count, width), F32),
            jax.ShapeDtypeStruct((rows, width), BF16),
            jax.ShapeDtypeStruct((rows, width), BF16),
            jax.ShapeDtypeStruct((hidden, width), F32),
            jax.ShapeDtypeStruct((width, hidden), F32),
            jax.ShapeDtypeStruct((8, width), F32),
        ],
        cost_estimate=pl.CostEstimate(
            flops=14 * rows * width * hidden,
            bytes_accessed=10 * rows * width + 14 * width * hidden,
            transcendentals=rows * hidden,
        ),
        scratch_shapes=[pltpu.VMEM((count, width), BF16)],
        name="middle",
    )(*pieces, tokens_all, *grads, *w_proj, w_up, w_down, vectors, bias)


def on_device(
    dp_size,
    fs_size,
    tokens,
    cotangent,
    segment_ids,
    valid_mask,
    ln1_gain,
    ln1_bias,
    qkv_weight,
    qkv_bias,
    query_gain,
    query_bias,
    key_gain,
    proj_weight,
    proj_bias,
    ln2_gain,
    ln2_bias,
    fc1_weight,
    fc1_bias,
    fc2_weight,
    fc2_bias,
):
    count, width = tokens.shape
    rank = lax.axis_index("fsdp")
    place = lax.axis_index("dp")
    near = functools.partial(swap, axis="fsdp", size=fs_size, bit=1)
    far = functools.partial(swap, axis="fsdp", size=fs_size, bit=2)
    own_heads = HEADS // fs_size
    part = own_heads * HEAD_DIM
    hidden = fc1_weight.shape[1]
    hidden_own = hidden // fs_size
    rows_own = qkv_weight.shape[0]
    rounds = [1 << i for i in range(dp_size.bit_length() - 1)]

    def gather(value):
        second = far(value)
        return [value, near(value), second, near(second)]

    def spread(pieces):
        return [pieces[0], near(pieces[1]), far(pieces[2]), swap(pieces[3], "fsdp", fs_size, 3)]

    def collect(low):
        low = [low[r * count : (r + 1) * count] for r in range(4)]
        other = near(jnp.concatenate([low[1], low[3]], axis=0)).astype(F32)
        first = low[0].astype(F32) + other[:count]
        second = far((low[2].astype(F32) + other[count:]).astype(BF16))
        return first + second.astype(F32)

    def at(r):
        return rank ^ r

    def ordered(pieces, axis):
        chosen = [lax.select_n(at(i), *[pieces[j] for j in range(4)]) for i in range(4)]
        return jnp.concatenate(chosen, axis=axis)

    small = pack(
        (ln1_gain, ln1_bias, ln2_gain, ln2_bias, proj_bias, fc2_bias, qkv_bias)
        + (query_gain, query_bias, key_gain),
        rows_own,
    )
    small_all = ordered([p[:, None] for p in gather(small)], 1).astype(F32)
    wide = small_all[:6].reshape(6, width)
    gain_one, shift_one, gain_two, shift_two, b_proj, b_down = [wide[i] for i in range(6)]
    narrow = query_gain.shape[0]
    gain_query, shift_query, gain_key = [
        small_all[i, :, :narrow].reshape(-1) for i in (9, 10, 11)
    ]
    b_qkv_all = small_all[6:9].transpose(1, 0, 2).reshape(-1)

    def own_columns(matrix, owner):
        return [
            lax.dynamic_slice_in_dim(matrix, block * width + owner * part, part, matrix.ndim - 1)
            for block in range(3)
        ]

    tokens_all = jnp.concatenate(gather(tokens), axis=0)
    w_qkv = ordered(
        spread([jnp.concatenate(own_columns(qkv_weight, at(r)), axis=1) for r in range(4)]), 0
    )
    def after(value, other):
        return lax.optimization_barrier((value, other))[0]

    w_proj_pieces = gather(after(proj_weight, w_qkv))
    w_up = ordered(
        spread(
            [
                lax.dynamic_slice_in_dim(
                    after(fc1_weight, w_qkv), at(r) * hidden_own, hidden_own, 1
                )
                for r in range(4)
            ]
        ),
        0,
    )
    weights_valid = valid_mask.astype(F32)[:, None]
    grad_mlp_own = (cotangent.astype(F32) * weights_valid).astype(BF16)
    grad_mlp_pieces = gather(after(grad_mlp_own, w_qkv))
    ids = jnp.concatenate(
        [lax.dynamic_slice_in_dim(segment_ids, at(r) * count, count) for r in range(4)]
    )
    rows_all = 4 * count

    b_qkv = jnp.concatenate(own_columns(b_qkv_all, rank))
    vectors_one = jnp.concatenate([gain_one[None], shift_one[None]])
    head_vectors = jnp.concatenate([gain_query[None], shift_query[None], gain_key[None]])
    mixed_own, probs, raw, queries, keys, values = front(
        count, tokens_all, w_qkv, vectors_one, b_qkv[None], head_vectors, ids
    )
    vectors = jnp.concatenate([b_proj[None], gain_two[None], shift_two[None]])
    branch_own, mlp_part, grad_two_part, total_down, total_up, sums_middle = middle(
        count, gather(mixed_own), tokens_all, grad_mlp_pieces, w_proj_pieces, w_up, fc2_weight, vectors,
        fc1_bias.astype(F32)[None],
    )
    inputs = tokens.astype(F32)
    hidden_one = inputs + branch_own

    def halve(total, marks=()):
        for order, bit in enumerate(rounds):
            size = total.shape[1] // 2
            low, high = total[:, :size], total[:, size:]
            upper = (place & bit) != 0
            sent = jnp.where(upper, low, high).astype(BF16)
            other = swap(sent, "dp", dp_size, bit)
            if order < len(marks):
                other = after(other, marks[order])
            total = jnp.where(upper, high, low).astype(F32) + other.astype(F32)
        return total

    def halve_last(total):
        first, second = total[:, :rows_own], total[:, rows_own:]
        for bit in rounds:
            size = first.shape[1] // 2
            some = second.shape[1] // 2
            upper = (place & bit) != 0
            low = jnp.concatenate([first[:, :size], second[:, :some]], axis=1)
            high = jnp.concatenate([first[:, size:], second[:, some:]], axis=1)
            sent = jnp.where(upper, low, high).astype(BF16)
            total = jnp.where(upper, high, low).astype(F32)
            total = total + swap(sent, "dp", dp_size, bit).astype(F32)
            first, second = total[:, :size], total[:, size:]
        return total

    def unite_blocks(share):
        share = share[None]
        for bit in reversed(rounds):
            other = swap(share, "dp", dp_size, bit)
            upper = (place & bit) != 0
            share = jnp.where(
                upper,
                jnp.concatenate([other, share], axis=0),
                jnp.concatenate([share, other], axis=0),
            )
        return share.astype(F32)

    def unite(share):
        share = share.astype(BF16)
        for bit in reversed(rounds):
            other = swap(share, "dp", dp_size, bit)
            upper = (place & bit) != 0
            share = jnp.where(
                upper,
                jnp.concatenate([other, share], axis=0),
                jnp.concatenate([share, other], axis=0),
            )
        return share.astype(F32)

    def to_rows(share):
        share = share.astype(BF16)
        return spread([lax.dynamic_index_in_dim(share, at(r), 0, False) for r in range(4)])

    grad_normed_two = collect(grad_two_part)
    grad_out = grad_mlp_own.astype(F32)
    unit_two, scale_two = norm_parts(hidden_one)
    grad_hidden = grad_out + norm_back(grad_normed_two * gain_two, unit_two, scale_two)
    grad_branch_own = grad_hidden.astype(BF16)
    grad_branch_low = jnp.concatenate(gather(grad_branch_own), axis=0)
    total_proj = left_cross(mixed_own, grad_branch_low)
    total_qkv, grad_one_part, sums_one, sums_bias, sums_heads = back(
        count, grad_branch_low, proj_weight, probs, raw, queries, keys, values, tokens_all, w_qkv,
        vectors_one, head_vectors,
    )
    grad_normed_one = collect(grad_one_part)
    unit_one, scale_one = norm_parts(inputs)
    tokens_grad = grad_hidden + norm_back(
        grad_normed_one * gain_one, unit_one, scale_one
    )

    branch_mlp = collect(mlp_part) + b_down
    result = hidden_one + branch_mlp
    rms_sums = jnp.stack(
        [
            jnp.sum(weights_valid * result * result),
            jnp.sum(weights_valid * branch_own * branch_own),
            jnp.sum(weights_valid * branch_mlp * branch_mlp),
            jnp.sum(weights_valid),
        ]
    )

    bias_qkv = sums_bias[0]
    bias_qkv_all = jnp.zeros((3 * width,), F32)
    for block in range(3):
        bias_qkv_all = lax.dynamic_update_slice(
            bias_qkv_all, bias_qkv[block * part : (block + 1) * part], (block * width + rank * part,)
        )
    bias_up_all = lax.dynamic_update_slice(jnp.zeros((hidden,), F32), sums_middle[0], (rank * hidden_own,))
    packed = [
        sums_one[0],
        sums_one[1],
        bias_qkv_all,
        sums_heads[0],
        sums_heads[1],
        sums_heads[2],
        jnp.sum(grad_branch_own.astype(F32), axis=0),
        sums_middle[1],
        sums_middle[2],
        bias_up_all,
        jnp.sum(grad_out, axis=0),
    ]
    lengths = [v.shape[0] // fs_size for v in packed] + [4]
    vector = jnp.concatenate(
        [v.reshape(fs_size, -1) for v in packed] + [jnp.broadcast_to(rms_sums[None], (fs_size, 4))],
        axis=1,
    )
    vector = jnp.pad(vector, ((0, 0), (0, dp_size * 3 * part - vector.shape[1])))
    vector = vector.reshape(fs_size, dp_size, 3 * part)

    share_down = halve(total_down[None], (grad_branch_own, grad_branch_low, sums_heads))[0]
    grad_down = unite(share_down)
    share_up = halve(
        jnp.concatenate(
            [total_up.reshape(fs_size, rows_own, hidden_own), total_proj[None]], axis=0
        ),
        (sums_heads,),
    )
    grad_up_proj = unite(
        jnp.concatenate(
            [ordered(to_rows(share_up[:fs_size]), 1), share_up[fs_size].astype(BF16)], axis=1
        )
    )
    grad_up, grad_proj = grad_up_proj[:, :hidden], grad_up_proj[:, hidden:]
    total_last = jnp.concatenate([total_qkv.reshape(fs_size, rows_own, 3 * part), vector], axis=1)
    pieces_last = to_rows(halve_last(total_last))
    share_rows = rows_own // dp_size
    rows_qkv = ordered([p[:share_rows].reshape(share_rows, 3, 1, part) for p in pieces_last], 2)
    rows_qkv = rows_qkv.reshape(share_rows, 3 * width)
    rows_sum = [p[share_rows:].astype(F32) for p in pieces_last]
    rows_sum = ((rows_sum[0] + rows_sum[1]) + (rows_sum[2] + rows_sum[3])).astype(BF16)
    last = jnp.concatenate(
        [rows_qkv, jnp.pad(rows_sum, ((0, 0), (0, 3 * width - 3 * part)))], axis=0
    )
    last = unite_blocks(last)
    grad_qkv = last[:, :share_rows].reshape(rows_own, 3 * width)
    vector = last[:, share_rows, : 3 * part].reshape(-1)
    finals = []
    start = 0
    for length in lengths:
        finals.append(vector[start : start + length])
        start += length
    sums = finals.pop()
    return (
        result.astype(BF16),
        tokens_grad,
        finals[0],
        finals[1],
        grad_qkv,
        finals[2],
        finals[3],
        finals[4],
        finals[5],
        grad_proj,
        finals[6],
        finals[7],
        finals[8],
        grad_up,
        finals[9],
        grad_down,
        finals[10],
        jnp.sqrt(sums[:3] / sums[3]),
    )


def solution(mesh):
    rows = P(("dp", "fsdp"), None)
    vector = P("fsdp")
    matrix = P("fsdp", None)
    return jax.shard_map(
        functools.partial(on_device, mesh.shape["dp"], mesh.shape["fsdp"]),
        mesh=mesh,
        in_specs=(
            rows, rows, P("dp"), P(("dp", "fsdp")), vector, vector, matrix, vector, vector, vector,
            vector, matrix, vector, vector, vector, matrix, vector, matrix, vector,
        ),
        out_specs=(
            rows, rows, vector, vector, matrix, vector, vector, vector, vector, matrix, vector,
            vector, vector, matrix, vector, matrix, vector, P(),
        ),
        check_vma=False,
    )
```

```python
import functools

import jax
import jax.numpy as jnp
from jax import lax
from jax.experimental import pallas as pl
from jax.experimental.pallas import tpu as pltpu
from jax.sharding import PartitionSpec as P


HEADS = 12
HEAD_DIM = 64
EPS = 1e-06
MASKED = -1e30
F32 = jnp.float32
BF16 = jnp.bfloat16


def swap(value, axis, size, bit):
    return lax.ppermute(value, axis, [(i, i ^ bit) for i in range(size)])


def dot(first, second):
    return jnp.dot(first, second, preferred_element_type=F32)


def left_cross(first, second):
    return lax.dot_general(first, second, (((0,), (0,)), ((), ())), preferred_element_type=F32)


def right_cross(first, second):
    return lax.dot_general(first, second, (((1,), (1,)), ((), ())), preferred_element_type=F32)


def norm_parts(values):
    average = jnp.mean(values, axis=-1, keepdims=True)
    centred = values - average
    spread = jnp.mean(centred * centred, axis=-1, keepdims=True)
    scale = lax.rsqrt(spread + EPS)
    return centred * scale, scale


def norm_back(grad, unit, scale):
    return scale * (
        grad
        - jnp.mean(grad, axis=-1, keepdims=True)
        - unit * jnp.mean(grad * unit, axis=-1, keepdims=True)
    )


def block_of(step, count):
    return pl.ds(pl.multiple_of(step * count, count), count)


def front_body(
    count, x_ref, w_ref, vec_ref, bias_ref, head_ref, rows_ref, cols_ref,
    o_ref, p_ref, raw_ref, q_ref, k_ref, v_ref,
):
    heads, rows, size = q_ref.shape
    scaling = size**-0.5

    @pl.loop(0, rows // count)
    def _(step):
        at = block_of(step, count)
        unit, _ = norm_parts(x_ref[at].astype(F32))
        normed = (unit * vec_ref[0:1] + vec_ref[1:2]).astype(BF16)
        projected = dot(normed, w_ref[...]) + bias_ref[...]
        for h in range(heads):
            query, key, value = [
                projected[:, (j * heads + h) * size : (j * heads + h + 1) * size] for j in range(3)
            ]
            raw_ref[h, at] = query
            raw_ref[heads + h, at] = key
            unit, _ = norm_parts(query)
            q_ref[h, at] = ((unit * head_ref[0:1] + head_ref[1:2]) * scaling).astype(BF16)
            unit, _ = norm_parts(key)
            k_ref[h, at] = (unit * head_ref[2:3]).astype(BF16)
            v_ref[h, at] = value.astype(BF16)

    for h in range(heads):

        @pl.loop(0, rows // count)
        def _(step):
            at = block_of(step, count)
            scores = right_cross(q_ref[h, at], k_ref[h])
            scores = jnp.where(rows_ref[at] == cols_ref[...], scores, MASKED)
            top = jnp.max(scores, axis=-1, keepdims=True)
            raised = jnp.exp(scores - top)
            total = jnp.sum(raised, axis=-1, keepdims=True)
            probs = (raised * (1.0 / total)).astype(BF16)
            p_ref[h, at] = probs
            o_ref[at, h * size : (h + 1) * size] = dot(probs, v_ref[h]).astype(BF16)


def front(count, tokens_all, w_qkv, vectors, bias, head_vectors, ids):
    rows, width = tokens_all.shape
    size = head_vectors.shape[1]
    part = w_qkv.shape[1] // 3
    heads = part // size
    return pl.pallas_call(
        functools.partial(front_body, count),
        out_shape=[
            jax.ShapeDtypeStruct((rows, part), BF16),
            jax.ShapeDtypeStruct((heads, rows, rows), BF16),
            jax.ShapeDtypeStruct((2 * heads, rows, size), F32),
            jax.ShapeDtypeStruct((heads, rows, size), BF16),
            jax.ShapeDtypeStruct((heads, rows, size), BF16),
            jax.ShapeDtypeStruct((heads, rows, size), BF16),
        ],
        cost_estimate=pl.CostEstimate(
            flops=6 * rows * width * part + 4 * heads * rows * rows * size,
            bytes_accessed=2 * rows * (width + heads * rows + 8 * part) + 6 * width * part,
            transcendentals=heads * rows * rows,
        ),
        name="front",
    )(tokens_all, w_qkv, vectors, bias, head_vectors, ids[:, None], ids[None, :])


def back_body(
    count, z_ref, wp_ref, p_ref, raw_ref, q_ref, k_ref, v_ref, x_ref, w_ref, vec_ref, head_ref,
    dw_ref, da_ref, sum_ref, bias_ref, heads_ref, g_ref, dk_ref, dv_ref, dq_ref,
):
    heads, rows, size = q_ref.shape
    scaling = size**-0.5
    steps = rows // count
    sum_ref[...] = jnp.zeros_like(sum_ref)
    bias_ref[...] = jnp.zeros_like(bias_ref)
    heads_ref[...] = jnp.zeros_like(heads_ref)
    dw_ref[...] = jnp.zeros_like(dw_ref)
    for h in range(heads):
        dk_ref[...] = jnp.zeros_like(dk_ref)
        dv_ref[...] = jnp.zeros_like(dv_ref)

        @pl.loop(0, steps)
        def _(step):
            at = block_of(step, count)
            grad = right_cross(z_ref[at], wp_ref[h * size : (h + 1) * size]).astype(BF16)
            low = p_ref[h, at]
            probs = low.astype(F32)
            grad_probs = right_cross(grad, v_ref[h])
            delta = jnp.sum(probs * grad_probs, axis=-1, keepdims=True)
            grad_scores = (probs * (grad_probs - delta)).astype(BF16)
            dq_ref[at] = dot(grad_scores, k_ref[h])
            dk_ref[...] += left_cross(grad_scores, q_ref[h, at])
            dv_ref[...] += left_cross(low, grad)

        @pl.loop(0, steps)
        def _(step):
            at = block_of(step, count)
            grad = dq_ref[at] * scaling
            unit, scale = norm_parts(raw_ref[h, at])
            heads_ref[0:1] += jnp.sum(grad * unit, axis=0, keepdims=True)
            heads_ref[1:2] += jnp.sum(grad, axis=0, keepdims=True)
            g_ref[at, h * size : (h + 1) * size] = norm_back(
                grad * head_ref[0:1], unit, scale
            ).astype(BF16)
            grad = dk_ref[at]
            unit, scale = norm_parts(raw_ref[heads + h, at])
            heads_ref[2:3] += jnp.sum(grad * unit, axis=0, keepdims=True)
            first = (heads + h) * size
            g_ref[at, first : first + size] = norm_back(grad * head_ref[2:3], unit, scale).astype(
                BF16
            )
            first = (2 * heads + h) * size
            g_ref[at, first : first + size] = dv_ref[at].astype(BF16)

    @pl.loop(0, steps)
    def _(step):
        at = block_of(step, count)
        unit, _ = norm_parts(x_ref[at].astype(F32))
        normed = (unit * vec_ref[0:1] + vec_ref[1:2]).astype(BF16)
        grad = g_ref[at]
        dw_ref[...] += left_cross(normed, grad)
        bias_ref[0:1] += jnp.sum(grad.astype(F32), axis=0, keepdims=True)
        grad_normed = right_cross(grad, w_ref[...])
        da_ref[at] = grad_normed.astype(BF16)
        sum_ref[0:1] += jnp.sum(grad_normed * unit, axis=0, keepdims=True)
        sum_ref[1:2] += jnp.sum(grad_normed, axis=0, keepdims=True)


def back(count, z_all, w_proj, probs, raw, queries, keys, values, tokens_all, w_qkv, vectors, head_vectors):
    rows, width = tokens_all.shape
    heads, _, size = queries.shape
    part = heads * size
    return pl.pallas_call(
        functools.partial(back_body, count),
        out_shape=[
            jax.ShapeDtypeStruct((width, 3 * part), F32),
            jax.ShapeDtypeStruct((rows, width), BF16),
            jax.ShapeDtypeStruct((8, width), F32),
            jax.ShapeDtypeStruct((8, 3 * part), F32),
            jax.ShapeDtypeStruct((8, size), F32),
        ],
        scratch_shapes=[
            pltpu.VMEM((rows, 3 * part), BF16),
            pltpu.VMEM((rows, size), F32),
            pltpu.VMEM((rows, size), F32),
            pltpu.VMEM((rows, size), F32),
        ],
        cost_estimate=pl.CostEstimate(
            flops=14 * rows * width * part + 8 * heads * rows * rows * size,
            bytes_accessed=2 * rows * (3 * width + heads * rows + 12 * part) + 18 * width * part,
            transcendentals=0,
        ),
        name="back",
    )(z_all, w_proj, probs, raw, queries, keys, values, tokens_all, w_qkv, vectors, head_vectors)


def pack_body(*refs):
    out = refs[-1]
    columns = out.shape[1]
    rows = []
    for ref in refs[:-1]:
        value = ref[...].astype(F32)[None]
        size = value.shape[1]
        if size < columns:
            rows.append(jnp.concatenate([value, jnp.zeros((1, columns - size), F32)], axis=1))
        else:
            rows += [value[:, i : i + columns] for i in range(0, size, columns)]
    rows.append(jnp.zeros((out.shape[0] - len(rows), columns), F32))
    out[...] = jnp.concatenate(rows, axis=0).astype(BF16)


def pack(vectors, columns):
    return pl.pallas_call(
        pack_body, out_shape=jax.ShapeDtypeStruct((16, columns), BF16), name="pack"
    )(*vectors)


def arrange_body(share_rows, rank_ref, p0, p1, p2, p3, o_ref):
    pieces = [p[...].astype(F32) for p in (p0, p1, p2, p3)]
    part = pieces[0].shape[1] // 3
    low, high = (rank_ref[0] & 1) == 1, (rank_ref[0] & 2) == 2
    pairs = [
        (jnp.where(low, a, b), jnp.where(low, b, a))
        for a, b in ((pieces[1], pieces[0]), (pieces[3], pieces[2]))
    ]
    total = (pieces[0] + pieces[1]) + (pieces[2] + pieces[3])
    chosen = [jnp.where(high, pairs[1][i], pairs[0][i]) for i in range(2)]
    chosen += [jnp.where(high, pairs[0][i], pairs[1][i]) for i in range(2)]
    placed = jnp.concatenate(
        [c[:, j * part : (j + 1) * part] for j in range(3) for c in chosen], axis=1
    )
    wide = jnp.concatenate([total] * 4, axis=1)
    row = lax.broadcasted_iota(jnp.int32, placed.shape, 0)
    o_ref[...] = jnp.where(row < share_rows, placed, wide).astype(BF16)


def arrange(share_rows, rank, pieces):
    rows, columns = pieces[0].shape
    vmem = pl.BlockSpec(memory_space=pltpu.VMEM)
    return pl.pallas_call(
        functools.partial(arrange_body, share_rows),
        in_specs=[pl.BlockSpec(memory_space=pltpu.SMEM)] + [vmem] * 4,
        out_specs=vmem,
        out_shape=jax.ShapeDtypeStruct((rows, 4 * columns), BF16),
        name="arrange",
    )(rank[None], *pieces)


GELU_SCALE = 0.7978845608028654
GELU_CUBE = 0.044715


def middle_body(
    m0, m1, m2, m3, x_ref, g0, g1, g2, g3, w0, w1, w2, w3, wu_ref, wd_ref, vec_ref, bias_ref,
    z_ref, m_ref, dc_ref, dd_ref, du_ref, sum_ref, g_ref,
):
    step = pl.program_id(0)

    @pl.when(step == 0)
    def _():
        dd_ref[...] = jnp.zeros_like(dd_ref)
        du_ref[...] = jnp.zeros_like(du_ref)
        sum_ref[...] = jnp.zeros_like(sum_ref)

    for r, piece in enumerate((g0, g1, g2, g3)):

        @pl.when(step == r)
        def _(piece=piece):
            g_ref[...] = piece[...]

    branch = vec_ref[0:1]
    for piece, weight in zip((m0, m1, m2, m3), (w0, w1, w2, w3)):
        branch = branch + dot(piece[...], weight[...])

    @pl.when(step == 0)
    def _():
        z_ref[...] = branch

    unit, _ = norm_parts(x_ref[...].astype(F32) + branch)
    normed = (unit * vec_ref[1:2] + vec_ref[2:3]).astype(BF16)
    inner = dot(normed, wu_ref[...]) + bias_ref[...]
    square = inner * inner
    bent = jnp.tanh(GELU_SCALE * (inner + GELU_CUBE * inner * square))
    half = 0.5 * (1.0 + bent)
    active = (inner * half).astype(BF16)
    slope = half + 0.5 * inner * (1.0 - bent * bent) * (
        GELU_SCALE * (1.0 + 3.0 * GELU_CUBE * square)
    )
    grad = g_ref[...]
    m_ref[...] = dot(active, wd_ref[...]).astype(BF16)
    dd_ref[...] += left_cross(active, grad)
    grad_inner = right_cross(grad, wd_ref[...]) * slope
    grad_low = grad_inner.astype(BF16)
    du_ref[...] += left_cross(normed, grad_low)
    grad_normed = right_cross(grad_low, wu_ref[...])
    dc_ref[...] = grad_normed.astype(BF16)
    sum_ref[0:1] += jnp.sum(grad_low.astype(F32), axis=0, keepdims=True)
    sum_ref[1:2] += jnp.sum(grad_normed * unit, axis=0, keepdims=True)
    sum_ref[2:3] += jnp.sum(grad_normed, axis=0, keepdims=True)


def middle(count, pieces, tokens_all, grads, w_proj, w_up, w_down, vectors, bias):
    rows, width = tokens_all.shape
    part = pieces[0].shape[1]
    hidden = w_up.shape[1]
    steps = rows // count

    def held(shape):
        return pl.BlockSpec(shape, lambda i: (0, 0))

    def shifted(r):
        return pl.BlockSpec((count, part), lambda i: (jnp.bitwise_xor(i, r), 0))

    block = pl.BlockSpec((count, width), lambda i: (i, 0))
    return pl.pallas_call(
        middle_body,
        grid=(steps,),
        in_specs=[shifted(r) for r in range(4)]
        + [block]
        + [held(v.shape) for v in (*grads, *w_proj, w_up, w_down)]
        + [held(vectors.shape), held(bias.shape)],
        out_specs=[
            held((count, width)),
            block,
            block,
            held((hidden, width)),
            held((width, hidden)),
            held((8, width)),
        ],
        out_shape=[
            jax.ShapeDtypeStruct((count, width), F32),
            jax.ShapeDtypeStruct((rows, width), BF16),
            jax.ShapeDtypeStruct((rows, width), BF16),
            jax.ShapeDtypeStruct((hidden, width), F32),
            jax.ShapeDtypeStruct((width, hidden), F32),
            jax.ShapeDtypeStruct((8, width), F32),
        ],
        cost_estimate=pl.CostEstimate(
            flops=14 * rows * width * hidden,
            bytes_accessed=10 * rows * width + 14 * width * hidden,
            transcendentals=rows * hidden,
        ),
        scratch_shapes=[pltpu.VMEM((count, width), BF16)],
        name="middle",
    )(*pieces, tokens_all, *grads, *w_proj, w_up, w_down, vectors, bias)


def on_device(
    dp_size,
    fs_size,
    tokens,
    cotangent,
    segment_ids,
    valid_mask,
    ln1_gain,
    ln1_bias,
    qkv_weight,
    qkv_bias,
    query_gain,
    query_bias,
    key_gain,
    proj_weight,
    proj_bias,
    ln2_gain,
    ln2_bias,
    fc1_weight,
    fc1_bias,
    fc2_weight,
    fc2_bias,
):
    count, width = tokens.shape
    rank = lax.axis_index("fsdp")
    place = lax.axis_index("dp")
    near = functools.partial(swap, axis="fsdp", size=fs_size, bit=1)
    far = functools.partial(swap, axis="fsdp", size=fs_size, bit=2)
    own_heads = HEADS // fs_size
    part = own_heads * HEAD_DIM
    hidden = fc1_weight.shape[1]
    hidden_own = hidden // fs_size
    rows_own = qkv_weight.shape[0]
    rounds = [1 << i for i in range(dp_size.bit_length() - 1)]

    def gather(value):
        second = far(value)
        return [value, near(value), second, near(second)]

    def spread(pieces):
        return [pieces[0], near(pieces[1]), far(pieces[2]), swap(pieces[3], "fsdp", fs_size, 3)]

    def collect(low):
        low = [low[r * count : (r + 1) * count] for r in range(4)]
        other = near(jnp.concatenate([low[1], low[3]], axis=0)).astype(F32)
        first = low[0].astype(F32) + other[:count]
        sent = (low[2].astype(F32) + other[count:]).astype(BF16)
        return first + far(sent).astype(F32), sent

    def at(r):
        return rank ^ r

    def ordered(pieces, axis):
        chosen = [lax.select_n(at(i), *[pieces[j] for j in range(4)]) for i in range(4)]
        return jnp.concatenate(chosen, axis=axis)

    small = pack(
        (ln1_gain, ln1_bias, ln2_gain, ln2_bias, proj_bias, fc2_bias, qkv_bias)
        + (query_gain, query_bias, key_gain),
        rows_own,
    )
    small_all = ordered([p[:, None] for p in gather(small)], 1).astype(F32)
    wide = small_all[:6].reshape(6, width)
    gain_one, shift_one, gain_two, shift_two, b_proj, b_down = [wide[i] for i in range(6)]
    narrow = query_gain.shape[0]
    gain_query, shift_query, gain_key = [
        small_all[i, :, :narrow].reshape(-1) for i in (9, 10, 11)
    ]
    b_qkv_all = small_all[6:9].transpose(1, 0, 2).reshape(-1)

    def own_columns(matrix, owner):
        return [
            lax.dynamic_slice_in_dim(matrix, block * width + owner * part, part, matrix.ndim - 1)
            for block in range(3)
        ]

    tokens_all = jnp.concatenate(gather(tokens), axis=0)
    w_qkv = ordered(
        spread([jnp.concatenate(own_columns(qkv_weight, at(r)), axis=1) for r in range(4)]), 0
    )

    def after(value, other):
        return lax.optimization_barrier((value, other))[0]

    w_proj_pieces = gather(after(proj_weight, w_qkv))
    up_pieces = [
        lax.dynamic_slice_in_dim(after(fc1_weight, w_qkv), at(r) * hidden_own, hidden_own, 1)
        for r in range(4)
    ]
    up_pieces[1] = near(up_pieces[1])
    up_pieces[2] = far(up_pieces[2])
    up_pieces[3] = swap(up_pieces[3], "fsdp", fs_size, 3)
    w_up = ordered(up_pieces, 0)
    weights_valid = valid_mask.astype(F32)[:, None]
    grad_mlp_own = (cotangent.astype(F32) * weights_valid).astype(BF16)
    grad_mlp_pieces = gather(after(grad_mlp_own, w_qkv))
    ids = jnp.concatenate(
        [lax.dynamic_slice_in_dim(segment_ids, at(r) * count, count) for r in range(4)]
    )

    b_qkv = jnp.concatenate(own_columns(b_qkv_all, rank))
    vectors_one = jnp.concatenate([gain_one[None], shift_one[None]])
    head_vectors = jnp.concatenate([gain_query[None], shift_query[None], gain_key[None]])
    mixed_own, probs, raw, queries, keys, values = front(
        count, tokens_all, w_qkv, vectors_one, b_qkv[None], head_vectors, ids
    )
    vectors = jnp.concatenate([b_proj[None], gain_two[None], shift_two[None]])
    branch_own, mlp_part, grad_two_part, total_down, total_up, sums_middle = middle(
        count, gather(mixed_own), tokens_all, grad_mlp_pieces, w_proj_pieces, w_up, fc2_weight, vectors,
        fc1_bias.astype(F32)[None],
    )
    inputs = tokens.astype(F32)
    hidden_one = inputs + branch_own

    def held_back(other, marks, order):
        return after(other, marks[order]) if order < len(marks) and marks[order] is not None else other

    def halve(total, marks=(), tail=0):
        seen = []
        first, second = total[:, : total.shape[1] - tail], total[:, total.shape[1] - tail :]
        for order, bit in enumerate(rounds):
            size = first.shape[1] // 2
            some = second.shape[1] // 2
            low, high = first[:, :size], first[:, size:]
            if tail:
                low = jnp.concatenate([low, second[:, :some]], axis=1)
                high = jnp.concatenate([high, second[:, some:]], axis=1)
            upper = (place & bit) != 0
            sent = jnp.where(upper, low, high).astype(BF16)
            other = held_back(swap(sent, "dp", dp_size, bit), marks, order)
            seen.append(other)
            total = jnp.where(upper, high, low).astype(F32) + other.astype(F32)
            first, second = total[:, :size], total[:, size:]
        return total, seen

    def unite(share, marks=()):
        share = share.astype(BF16)[None]
        seen = []
        for order, bit in enumerate(reversed(rounds)):
            other = held_back(swap(share, "dp", dp_size, bit), marks, order)
            seen.append(other)
            upper = (place & bit) != 0
            share = jnp.where(
                upper,
                jnp.concatenate([other, share], axis=0),
                jnp.concatenate([share, other], axis=0),
            )
        return share, seen

    def to_rows(share):
        share = share.astype(BF16)
        return spread([lax.dynamic_index_in_dim(share, at(r), 0, False) for r in range(4)])

    grad_normed_two, mark_two = collect(grad_two_part)
    grad_out = grad_mlp_own.astype(F32)
    unit_two, scale_two = norm_parts(hidden_one)
    grad_hidden = grad_out + norm_back(grad_normed_two * gain_two, unit_two, scale_two)
    grad_branch_own = grad_hidden.astype(BF16)
    grad_branch_low = jnp.concatenate(gather(grad_branch_own), axis=0)
    total_proj = left_cross(mixed_own, grad_branch_low)
    total_qkv, grad_one_part, sums_one, sums_bias, sums_heads = back(
        count, grad_branch_low, proj_weight, probs, raw, queries, keys, values, tokens_all, w_qkv,
        vectors_one, head_vectors,
    )
    grad_normed_one, _ = collect(grad_one_part)
    unit_one, scale_one = norm_parts(inputs)
    tokens_grad = grad_hidden + norm_back(
        grad_normed_one * gain_one, unit_one, scale_one
    )

    branch_mlp = collect(after(mlp_part, sums_heads))[0] + b_down
    result = hidden_one + branch_mlp
    rms_sums = jnp.stack(
        [
            jnp.sum(weights_valid * result * result),
            jnp.sum(weights_valid * branch_own * branch_own),
            jnp.sum(weights_valid * branch_mlp * branch_mlp),
            jnp.sum(weights_valid),
        ]
    )

    bias_qkv = sums_bias[0]
    bias_qkv_all = jnp.zeros((3 * width,), F32)
    for block in range(3):
        bias_qkv_all = lax.dynamic_update_slice(
            bias_qkv_all, bias_qkv[block * part : (block + 1) * part], (block * width + rank * part,)
        )
    bias_up_all = lax.dynamic_update_slice(jnp.zeros((hidden,), F32), sums_middle[0], (rank * hidden_own,))
    packed = [
        sums_one[0],
        sums_one[1],
        bias_qkv_all,
        sums_heads[0],
        sums_heads[1],
        sums_heads[2],
        jnp.sum(grad_branch_own.astype(F32), axis=0),
        sums_middle[1],
        sums_middle[2],
        bias_up_all,
        jnp.sum(grad_out, axis=0),
    ]
    lengths = [v.shape[0] // fs_size for v in packed] + [4]
    vector = jnp.concatenate(
        [v.reshape(fs_size, -1) for v in packed] + [jnp.broadcast_to(rms_sums[None], (fs_size, 4))],
        axis=1,
    )
    vector = jnp.pad(vector, ((0, 0), (0, dp_size * 3 * part - vector.shape[1])))
    vector = vector.reshape(fs_size, dp_size, 3 * part)

    count_rounds = len(rounds)
    total_last = jnp.concatenate([total_qkv.reshape(fs_size, rows_own, 3 * part), vector], axis=1)
    share_last, seen = halve(total_last, tail=dp_size)
    pieces_last = to_rows(share_last)
    share_rows = rows_own // dp_size
    last, seen_back = unite(arrange(share_rows, rank, pieces_last))
    seen = [*seen, pieces_last[3], *seen_back]

    early = [mark_two, grad_branch_own] + [grad_branch_low] * (count_rounds - 2)
    share_down, seen_down = halve(total_down[None], early)
    grad_down, _ = unite(share_down[0], [sums_heads, seen[0], seen[1]])
    grad_down = grad_down.astype(F32).reshape(hidden_own, width)
    total_up = after(total_up, seen_down[0])
    late = [grad_branch_own] + [sums_heads] * (count_rounds - 1)
    share_up, _ = halve(total_up.reshape(fs_size, rows_own, hidden_own), late)
    grad_up, _ = unite(ordered(to_rows(share_up), 1), [seen[1], seen[2], seen[count_rounds]])
    grad_up = grad_up.astype(F32).reshape(rows_own, hidden)
    share_proj, _ = halve(total_proj[None], seen[:count_rounds])
    grad_proj, _ = unite(share_proj[0], seen[count_rounds:])
    grad_proj = grad_proj.astype(F32).reshape(rows_own, width)
    last = last.astype(F32)
    grad_qkv = last[:, :share_rows].reshape(rows_own, 3 * width)
    vector = last[:, share_rows, : 3 * part].reshape(-1)
    finals = []
    start = 0
    for length in lengths:
        finals.append(vector[start : start + length])
        start += length
    sums = finals.pop()
    return (
        result.astype(BF16),
        tokens_grad,
        finals[0],
        finals[1],
        grad_qkv,
        finals[2],
        finals[3],
        finals[4],
        finals[5],
        grad_proj,
        finals[6],
        finals[7],
        finals[8],
        grad_up,
        finals[9],
        grad_down,
        finals[10],
        jnp.sqrt(sums[:3] / sums[3]),
    )


def solution(mesh):
    rows = P(("dp", "fsdp"), None)
    vector = P("fsdp")
    matrix = P("fsdp", None)
    device = functools.partial(on_device, mesh.shape["dp"], mesh.shape["fsdp"])

    return jax.shard_map(
        device,
        mesh=mesh,
        in_specs=(
            rows, rows, P("dp"), P(("dp", "fsdp")), vector, vector, matrix, vector, vector, vector,
            vector, matrix, vector, vector, vector, matrix, vector, matrix, vector,
        ),
        out_specs=(
            rows, rows, vector, vector, matrix, vector, vector, vector, vector, matrix, vector,
            vector, vector, matrix, vector, matrix, vector, P(),
        ),
        check_vma=False,
    )
```

```python
import functools

import jax
import jax.numpy as jnp
from jax import lax
from jax.experimental import pallas as pl
from jax.experimental.pallas import tpu as pltpu
from jax.sharding import PartitionSpec as P


HEADS = 12
HEAD_DIM = 64
EPS = 1e-06
MASKED = -1e30
F32 = jnp.float32
BF16 = jnp.bfloat16


def swap(value, axis, size, bit):
    return lax.ppermute(value, axis, [(i, i ^ bit) for i in range(size)])


def dot(first, second):
    return jnp.dot(first, second, preferred_element_type=F32)


def left_cross(first, second):
    return lax.dot_general(first, second, (((0,), (0,)), ((), ())), preferred_element_type=F32)


def right_cross(first, second):
    return lax.dot_general(first, second, (((1,), (1,)), ((), ())), preferred_element_type=F32)


def norm_parts(values):
    average = jnp.mean(values, axis=-1, keepdims=True)
    centred = values - average
    spread = jnp.mean(centred * centred, axis=-1, keepdims=True)
    scale = lax.rsqrt(spread + EPS)
    return centred * scale, scale


def norm_back(grad, unit, scale):
    return scale * (
        grad
        - jnp.mean(grad, axis=-1, keepdims=True)
        - unit * jnp.mean(grad * unit, axis=-1, keepdims=True)
    )


def block_of(step, count):
    return pl.ds(pl.multiple_of(step * count, count), count)


def front_body(
    count, x_ref, w_ref, vec_ref, bias_ref, head_ref, rows_ref, cols_ref,
    o_ref, p_ref, raw_ref, q_ref, k_ref, v_ref,
):
    heads, rows, size = q_ref.shape
    scaling = size**-0.5

    @pl.loop(0, rows // count)
    def _(step):
        at = block_of(step, count)
        unit, _ = norm_parts(x_ref[at].astype(F32))
        normed = (unit * vec_ref[0:1] + vec_ref[1:2]).astype(BF16)
        projected = dot(normed, w_ref[...]) + bias_ref[...]
        for h in range(heads):
            query, key, value = [
                projected[:, (j * heads + h) * size : (j * heads + h + 1) * size] for j in range(3)
            ]
            raw_ref[h, at] = query
            raw_ref[heads + h, at] = key
            unit, _ = norm_parts(query)
            q_ref[h, at] = ((unit * head_ref[0:1] + head_ref[1:2]) * scaling).astype(BF16)
            unit, _ = norm_parts(key)
            k_ref[h, at] = (unit * head_ref[2:3]).astype(BF16)
            v_ref[h, at] = value.astype(BF16)

    for h in range(heads):

        @pl.loop(0, rows // count)
        def _(step):
            at = block_of(step, count)
            scores = right_cross(q_ref[h, at], k_ref[h])
            scores = jnp.where(rows_ref[at] == cols_ref[...], scores, MASKED)
            top = jnp.max(scores, axis=-1, keepdims=True)
            raised = jnp.exp(scores - top)
            total = jnp.sum(raised, axis=-1, keepdims=True)
            probs = (raised * (1.0 / total)).astype(BF16)
            p_ref[h, at] = probs
            o_ref[at, h * size : (h + 1) * size] = dot(probs, v_ref[h]).astype(BF16)


def front(count, tokens_all, w_qkv, vectors, bias, head_vectors, ids):
    rows, width = tokens_all.shape
    size = head_vectors.shape[1]
    part = w_qkv.shape[1] // 3
    heads = part // size
    return pl.pallas_call(
        functools.partial(front_body, count),
        out_shape=[
            jax.ShapeDtypeStruct((rows, part), BF16),
            jax.ShapeDtypeStruct((heads, rows, rows), BF16),
            jax.ShapeDtypeStruct((2 * heads, rows, size), F32),
            jax.ShapeDtypeStruct((heads, rows, size), BF16),
            jax.ShapeDtypeStruct((heads, rows, size), BF16),
            jax.ShapeDtypeStruct((heads, rows, size), BF16),
        ],
        cost_estimate=pl.CostEstimate(
            flops=6 * rows * width * part + 4 * heads * rows * rows * size,
            bytes_accessed=2 * rows * (width + heads * rows + 8 * part) + 6 * width * part,
            transcendentals=heads * rows * rows,
        ),
        name="front",
    )(tokens_all, w_qkv, vectors, bias, head_vectors, ids[:, None], ids[None, :])


def back_body(
    count, rank_ref, z_ref, wp_ref, p_ref, raw_ref, q_ref, k_ref, v_ref, x_ref, w_ref, vec_ref,
    head_ref, early_ref, out_ref, da_ref, sum_ref, bias_ref, heads_ref, dw_ref, g_ref, dk_ref,
    dv_ref, dq_ref,
):
    heads, rows, size = q_ref.shape
    scaling = size**-0.5
    steps = rows // count
    sum_ref[...] = jnp.zeros_like(sum_ref)
    bias_ref[...] = jnp.zeros_like(bias_ref)
    heads_ref[...] = jnp.zeros_like(heads_ref)
    dw_ref[...] = jnp.zeros_like(dw_ref)
    for h in range(heads):
        dk_ref[...] = jnp.zeros_like(dk_ref)
        dv_ref[...] = jnp.zeros_like(dv_ref)

        @pl.loop(0, steps)
        def _(step):
            at = block_of(step, count)
            grad = right_cross(z_ref[at], wp_ref[h * size : (h + 1) * size]).astype(BF16)
            low = p_ref[h, at]
            probs = low.astype(F32)
            grad_probs = right_cross(grad, v_ref[h])
            delta = jnp.sum(probs * grad_probs, axis=-1, keepdims=True)
            grad_scores = (probs * (grad_probs - delta)).astype(BF16)
            dq_ref[at] = dot(grad_scores, k_ref[h])
            dk_ref[...] += left_cross(grad_scores, q_ref[h, at])
            dv_ref[...] += left_cross(low, grad)

        @pl.loop(0, steps)
        def _(step):
            at = block_of(step, count)
            grad = dq_ref[at] * scaling
            unit, scale = norm_parts(raw_ref[h, at])
            heads_ref[0:1] += jnp.sum(grad * unit, axis=0, keepdims=True)
            heads_ref[1:2] += jnp.sum(grad, axis=0, keepdims=True)
            g_ref[at, h * size : (h + 1) * size] = norm_back(
                grad * head_ref[0:1], unit, scale
            ).astype(BF16)
            grad = dk_ref[at]
            unit, scale = norm_parts(raw_ref[heads + h, at])
            heads_ref[2:3] += jnp.sum(grad * unit, axis=0, keepdims=True)
            first = (heads + h) * size
            g_ref[at, first : first + size] = norm_back(grad * head_ref[2:3], unit, scale).astype(
                BF16
            )
            first = (2 * heads + h) * size
            g_ref[at, first : first + size] = dv_ref[at].astype(BF16)

    @pl.loop(0, steps)
    def _(step):
        at = block_of(step, count)
        unit, _ = norm_parts(x_ref[at].astype(F32))
        normed = (unit * vec_ref[0:1] + vec_ref[1:2]).astype(BF16)
        grad = g_ref[at]
        dw_ref[...] += left_cross(normed, grad)
        bias_ref[0:1] += jnp.sum(grad.astype(F32), axis=0, keepdims=True)
        grad_normed = right_cross(grad, w_ref[...])
        da_ref[at] = grad_normed.astype(BF16)
        sum_ref[0:1] += jnp.sum(grad_normed * unit, axis=0, keepdims=True)
        sum_ref[1:2] += jnp.sum(grad_normed, axis=0, keepdims=True)


    owners, total_rows, columns = out_ref.shape
    own = dw_ref.shape[0] // owners
    part = columns // 3
    rank = rank_ref[0]
    narrow = size // owners
    for o in range(owners):
        out_ref[o, :own] = dw_ref[o * own : (o + 1) * own]
        first = jnp.concatenate(
            [sum_ref[i : i + 1, o * own : (o + 1) * own] for i in range(2)]
            + [jnp.zeros((1, columns - 2 * own), F32)],
            axis=1,
        )
        groups = []
        for j in range(3):
            group = 3 * o + j
            value = bias_ref[0:1, group // owners * part : (group // owners + 1) * part]
            groups.append(jnp.where(rank == group % owners, value, 0.0))
        gains = [heads_ref[i : i + 1, o * narrow : (o + 1) * narrow] for i in range(3)]
        third = jnp.concatenate([*gains, jnp.zeros((1, columns - 3 * narrow), F32)], axis=1)
        out_ref[o, own:] = jnp.concatenate(
            [first, jnp.concatenate(groups, axis=1), third, early_ref[o]]
            + [jnp.zeros((total_rows - own - 3 - early_ref.shape[1], columns), F32)],
            axis=0,
        )


def back(count, extra, rank, *values):
    _, _, _, _, queries, _, _, tokens_all, _, _, _, early = values
    rows, width = tokens_all.shape
    heads, _, size = queries.shape
    part = heads * size
    owners = early.shape[0]
    vmem = pl.BlockSpec(memory_space=pltpu.VMEM)
    return pl.pallas_call(
        functools.partial(back_body, count),
        in_specs=[pl.BlockSpec(memory_space=pltpu.SMEM)] + [vmem] * len(values),
        out_specs=[vmem, vmem],
        out_shape=[
            jax.ShapeDtypeStruct((owners, width // owners + extra, 3 * part), F32),
            jax.ShapeDtypeStruct((rows, width), BF16),
        ],
        scratch_shapes=[
            pltpu.VMEM((8, width), F32),
            pltpu.VMEM((8, 3 * part), F32),
            pltpu.VMEM((8, size), F32),
            pltpu.VMEM((width, 3 * part), F32),
            pltpu.VMEM((rows, 3 * part), BF16),
            pltpu.VMEM((rows, size), F32),
            pltpu.VMEM((rows, size), F32),
            pltpu.VMEM((rows, size), F32),
        ],
        cost_estimate=pl.CostEstimate(
            flops=14 * rows * width * part + 8 * heads * rows * rows * size,
            bytes_accessed=2 * rows * (3 * width + heads * rows + 12 * part) + 18 * width * part,
            transcendentals=0,
        ),
        name="back",
    )(rank[None], *values)


def pack_body(*refs):
    out = refs[-1]
    columns = out.shape[1]
    rows = []
    for ref in refs[:-1]:
        value = ref[...].astype(F32)[None]
        size = value.shape[1]
        if size < columns:
            rows.append(jnp.concatenate([value, jnp.zeros((1, columns - size), F32)], axis=1))
        else:
            rows += [value[:, i : i + columns] for i in range(0, size, columns)]
    rows.append(jnp.zeros((out.shape[0] - len(rows), columns), F32))
    out[...] = jnp.concatenate(rows, axis=0).astype(BF16)


def pack(vectors, columns):
    return pl.pallas_call(
        pack_body, out_shape=jax.ShapeDtypeStruct((16, columns), BF16), name="pack"
    )(*vectors)


def arrange_body(share_rows, rank_ref, p0, p1, p2, p3, o_ref):
    pieces = [p[...].astype(F32) for p in (p0, p1, p2, p3)]
    part = pieces[0].shape[1] // 3
    low, high = (rank_ref[0] & 1) == 1, (rank_ref[0] & 2) == 2
    pairs = [
        (jnp.where(low, a, b), jnp.where(low, b, a))
        for a, b in ((pieces[1], pieces[0]), (pieces[3], pieces[2]))
    ]
    total = (pieces[0] + pieces[1]) + (pieces[2] + pieces[3])
    chosen = [jnp.where(high, pairs[1][i], pairs[0][i]) for i in range(2)]
    chosen += [jnp.where(high, pairs[0][i], pairs[1][i]) for i in range(2)]
    placed = jnp.concatenate(
        [c[:, j * part : (j + 1) * part] for j in range(3) for c in chosen], axis=1
    )
    wide = jnp.concatenate([total] * 4, axis=1)
    row = lax.broadcasted_iota(jnp.int32, placed.shape, 0)
    o_ref[...] = jnp.where(row < share_rows, placed, wide).astype(BF16)


def arrange(share_rows, rank, pieces):
    rows, columns = pieces[0].shape
    vmem = pl.BlockSpec(memory_space=pltpu.VMEM)
    return pl.pallas_call(
        functools.partial(arrange_body, share_rows),
        in_specs=[pl.BlockSpec(memory_space=pltpu.SMEM)] + [vmem] * 4,
        out_specs=vmem,
        out_shape=jax.ShapeDtypeStruct((rows, 4 * columns), BF16),
        name="arrange",
    )(rank[None], *pieces)


GELU_SCALE = 0.7978845608028654
GELU_CUBE = 0.044715


def middle_body(
    m0, m1, m2, m3, x_ref, g0, g1, g2, g3, w0, w1, w2, w3, wu_ref, wd_ref, vec_ref, bias_ref,
    z_ref, m_ref, dc_ref, dd_ref, du_ref, sum_ref, g_ref,
):
    step = pl.program_id(0)

    @pl.when(step == 0)
    def _():
        dd_ref[...] = jnp.zeros_like(dd_ref)
        du_ref[...] = jnp.zeros_like(du_ref)
        sum_ref[...] = jnp.zeros_like(sum_ref)

    for r, piece in enumerate((g0, g1, g2, g3)):

        @pl.when(step == r)
        def _(piece=piece):
            g_ref[...] = piece[...]

    branch = vec_ref[0:1]
    for piece, weight in zip((m0, m1, m2, m3), (w0, w1, w2, w3)):
        branch = branch + dot(piece[...], weight[...])

    @pl.when(step == 0)
    def _():
        z_ref[...] = branch

    unit, _ = norm_parts(x_ref[...].astype(F32) + branch)
    normed = (unit * vec_ref[1:2] + vec_ref[2:3]).astype(BF16)
    inner = dot(normed, wu_ref[...]) + bias_ref[...]
    square = inner * inner
    bent = jnp.tanh(GELU_SCALE * (inner + GELU_CUBE * inner * square))
    half = 0.5 * (1.0 + bent)
    active = (inner * half).astype(BF16)
    slope = half + 0.5 * inner * (1.0 - bent * bent) * (
        GELU_SCALE * (1.0 + 3.0 * GELU_CUBE * square)
    )
    grad = g_ref[...]
    m_ref[...] = dot(active, wd_ref[...]).astype(BF16)
    dd_ref[...] += left_cross(active, grad)
    grad_inner = right_cross(grad, wd_ref[...]) * slope
    grad_low = grad_inner.astype(BF16)
    du_ref[...] += left_cross(normed, grad_low)
    grad_normed = right_cross(grad_low, wu_ref[...])
    dc_ref[...] = grad_normed.astype(BF16)
    sum_ref[0:1] += jnp.sum(grad_low.astype(F32), axis=0, keepdims=True)
    sum_ref[1:2] += jnp.sum(grad_normed * unit, axis=0, keepdims=True)
    sum_ref[2:3] += jnp.sum(grad_normed, axis=0, keepdims=True)


def middle(count, pieces, tokens_all, grads, w_proj, w_up, w_down, vectors, bias):
    rows, width = tokens_all.shape
    part = pieces[0].shape[1]
    hidden = w_up.shape[1]
    steps = rows // count

    def held(shape):
        return pl.BlockSpec(shape, lambda i: (0, 0))

    def shifted(r):
        return pl.BlockSpec((count, part), lambda i: (jnp.bitwise_xor(i, r), 0))

    block = pl.BlockSpec((count, width), lambda i: (i, 0))
    return pl.pallas_call(
        middle_body,
        grid=(steps,),
        in_specs=[shifted(r) for r in range(4)]
        + [block]
        + [held(v.shape) for v in (*grads, *w_proj, w_up, w_down)]
        + [held(vectors.shape), held(bias.shape)],
        out_specs=[
            held((count, width)),
            block,
            block,
            held((hidden, width)),
            held((width, hidden)),
            held((8, width)),
        ],
        out_shape=[
            jax.ShapeDtypeStruct((count, width), F32),
            jax.ShapeDtypeStruct((rows, width), BF16),
            jax.ShapeDtypeStruct((rows, width), BF16),
            jax.ShapeDtypeStruct((hidden, width), F32),
            jax.ShapeDtypeStruct((width, hidden), F32),
            jax.ShapeDtypeStruct((8, width), F32),
        ],
        cost_estimate=pl.CostEstimate(
            flops=14 * rows * width * hidden,
            bytes_accessed=10 * rows * width + 14 * width * hidden,
            transcendentals=rows * hidden,
        ),
        scratch_shapes=[pltpu.VMEM((count, width), BF16)],
        name="middle",
    )(*pieces, tokens_all, *grads, *w_proj, w_up, w_down, vectors, bias)


def on_device(
    dp_size,
    fs_size,
    tokens,
    cotangent,
    segment_ids,
    valid_mask,
    ln1_gain,
    ln1_bias,
    qkv_weight,
    qkv_bias,
    query_gain,
    query_bias,
    key_gain,
    proj_weight,
    proj_bias,
    ln2_gain,
    ln2_bias,
    fc1_weight,
    fc1_bias,
    fc2_weight,
    fc2_bias,
):
    count, width = tokens.shape
    rank = lax.axis_index("fsdp")
    place = lax.axis_index("dp")
    near = functools.partial(swap, axis="fsdp", size=fs_size, bit=1)
    far = functools.partial(swap, axis="fsdp", size=fs_size, bit=2)
    own_heads = HEADS // fs_size
    part = own_heads * HEAD_DIM
    hidden = fc1_weight.shape[1]
    hidden_own = hidden // fs_size
    rows_own = qkv_weight.shape[0]
    rounds = [1 << i for i in range(dp_size.bit_length() - 1)]

    def gather(value):
        second = far(value)
        return [value, near(value), second, near(second)]

    def spread(pieces):
        return [pieces[0], near(pieces[1]), far(pieces[2]), swap(pieces[3], "fsdp", fs_size, 3)]

    def collect(low):
        low = [low[r * count : (r + 1) * count] for r in range(4)]
        other = near(jnp.concatenate([low[1], low[3]], axis=0)).astype(F32)
        first = low[0].astype(F32) + other[:count]
        sent = (low[2].astype(F32) + other[count:]).astype(BF16)
        return first + far(sent).astype(F32), sent

    def at(r):
        return rank ^ r

    def ordered(pieces, axis):
        chosen = [lax.select_n(at(i), *[pieces[j] for j in range(4)]) for i in range(4)]
        return jnp.concatenate(chosen, axis=axis)

    small = pack(
        (ln1_gain, ln1_bias, ln2_gain, ln2_bias, proj_bias, fc2_bias, qkv_bias)
        + (query_gain, query_bias, key_gain),
        rows_own,
    )
    small_all = ordered([p[:, None] for p in gather(small)], 1).astype(F32)
    wide = small_all[:6].reshape(6, width)
    gain_one, shift_one, gain_two, shift_two, b_proj, b_down = [wide[i] for i in range(6)]
    narrow = query_gain.shape[0]
    gain_query, shift_query, gain_key = [
        small_all[i, :, :narrow].reshape(-1) for i in (9, 10, 11)
    ]
    b_qkv_all = small_all[6:9].transpose(1, 0, 2).reshape(-1)

    def own_columns(matrix, owner):
        return [
            lax.dynamic_slice_in_dim(matrix, block * width + owner * part, part, matrix.ndim - 1)
            for block in range(3)
        ]

    tokens_all = jnp.concatenate(gather(tokens), axis=0)
    w_qkv = ordered(
        spread([jnp.concatenate(own_columns(qkv_weight, at(r)), axis=1) for r in range(4)]), 0
    )

    def after(value, other):
        return lax.optimization_barrier((value, other))[0]

    w_proj_pieces = gather(after(proj_weight, w_qkv))
    up_pieces = [
        lax.dynamic_slice_in_dim(after(fc1_weight, w_qkv), at(r) * hidden_own, hidden_own, 1)
        for r in range(4)
    ]
    up_pieces[1] = near(up_pieces[1])
    up_pieces[2] = far(up_pieces[2])
    up_pieces[3] = swap(up_pieces[3], "fsdp", fs_size, 3)
    w_up = ordered(up_pieces, 0)
    weights_valid = valid_mask.astype(F32)[:, None]
    grad_mlp_own = (cotangent.astype(F32) * weights_valid).astype(BF16)
    grad_mlp_pieces = gather(after(grad_mlp_own, w_qkv))
    ids = jnp.concatenate(
        [lax.dynamic_slice_in_dim(segment_ids, at(r) * count, count) for r in range(4)]
    )

    b_qkv = jnp.concatenate(own_columns(b_qkv_all, rank))
    vectors_one = jnp.concatenate([gain_one[None], shift_one[None]])
    head_vectors = jnp.concatenate([gain_query[None], shift_query[None], gain_key[None]])
    mixed_own, probs, raw, queries, keys, values = front(
        count, tokens_all, w_qkv, vectors_one, b_qkv[None], head_vectors, ids
    )
    vectors = jnp.concatenate([b_proj[None], gain_two[None], shift_two[None]])
    branch_own, mlp_part, grad_two_part, total_down, total_up, sums_middle = middle(
        count, gather(mixed_own), tokens_all, grad_mlp_pieces, w_proj_pieces, w_up, fc2_weight, vectors,
        fc1_bias.astype(F32)[None],
    )
    inputs = tokens.astype(F32)
    hidden_one = inputs + branch_own

    def held_back(other, marks, order):
        return after(other, marks[order]) if order < len(marks) and marks[order] is not None else other

    def halve(total, marks=(), tail=0):
        seen, lead = [], None
        first, second = total[:, : total.shape[1] - tail], total[:, total.shape[1] - tail :]
        for order, bit in enumerate(rounds):
            size = first.shape[1] // 2
            some = second.shape[1] // 2
            low, high = first[:, :size], first[:, size:]
            if tail:
                low = jnp.concatenate([low, second[:, :some]], axis=1)
                high = jnp.concatenate([high, second[:, some:]], axis=1)
            upper = (place & bit) != 0
            sent = jnp.where(upper, low, high).astype(BF16)
            lead = sent if order == 0 else lead
            other = held_back(swap(sent, "dp", dp_size, bit), marks, order)
            seen.append(other)
            total = jnp.where(upper, high, low).astype(F32) + other.astype(F32)
            first, second = total[:, :size], total[:, size:]
        return total, seen, lead

    def unite(share, marks=()):
        share = share.astype(BF16)[None]
        seen = []
        for order, bit in enumerate(reversed(rounds)):
            other = held_back(swap(share, "dp", dp_size, bit), marks, order)
            seen.append(other)
            upper = (place & bit) != 0
            share = jnp.where(
                upper,
                jnp.concatenate([other, share], axis=0),
                jnp.concatenate([share, other], axis=0),
            )
        return share, seen

    def to_rows(share):
        share = share.astype(BF16)
        return spread([lax.dynamic_index_in_dim(share, at(r), 0, False) for r in range(4)])

    grad_normed_two, mark_two = collect(grad_two_part)
    grad_out = grad_mlp_own.astype(F32)
    unit_two, scale_two = norm_parts(hidden_one)
    grad_hidden = grad_out + norm_back(grad_normed_two * gain_two, unit_two, scale_two)
    grad_branch_own = grad_hidden.astype(BF16)
    grad_branch_low = jnp.concatenate(gather(grad_branch_own), axis=0)
    total_proj = left_cross(mixed_own, grad_branch_low)
    own_sums = [sums_middle[1], sums_middle[2], jnp.sum(grad_branch_own.astype(F32), axis=0)]
    own_sums = jnp.stack(own_sums).reshape(3, fs_size, rows_own)
    bias_up = jnp.where(jnp.arange(fs_size)[:, None] == rank, sums_middle[0][None], 0.0)
    bias_down = jnp.sum(grad_out, axis=0).reshape(fs_size, rows_own)
    early_rows = jnp.concatenate(
        [own_sums[0], own_sums[1], own_sums[2], bias_up, bias_down], axis=1
    )
    early_rows = jnp.pad(early_rows, ((0, 0), (0, 9 * part - early_rows.shape[1])))
    early_rows = early_rows.reshape(fs_size, 3, 3 * part)
    total_last, grad_one_part = back(
        count, dp_size, rank, grad_branch_low, proj_weight, probs, raw, queries, keys, values,
        tokens_all, w_qkv, vectors_one, head_vectors, early_rows,
    )
    share_last, seen, lead = halve(total_last, tail=dp_size)
    grad_normed_one, _ = collect(after(grad_one_part, lead))
    unit_one, scale_one = norm_parts(inputs)
    tokens_grad = grad_hidden + norm_back(
        grad_normed_one * gain_one, unit_one, scale_one
    )

    branch_mlp = collect(after(mlp_part, lead))[0] + b_down
    result = hidden_one + branch_mlp
    rms_sums = jnp.stack(
        [
            jnp.sum(weights_valid * result * result),
            jnp.sum(weights_valid * branch_own * branch_own),
            jnp.sum(weights_valid * branch_mlp * branch_mlp),
            jnp.sum(weights_valid),
        ]
    )

    rms_sums = jnp.broadcast_to(rms_sums[:, None], (4, 128))
    for bit in (1, 2):
        rms_sums = rms_sums + swap(rms_sums, "fsdp", fs_size, bit)
    for bit in rounds:
        rms_sums = rms_sums + swap(rms_sums, "dp", dp_size, bit)
    sums = rms_sums[:, 0]

    count_rounds = len(rounds)
    pieces_last = to_rows(share_last)
    share_rows = rows_own // dp_size
    last, seen_back = unite(arrange(share_rows, rank, pieces_last))
    seen = [*seen, pieces_last[3], *seen_back]

    early = [mark_two, grad_branch_own] + [grad_branch_low] * (count_rounds - 2)
    share_down, seen_down, _ = halve(total_down[None], early)
    grad_down, _ = unite(share_down[0], [lead, seen[0], seen[1]])
    grad_down = grad_down.astype(F32).reshape(hidden_own, width)
    total_up = after(total_up, seen_down[0])
    late = [grad_branch_own] + [lead] * (count_rounds - 1)
    share_up, _, _ = halve(total_up.reshape(fs_size, rows_own, hidden_own), late)
    grad_up, _ = unite(ordered(to_rows(share_up), 1), [seen[1], seen[2], seen[count_rounds]])
    grad_up = grad_up.astype(F32).reshape(rows_own, hidden)
    share_proj, _, _ = halve(total_proj[None], seen[:count_rounds])
    grad_proj, _ = unite(share_proj[0], seen[count_rounds:])
    grad_proj = grad_proj.astype(F32).reshape(rows_own, width)
    last = last.astype(F32)
    grad_qkv = last[:, :share_rows].reshape(rows_own, 3 * width)
    table = last[:, share_rows, : 3 * part]
    narrow = HEAD_DIM // fs_size
    flat = table[3:6].reshape(-1)
    finals = [table[0, :rows_own], table[0, rows_own : 2 * rows_own], table[1]]
    finals += [table[2, i * narrow : (i + 1) * narrow] for i in range(3)]
    finals += [flat[2 * rows_own : 3 * rows_own], flat[:rows_own], flat[rows_own : 2 * rows_own]]
    finals += [flat[3 * rows_own : 3 * rows_own + hidden_own]]
    finals += [flat[3 * rows_own + hidden_own : 4 * rows_own + hidden_own]]
    return (
        result.astype(BF16),
        tokens_grad,
        finals[0],
        finals[1],
        grad_qkv,
        finals[2],
        finals[3],
        finals[4],
        finals[5],
        grad_proj,
        finals[6],
        finals[7],
        finals[8],
        grad_up,
        finals[9],
        grad_down,
        finals[10],
        jnp.sqrt(sums[:3] / sums[3]),
    )


def solution(mesh):
    rows = P(("dp", "fsdp"), None)
    vector = P("fsdp")
    matrix = P("fsdp", None)
    device = functools.partial(on_device, mesh.shape["dp"], mesh.shape["fsdp"])

    return jax.shard_map(
        device,
        mesh=mesh,
        in_specs=(
            rows, rows, P("dp"), P(("dp", "fsdp")), vector, vector, matrix, vector, vector, vector,
            vector, matrix, vector, vector, vector, matrix, vector, matrix, vector,
        ),
        out_specs=(
            rows, rows, vector, vector, matrix, vector, vector, vector, vector, matrix, vector,
            vector, vector, matrix, vector, matrix, vector, P(),
        ),
        check_vma=False,
    )
```

```python
import functools

import jax
import jax.numpy as jnp
from jax import lax
from jax.experimental import pallas as pl
from jax.experimental.pallas import tpu as pltpu
from jax.sharding import PartitionSpec as P


HEADS = 12
HEAD_DIM = 64
EPS = 1e-06
MASKED = -1e30
F32 = jnp.float32
BF16 = jnp.bfloat16


def swap(value, axis, size, bit):
    return lax.ppermute(value, axis, [(i, i ^ bit) for i in range(size)])


def dot(first, second):
    return jnp.dot(first, second, preferred_element_type=F32)


def left_cross(first, second):
    return lax.dot_general(first, second, (((0,), (0,)), ((), ())), preferred_element_type=F32)


def right_cross(first, second):
    return lax.dot_general(first, second, (((1,), (1,)), ((), ())), preferred_element_type=F32)


def norm_parts(values):
    average = jnp.mean(values, axis=-1, keepdims=True)
    centred = values - average
    spread = jnp.mean(centred * centred, axis=-1, keepdims=True)
    scale = lax.rsqrt(spread + EPS)
    return centred * scale, scale


def norm_back(grad, unit, scale):
    return scale * (
        grad
        - jnp.mean(grad, axis=-1, keepdims=True)
        - unit * jnp.mean(grad * unit, axis=-1, keepdims=True)
    )


def block_of(step, count):
    return pl.ds(pl.multiple_of(step * count, count), count)


def front_body(
    count, x_ref, w_ref, vec_ref, bias_ref, head_ref, rows_ref, cols_ref,
    o_ref, p_ref, raw_ref, q_ref, k_ref, v_ref,
):
    heads, rows, size = q_ref.shape
    scaling = size**-0.5

    @pl.loop(0, rows // count)
    def _(step):
        at = block_of(step, count)
        unit, _ = norm_parts(x_ref[at].astype(F32))
        normed = (unit * vec_ref[0:1] + vec_ref[1:2]).astype(BF16)
        projected = dot(normed, w_ref[...]) + bias_ref[...]
        for h in range(heads):
            query, key, value = [
                projected[:, (j * heads + h) * size : (j * heads + h + 1) * size] for j in range(3)
            ]
            raw_ref[h, at] = query
            raw_ref[heads + h, at] = key
            unit, _ = norm_parts(query)
            q_ref[h, at] = ((unit * head_ref[0:1] + head_ref[1:2]) * scaling).astype(BF16)
            unit, _ = norm_parts(key)
            k_ref[h, at] = (unit * head_ref[2:3]).astype(BF16)
            v_ref[h, at] = value.astype(BF16)

    for h in range(heads):

        @pl.loop(0, rows // count)
        def _(step):
            at = block_of(step, count)
            scores = right_cross(q_ref[h, at], k_ref[h])
            scores = jnp.where(rows_ref[at] == cols_ref[...], scores, MASKED)
            top = jnp.max(scores, axis=-1, keepdims=True)
            raised = jnp.exp(scores - top)
            total = jnp.sum(raised, axis=-1, keepdims=True)
            probs = (raised * (1.0 / total)).astype(BF16)
            p_ref[h, at] = probs
            o_ref[at, h * size : (h + 1) * size] = dot(probs, v_ref[h]).astype(BF16)


def front(count, tokens_all, w_qkv, vectors, bias, head_vectors, ids):
    rows, width = tokens_all.shape
    size = head_vectors.shape[1]
    part = w_qkv.shape[1] // 3
    heads = part // size
    return pl.pallas_call(
        functools.partial(front_body, count),
        out_shape=[
            jax.ShapeDtypeStruct((rows, part), BF16),
            jax.ShapeDtypeStruct((heads, rows, rows), BF16),
            jax.ShapeDtypeStruct((2 * heads, rows, size), F32),
            jax.ShapeDtypeStruct((heads, rows, size), BF16),
            jax.ShapeDtypeStruct((heads, rows, size), BF16),
            jax.ShapeDtypeStruct((heads, rows, size), BF16),
        ],
        cost_estimate=pl.CostEstimate(
            flops=6 * rows * width * part + 4 * heads * rows * rows * size,
            bytes_accessed=2 * rows * (width + heads * rows + 8 * part) + 6 * width * part,
            transcendentals=heads * rows * rows,
        ),
        name="front",
    )(tokens_all, w_qkv, vectors, bias, head_vectors, ids[:, None], ids[None, :])


def back_body(
    count, rank_ref, z_ref, wp_ref, p_ref, raw_ref, q_ref, k_ref, v_ref, x_ref, w_ref, vec_ref,
    head_ref, early_ref, out_ref, da_ref, sum_ref, bias_ref, heads_ref, dw_ref, g_ref, dk_ref,
    dv_ref, dq_ref, dkt_ref, dvt_ref,
):
    heads, rows, size = q_ref.shape
    scaling = size**-0.5
    steps = rows // count
    sum_ref[...] = jnp.zeros_like(sum_ref)
    bias_ref[...] = jnp.zeros_like(bias_ref)
    heads_ref[...] = jnp.zeros_like(heads_ref)
    dw_ref[...] = jnp.zeros_like(dw_ref)
    for h in range(heads):
        dk_ref[...] = jnp.zeros_like(dk_ref)
        dv_ref[...] = jnp.zeros_like(dv_ref)

        @pl.loop(0, steps)
        def _(step):
            at = block_of(step, count)
            grad = right_cross(z_ref[at], wp_ref[h * size : (h + 1) * size]).astype(BF16)
            low = p_ref[h, at]
            probs = low.astype(F32)
            grad_probs = right_cross(grad, v_ref[h])
            delta = jnp.sum(probs * grad_probs, axis=-1, keepdims=True)
            grad_scores = (probs * (grad_probs - delta)).astype(BF16)
            dq_ref[at] = dot(grad_scores, k_ref[h])
            dk_ref[...] += left_cross(q_ref[h, at], grad_scores)
            dv_ref[...] += left_cross(grad, low)

        dkt_ref[...] = dk_ref[...].T
        dvt_ref[...] = dv_ref[...].T

        @pl.loop(0, steps)
        def _(step):
            at = block_of(step, count)
            grad = dq_ref[at] * scaling
            unit, scale = norm_parts(raw_ref[h, at])
            heads_ref[0:1] += jnp.sum(grad * unit, axis=0, keepdims=True)
            heads_ref[1:2] += jnp.sum(grad, axis=0, keepdims=True)
            g_ref[at, h * size : (h + 1) * size] = norm_back(
                grad * head_ref[0:1], unit, scale
            ).astype(BF16)
            grad = dkt_ref[at]
            unit, scale = norm_parts(raw_ref[heads + h, at])
            heads_ref[2:3] += jnp.sum(grad * unit, axis=0, keepdims=True)
            first = (heads + h) * size
            g_ref[at, first : first + size] = norm_back(grad * head_ref[2:3], unit, scale).astype(
                BF16
            )
            first = (2 * heads + h) * size
            g_ref[at, first : first + size] = dvt_ref[at].astype(BF16)

    @pl.loop(0, steps)
    def _(step):
        at = block_of(step, count)
        unit, _ = norm_parts(x_ref[at].astype(F32))
        normed = (unit * vec_ref[0:1] + vec_ref[1:2]).astype(BF16)
        grad = g_ref[at]
        dw_ref[...] += left_cross(normed, grad)
        bias_ref[0:1] += jnp.sum(grad.astype(F32), axis=0, keepdims=True)
        grad_normed = right_cross(grad, w_ref[...])
        da_ref[at] = grad_normed.astype(BF16)
        sum_ref[0:1] += jnp.sum(grad_normed * unit, axis=0, keepdims=True)
        sum_ref[1:2] += jnp.sum(grad_normed, axis=0, keepdims=True)


    owners, total_rows, columns = out_ref.shape
    own = dw_ref.shape[0] // owners
    part = columns // 3
    rank = rank_ref[0]
    narrow = size // owners
    for o in range(owners):
        out_ref[o, :own] = dw_ref[o * own : (o + 1) * own]
        first = jnp.concatenate(
            [sum_ref[i : i + 1, o * own : (o + 1) * own] for i in range(2)]
            + [jnp.zeros((1, columns - 2 * own), F32)],
            axis=1,
        )
        groups = []
        for j in range(3):
            group = 3 * o + j
            value = bias_ref[0:1, group // owners * part : (group // owners + 1) * part]
            groups.append(jnp.where(rank == group % owners, value, 0.0))
        gains = [heads_ref[i : i + 1, o * narrow : (o + 1) * narrow] for i in range(3)]
        third = jnp.concatenate([*gains, jnp.zeros((1, columns - 3 * narrow), F32)], axis=1)
        out_ref[o, own:] = jnp.concatenate(
            [first, jnp.concatenate(groups, axis=1), third, early_ref[o]]
            + [jnp.zeros((total_rows - own - 3 - early_ref.shape[1], columns), F32)],
            axis=0,
        )


def back(count, extra, rank, *values):
    _, _, _, _, queries, _, _, tokens_all, _, _, _, early = values
    rows, width = tokens_all.shape
    heads, _, size = queries.shape
    part = heads * size
    owners = early.shape[0]
    vmem = pl.BlockSpec(memory_space=pltpu.VMEM)
    return pl.pallas_call(
        functools.partial(back_body, count),
        in_specs=[pl.BlockSpec(memory_space=pltpu.SMEM)] + [vmem] * len(values),
        out_specs=[vmem, vmem],
        out_shape=[
            jax.ShapeDtypeStruct((owners, width // owners + extra, 3 * part), F32),
            jax.ShapeDtypeStruct((rows, width), BF16),
        ],
        scratch_shapes=[
            pltpu.VMEM((8, width), F32),
            pltpu.VMEM((8, 3 * part), F32),
            pltpu.VMEM((8, size), F32),
            pltpu.VMEM((width, 3 * part), F32),
            pltpu.VMEM((rows, 3 * part), BF16),
            pltpu.VMEM((size, rows), F32),
            pltpu.VMEM((size, rows), F32),
            pltpu.VMEM((rows, size), F32),
            pltpu.VMEM((rows, size), F32),
            pltpu.VMEM((rows, size), F32),
        ],
        cost_estimate=pl.CostEstimate(
            flops=14 * rows * width * part + 8 * heads * rows * rows * size,
            bytes_accessed=2 * rows * (3 * width + heads * rows + 12 * part) + 18 * width * part,
            transcendentals=0,
        ),
        name="back",
    )(rank[None], *values)


def pack_body(*refs):
    out = refs[-1]
    columns = out.shape[1]
    rows = []
    for ref in refs[:-1]:
        value = ref[...].astype(F32)[None]
        size = value.shape[1]
        if size < columns:
            rows.append(jnp.concatenate([value, jnp.zeros((1, columns - size), F32)], axis=1))
        else:
            rows += [value[:, i : i + columns] for i in range(0, size, columns)]
    rows.append(jnp.zeros((out.shape[0] - len(rows), columns), F32))
    out[...] = jnp.concatenate(rows, axis=0).astype(BF16)


def pack(vectors, columns):
    return pl.pallas_call(
        pack_body, out_shape=jax.ShapeDtypeStruct((16, columns), BF16), name="pack"
    )(*vectors)


def arrange_body(share_rows, rank_ref, p0, p1, p2, p3, o_ref):
    pieces = [p[...].astype(F32) for p in (p0, p1, p2, p3)]
    part = pieces[0].shape[1] // 3
    low, high = (rank_ref[0] & 1) == 1, (rank_ref[0] & 2) == 2
    pairs = [
        (jnp.where(low, a, b), jnp.where(low, b, a))
        for a, b in ((pieces[1], pieces[0]), (pieces[3], pieces[2]))
    ]
    total = (pieces[0] + pieces[1]) + (pieces[2] + pieces[3])
    chosen = [jnp.where(high, pairs[1][i], pairs[0][i]) for i in range(2)]
    chosen += [jnp.where(high, pairs[0][i], pairs[1][i]) for i in range(2)]
    placed = jnp.concatenate(
        [c[:, j * part : (j + 1) * part] for j in range(3) for c in chosen], axis=1
    )
    wide = jnp.concatenate([total] * 4, axis=1)
    row = lax.broadcasted_iota(jnp.int32, placed.shape, 0)
    o_ref[...] = jnp.where(row < share_rows, placed, wide).astype(BF16)


def arrange(share_rows, rank, pieces):
    rows, columns = pieces[0].shape
    vmem = pl.BlockSpec(memory_space=pltpu.VMEM)
    return pl.pallas_call(
        functools.partial(arrange_body, share_rows),
        in_specs=[pl.BlockSpec(memory_space=pltpu.SMEM)] + [vmem] * 4,
        out_specs=vmem,
        out_shape=jax.ShapeDtypeStruct((rows, 4 * columns), BF16),
        name="arrange",
    )(rank[None], *pieces)


GELU_SCALE = 0.7978845608028654
GELU_CUBE = 0.044715


def middle_body(
    m0, m1, m2, m3, x_ref, g0, g1, g2, g3, w0, w1, w2, w3, wu_ref, wd_ref, vec_ref, bias_ref,
    z_ref, m_ref, dc_ref, dd_ref, du_ref, sum_ref, g_ref,
):
    step = pl.program_id(0)

    @pl.when(step == 0)
    def _():
        dd_ref[...] = jnp.zeros_like(dd_ref)
        du_ref[...] = jnp.zeros_like(du_ref)
        sum_ref[...] = jnp.zeros_like(sum_ref)

    for r, piece in enumerate((g0, g1, g2, g3)):

        @pl.when(step == r)
        def _(piece=piece):
            g_ref[...] = piece[...]

    branch = vec_ref[0:1]
    for piece, weight in zip((m0, m1, m2, m3), (w0, w1, w2, w3)):
        branch = branch + dot(piece[...], weight[...])

    @pl.when(step == 0)
    def _():
        z_ref[...] = branch

    unit, _ = norm_parts(x_ref[...].astype(F32) + branch)
    normed = (unit * vec_ref[1:2] + vec_ref[2:3]).astype(BF16)
    inner = dot(normed, wu_ref[...]) + bias_ref[...]
    square = inner * inner
    bent = jnp.tanh(GELU_SCALE * (inner + GELU_CUBE * inner * square))
    half = 0.5 * (1.0 + bent)
    active = (inner * half).astype(BF16)
    slope = half + 0.5 * inner * (1.0 - bent * bent) * (
        GELU_SCALE * (1.0 + 3.0 * GELU_CUBE * square)
    )
    grad = g_ref[...]
    m_ref[...] = dot(active, wd_ref[...]).astype(BF16)
    dd_ref[...] += left_cross(active, grad)
    grad_inner = right_cross(grad, wd_ref[...]) * slope
    grad_low = grad_inner.astype(BF16)
    du_ref[...] += left_cross(normed, grad_low)
    grad_normed = right_cross(grad_low, wu_ref[...])
    dc_ref[...] = grad_normed.astype(BF16)
    sum_ref[0:1] += jnp.sum(grad_low.astype(F32), axis=0, keepdims=True)
    sum_ref[1:2] += jnp.sum(grad_normed * unit, axis=0, keepdims=True)
    sum_ref[2:3] += jnp.sum(grad_normed, axis=0, keepdims=True)


def middle(count, pieces, tokens_all, grads, w_proj, w_up, w_down, vectors, bias):
    rows, width = tokens_all.shape
    part = pieces[0].shape[1]
    hidden = w_up.shape[1]
    steps = rows // count

    def held(shape):
        return pl.BlockSpec(shape, lambda i: (0, 0))

    def shifted(r):
        return pl.BlockSpec((count, part), lambda i: (jnp.bitwise_xor(i, r), 0))

    block = pl.BlockSpec((count, width), lambda i: (i, 0))
    return pl.pallas_call(
        middle_body,
        grid=(steps,),
        in_specs=[shifted(r) for r in range(4)]
        + [block]
        + [held(v.shape) for v in (*grads, *w_proj, w_up, w_down)]
        + [held(vectors.shape), held(bias.shape)],
        out_specs=[
            held((count, width)),
            block,
            block,
            held((hidden, width)),
            held((width, hidden)),
            held((8, width)),
        ],
        out_shape=[
            jax.ShapeDtypeStruct((count, width), F32),
            jax.ShapeDtypeStruct((rows, width), BF16),
            jax.ShapeDtypeStruct((rows, width), BF16),
            jax.ShapeDtypeStruct((hidden, width), F32),
            jax.ShapeDtypeStruct((width, hidden), F32),
            jax.ShapeDtypeStruct((8, width), F32),
        ],
        cost_estimate=pl.CostEstimate(
            flops=14 * rows * width * hidden,
            bytes_accessed=10 * rows * width + 14 * width * hidden,
            transcendentals=rows * hidden,
        ),
        scratch_shapes=[pltpu.VMEM((count, width), BF16)],
        name="middle",
    )(*pieces, tokens_all, *grads, *w_proj, w_up, w_down, vectors, bias)


def on_device(
    dp_size,
    fs_size,
    tokens,
    cotangent,
    segment_ids,
    valid_mask,
    ln1_gain,
    ln1_bias,
    qkv_weight,
    qkv_bias,
    query_gain,
    query_bias,
    key_gain,
    proj_weight,
    proj_bias,
    ln2_gain,
    ln2_bias,
    fc1_weight,
    fc1_bias,
    fc2_weight,
    fc2_bias,
):
    count, width = tokens.shape
    rank = lax.axis_index("fsdp")
    place = lax.axis_index("dp")
    near = functools.partial(swap, axis="fsdp", size=fs_size, bit=1)
    far = functools.partial(swap, axis="fsdp", size=fs_size, bit=2)
    own_heads = HEADS // fs_size
    part = own_heads * HEAD_DIM
    hidden = fc1_weight.shape[1]
    hidden_own = hidden // fs_size
    rows_own = qkv_weight.shape[0]
    rounds = [1 << i for i in range(dp_size.bit_length() - 1)]

    def gather(value):
        second = far(value)
        return [value, near(value), second, near(second)]

    def spread(pieces):
        return [pieces[0], near(pieces[1]), far(pieces[2]), swap(pieces[3], "fsdp", fs_size, 3)]

    def collect(low, mark=None):
        low = [low[r * count : (r + 1) * count] for r in range(4)]
        other = near(jnp.concatenate([low[1], low[3]], axis=0)).astype(F32)
        first = low[0].astype(F32) + other[:count]
        sent = (low[2].astype(F32) + other[count:]).astype(BF16)
        sent = sent if mark is None else after(sent, mark)
        return first + far(sent).astype(F32), sent

    def at(r):
        return rank ^ r

    def ordered(pieces, axis):
        chosen = [lax.select_n(at(i), *[pieces[j] for j in range(4)]) for i in range(4)]
        return jnp.concatenate(chosen, axis=axis)

    small = pack(
        (ln1_gain, ln1_bias, ln2_gain, ln2_bias, proj_bias, fc2_bias, qkv_bias)
        + (query_gain, query_bias, key_gain),
        rows_own,
    )
    small_all = ordered([p[:, None] for p in gather(small)], 1).astype(F32)
    wide = small_all[:6].reshape(6, width)
    gain_one, shift_one, gain_two, shift_two, b_proj, b_down = [wide[i] for i in range(6)]
    narrow = query_gain.shape[0]
    gain_query, shift_query, gain_key = [
        small_all[i, :, :narrow].reshape(-1) for i in (9, 10, 11)
    ]
    b_qkv_all = small_all[6:9].transpose(1, 0, 2).reshape(-1)

    def own_columns(matrix, owner):
        return [
            lax.dynamic_slice_in_dim(matrix, block * width + owner * part, part, matrix.ndim - 1)
            for block in range(3)
        ]

    tokens_all = jnp.concatenate(gather(tokens), axis=0)
    w_qkv = ordered(
        spread([jnp.concatenate(own_columns(qkv_weight, at(r)), axis=1) for r in range(4)]), 0
    )

    def after(value, other):
        return lax.optimization_barrier((value, other))[0]

    w_proj_pieces = gather(after(proj_weight, w_qkv))
    up_pieces = [
        lax.dynamic_slice_in_dim(after(fc1_weight, w_qkv), at(r) * hidden_own, hidden_own, 1)
        for r in range(4)
    ]
    up_pieces[1] = near(up_pieces[1])
    up_pieces[2] = far(up_pieces[2])
    up_pieces[3] = swap(up_pieces[3], "fsdp", fs_size, 3)
    w_up = ordered(up_pieces, 0)
    weights_valid = valid_mask.astype(F32)[:, None]
    grad_mlp_own = (cotangent.astype(F32) * weights_valid).astype(BF16)
    grad_mlp_pieces = gather(after(grad_mlp_own, w_qkv))
    ids = jnp.concatenate(
        [lax.dynamic_slice_in_dim(segment_ids, at(r) * count, count) for r in range(4)]
    )

    b_qkv = jnp.concatenate(own_columns(b_qkv_all, rank))
    vectors_one = jnp.concatenate([gain_one[None], shift_one[None]])
    head_vectors = jnp.concatenate([gain_query[None], shift_query[None], gain_key[None]])
    mixed_own, probs, raw, queries, keys, values = front(
        count, tokens_all, w_qkv, vectors_one, b_qkv[None], head_vectors, ids
    )
    vectors = jnp.concatenate([b_proj[None], gain_two[None], shift_two[None]])
    mixed_pieces = gather(mixed_own)
    branch_own, mlp_part, grad_two_part, total_down, total_up, sums_middle = middle(
        count, mixed_pieces, tokens_all, grad_mlp_pieces, w_proj_pieces, w_up, fc2_weight, vectors,
        fc1_bias.astype(F32)[None],
    )
    inputs = tokens.astype(F32)
    hidden_one = inputs + branch_own

    def held_back(other, marks, order):
        return after(other, marks[order]) if order < len(marks) and marks[order] is not None else other

    def halve(total, marks=(), tail=0):
        seen, lead = [], None
        first, second = total[:, : total.shape[1] - tail], total[:, total.shape[1] - tail :]
        for order, bit in enumerate(rounds):
            size = first.shape[1] // 2
            some = second.shape[1] // 2
            low, high = first[:, :size], first[:, size:]
            if tail:
                low = jnp.concatenate([low, second[:, :some]], axis=1)
                high = jnp.concatenate([high, second[:, some:]], axis=1)
            upper = (place & bit) != 0
            sent = jnp.where(upper, low, high).astype(BF16)
            lead = sent if order == 0 else lead
            other = held_back(swap(sent, "dp", dp_size, bit), marks, order)
            seen.append(other)
            total = jnp.where(upper, high, low).astype(F32) + other.astype(F32)
            first, second = total[:, :size], total[:, size:]
        return total, seen, lead

    def unite(share, marks=()):
        share = share.astype(BF16)[None]
        seen = []
        for order, bit in enumerate(reversed(rounds)):
            other = held_back(swap(share, "dp", dp_size, bit), marks, order)
            seen.append(other)
            upper = (place & bit) != 0
            share = jnp.where(
                upper,
                jnp.concatenate([other, share], axis=0),
                jnp.concatenate([share, other], axis=0),
            )
        return share, seen

    def to_rows(share):
        share = share.astype(BF16)
        return spread([lax.dynamic_index_in_dim(share, at(r), 0, False) for r in range(4)])

    grad_normed_two, mark_two = collect(grad_two_part)
    grad_out = grad_mlp_own.astype(F32)
    unit_two, scale_two = norm_parts(hidden_one)
    grad_hidden = grad_out + norm_back(grad_normed_two * gain_two, unit_two, scale_two)
    grad_branch_own = grad_hidden.astype(BF16)
    grad_branch_low = jnp.concatenate(gather(grad_branch_own), axis=0)
    total_proj = left_cross(mixed_own, grad_branch_low)
    branch_mlp = collect(mlp_part, grad_normed_two)[0] + b_down
    result = hidden_one + branch_mlp
    rms_sums = jnp.stack(
        [
            jnp.sum(weights_valid * result * result),
            jnp.sum(weights_valid * branch_own * branch_own),
            jnp.sum(weights_valid * branch_mlp * branch_mlp),
            jnp.sum(weights_valid),
        ]
    )

    own_sums = [sums_middle[1], sums_middle[2], jnp.sum(grad_branch_own.astype(F32), axis=0)]
    own_sums = jnp.stack(own_sums).reshape(3, fs_size, rows_own)
    bias_up = jnp.where(jnp.arange(fs_size)[:, None] == rank, sums_middle[0][None], 0.0)
    bias_down = jnp.sum(grad_out, axis=0).reshape(fs_size, rows_own)
    early_rows = jnp.concatenate(
        [own_sums[0], own_sums[1], own_sums[2], bias_up, bias_down]
        + [jnp.broadcast_to(rms_sums[None], (fs_size, 4))],
        axis=1,
    )
    early_rows = jnp.pad(early_rows, ((0, 0), (0, 9 * part - early_rows.shape[1])))
    early_rows = early_rows.reshape(fs_size, 3, 3 * part)
    total_last, grad_one_part = back(
        count, dp_size, rank, grad_branch_low, proj_weight, probs, raw, queries, keys, values,
        tokens_all, w_qkv, vectors_one, head_vectors, early_rows,
    )
    share_last, seen, lead = halve(total_last, tail=dp_size)
    grad_normed_one, _ = collect(after(grad_one_part, lead))
    unit_one, scale_one = norm_parts(inputs)
    tokens_grad = grad_hidden + norm_back(
        grad_normed_one * gain_one, unit_one, scale_one
    )

    count_rounds = len(rounds)
    pieces_last = to_rows(share_last)
    share_rows = rows_own // dp_size
    last, seen_back = unite(arrange(share_rows, rank, pieces_last))
    seen = [*seen, pieces_last[3], *seen_back]

    early = [mark_two, grad_branch_own] + [grad_branch_low] * (count_rounds - 2)
    share_down, seen_down, _ = halve(total_down[None], early)
    grad_down, _ = unite(share_down[0], [lead, seen[0], seen[1]])
    grad_down = grad_down.astype(F32).reshape(hidden_own, width)
    total_up = after(total_up, seen_down[0])
    late = [grad_branch_own] + [lead] * (count_rounds - 1)
    share_up, _, _ = halve(total_up.reshape(fs_size, rows_own, hidden_own), late)
    grad_up, _ = unite(ordered(to_rows(share_up), 1), [seen[1], seen[2], seen[count_rounds]])
    grad_up = grad_up.astype(F32).reshape(rows_own, hidden)
    share_proj, _, _ = halve(total_proj[None], seen[:count_rounds])
    grad_proj, _ = unite(share_proj[0], seen[count_rounds:])
    grad_proj = grad_proj.astype(F32).reshape(rows_own, width)
    last = last.astype(F32)
    grad_qkv = last[:, :share_rows].reshape(rows_own, 3 * width)
    table = last[:, share_rows, : 3 * part]
    narrow = HEAD_DIM // fs_size
    flat = table[3:6].reshape(-1)
    finals = [table[0, :rows_own], table[0, rows_own : 2 * rows_own], table[1]]
    finals += [table[2, i * narrow : (i + 1) * narrow] for i in range(3)]
    finals += [flat[2 * rows_own : 3 * rows_own], flat[:rows_own], flat[rows_own : 2 * rows_own]]
    finals += [flat[3 * rows_own : 3 * rows_own + hidden_own]]
    finals += [flat[3 * rows_own + hidden_own : 4 * rows_own + hidden_own]]
    sums = flat[4 * rows_own + hidden_own :]
    return (
        result.astype(BF16),
        tokens_grad,
        finals[0],
        finals[1],
        grad_qkv,
        finals[2],
        finals[3],
        finals[4],
        finals[5],
        grad_proj,
        finals[6],
        finals[7],
        finals[8],
        grad_up,
        finals[9],
        grad_down,
        finals[10],
        jnp.sqrt(sums[:3] / sums[3]),
    )


def solution(mesh):
    rows = P(("dp", "fsdp"), None)
    vector = P("fsdp")
    matrix = P("fsdp", None)
    device = functools.partial(on_device, mesh.shape["dp"], mesh.shape["fsdp"])

    return jax.shard_map(
        device,
        mesh=mesh,
        in_specs=(
            rows, rows, P("dp"), P(("dp", "fsdp")), vector, vector, matrix, vector, vector, vector,
            vector, matrix, vector, vector, vector, matrix, vector, matrix, vector,
        ),
        out_specs=(
            rows, rows, vector, vector, matrix, vector, vector, vector, vector, matrix, vector,
            vector, vector, matrix, vector, matrix, vector, P(),
        ),
        check_vma=False,
    )
```

```python
import functools

import jax
import jax.numpy as jnp
from jax import lax
from jax.experimental import pallas as pl
from jax.experimental.pallas import tpu as pltpu
from jax.sharding import PartitionSpec as P


HEADS = 12
HEAD_DIM = 64
EPS = 1e-06
MASKED = -1e30
F32 = jnp.float32
BF16 = jnp.bfloat16


def swap(value, axis, size, bit):
    return lax.ppermute(value, axis, [(i, i ^ bit) for i in range(size)])


def dot(first, second):
    return jnp.dot(first, second, preferred_element_type=F32)


def left_cross(first, second):
    return lax.dot_general(first, second, (((0,), (0,)), ((), ())), preferred_element_type=F32)


def right_cross(first, second):
    return lax.dot_general(first, second, (((1,), (1,)), ((), ())), preferred_element_type=F32)


def norm_parts(values):
    average = jnp.mean(values, axis=-1, keepdims=True)
    centred = values - average
    spread = jnp.mean(centred * centred, axis=-1, keepdims=True)
    scale = lax.rsqrt(spread + EPS)
    return centred * scale, scale


def norm_back(grad, unit, scale):
    return scale * (
        grad
        - jnp.mean(grad, axis=-1, keepdims=True)
        - unit * jnp.mean(grad * unit, axis=-1, keepdims=True)
    )


def block_of(step, count):
    return pl.ds(pl.multiple_of(step * count, count), count)


def front_body(
    count, x_ref, w_ref, vec_ref, bias_ref, head_ref, rows_ref, cols_ref,
    o_ref, p_ref, raw_ref, q_ref, k_ref, v_ref,
):
    heads, rows, size = q_ref.shape
    scaling = size**-0.5

    @pl.loop(0, rows // count)
    def _(step):
        at = block_of(step, count)
        unit, _ = norm_parts(x_ref[at].astype(F32))
        normed = (unit * vec_ref[0:1] + vec_ref[1:2]).astype(BF16)
        projected = dot(normed, w_ref[...]) + bias_ref[...]
        for h in range(heads):
            query, key, value = [
                projected[:, (j * heads + h) * size : (j * heads + h + 1) * size] for j in range(3)
            ]
            raw_ref[h, at] = query
            raw_ref[heads + h, at] = key
            unit, _ = norm_parts(query)
            q_ref[h, at] = ((unit * head_ref[0:1] + head_ref[1:2]) * scaling).astype(BF16)
            unit, _ = norm_parts(key)
            k_ref[h, at] = (unit * head_ref[2:3]).astype(BF16)
            v_ref[h, at] = value.astype(BF16)

    for h in range(heads):

        @pl.loop(0, rows // count)
        def _(step):
            at = block_of(step, count)
            scores = right_cross(q_ref[h, at], k_ref[h])
            scores = jnp.where(rows_ref[at] == cols_ref[...], scores, MASKED)
            top = jnp.max(scores, axis=-1, keepdims=True)
            raised = jnp.exp(scores - top)
            total = jnp.sum(raised, axis=-1, keepdims=True)
            probs = (raised * (1.0 / total)).astype(BF16)
            p_ref[h, at] = probs
            o_ref[at, h * size : (h + 1) * size] = dot(probs, v_ref[h]).astype(BF16)


def front(count, tokens_all, w_qkv, vectors, bias, head_vectors, ids):
    rows, width = tokens_all.shape
    size = head_vectors.shape[1]
    part = w_qkv.shape[1] // 3
    heads = part // size
    return pl.pallas_call(
        functools.partial(front_body, count),
        out_shape=[
            jax.ShapeDtypeStruct((rows, part), BF16),
            jax.ShapeDtypeStruct((heads, rows, rows), BF16),
            jax.ShapeDtypeStruct((2 * heads, rows, size), F32),
            jax.ShapeDtypeStruct((heads, rows, size), BF16),
            jax.ShapeDtypeStruct((heads, rows, size), BF16),
            jax.ShapeDtypeStruct((heads, rows, size), BF16),
        ],
        cost_estimate=pl.CostEstimate(
            flops=6 * rows * width * part + 4 * heads * rows * rows * size,
            bytes_accessed=2 * rows * (width + heads * rows + 8 * part) + 6 * width * part,
            transcendentals=heads * rows * rows,
        ),
        name="front",
    )(tokens_all, w_qkv, vectors, bias, head_vectors, ids[:, None], ids[None, :])


def back_body(
    count, rank_ref, z_ref, wp_ref, p_ref, raw_ref, q_ref, k_ref, v_ref, x_ref, w_ref, vec_ref,
    head_ref, early_ref, out_ref, da_ref, sum_ref, bias_ref, heads_ref, dw_ref, g_ref, dk_ref,
    dv_ref, dq_ref, dkt_ref, dvt_ref,
):
    heads, rows, size = q_ref.shape
    scaling = size**-0.5
    steps = rows // count
    sum_ref[...] = jnp.zeros_like(sum_ref)
    bias_ref[...] = jnp.zeros_like(bias_ref)
    heads_ref[...] = jnp.zeros_like(heads_ref)
    dw_ref[...] = jnp.zeros_like(dw_ref)
    for h in range(heads):
        dk_ref[...] = jnp.zeros_like(dk_ref)
        dv_ref[...] = jnp.zeros_like(dv_ref)

        @pl.loop(0, steps)
        def _(step):
            at = block_of(step, count)
            grad = right_cross(z_ref[at], wp_ref[h * size : (h + 1) * size]).astype(BF16)
            low = p_ref[h, at]
            probs = low.astype(F32)
            grad_probs = right_cross(grad, v_ref[h])
            delta = jnp.sum(probs * grad_probs, axis=-1, keepdims=True)
            grad_scores = (probs * (grad_probs - delta)).astype(BF16)
            dq_ref[at] = dot(grad_scores, k_ref[h])
            dk_ref[...] += left_cross(q_ref[h, at], grad_scores)
            dv_ref[...] += left_cross(grad, low)

        dkt_ref[...] = dk_ref[...].T
        dvt_ref[...] = dv_ref[...].T

        @pl.loop(0, steps)
        def _(step):
            at = block_of(step, count)
            grad = dq_ref[at] * scaling
            unit, scale = norm_parts(raw_ref[h, at])
            heads_ref[0:1] += jnp.sum(grad * unit, axis=0, keepdims=True)
            heads_ref[1:2] += jnp.sum(grad, axis=0, keepdims=True)
            g_ref[at, h * size : (h + 1) * size] = norm_back(
                grad * head_ref[0:1], unit, scale
            ).astype(BF16)
            grad = dkt_ref[at]
            unit, scale = norm_parts(raw_ref[heads + h, at])
            heads_ref[2:3] += jnp.sum(grad * unit, axis=0, keepdims=True)
            first = (heads + h) * size
            g_ref[at, first : first + size] = norm_back(grad * head_ref[2:3], unit, scale).astype(
                BF16
            )
            first = (2 * heads + h) * size
            g_ref[at, first : first + size] = dvt_ref[at].astype(BF16)

    @pl.loop(0, steps)
    def _(step):
        at = block_of(step, count)
        unit, _ = norm_parts(x_ref[at].astype(F32))
        normed = (unit * vec_ref[0:1] + vec_ref[1:2]).astype(BF16)
        grad = g_ref[at]
        dw_ref[...] += left_cross(normed, grad)
        bias_ref[0:1] += jnp.sum(grad.astype(F32), axis=0, keepdims=True)
        grad_normed = right_cross(grad, w_ref[...])
        da_ref[at] = grad_normed.astype(BF16)
        sum_ref[0:1] += jnp.sum(grad_normed * unit, axis=0, keepdims=True)
        sum_ref[1:2] += jnp.sum(grad_normed, axis=0, keepdims=True)


    owners, total_rows, columns = out_ref.shape
    own = dw_ref.shape[0] // owners
    part = columns // 3
    rank = rank_ref[0]
    narrow = size // owners
    for o in range(owners):
        out_ref[o, :own] = dw_ref[o * own : (o + 1) * own]
        first = jnp.concatenate(
            [sum_ref[i : i + 1, o * own : (o + 1) * own] for i in range(2)]
            + [jnp.zeros((1, columns - 2 * own), F32)],
            axis=1,
        )
        groups = []
        for j in range(3):
            group = 3 * o + j
            value = bias_ref[0:1, group // owners * part : (group // owners + 1) * part]
            groups.append(jnp.where(rank == group % owners, value, 0.0))
        gains = [heads_ref[i : i + 1, o * narrow : (o + 1) * narrow] for i in range(3)]
        third = jnp.concatenate([*gains, jnp.zeros((1, columns - 3 * narrow), F32)], axis=1)
        out_ref[o, own:] = jnp.concatenate(
            [first, jnp.concatenate(groups, axis=1), third, early_ref[o]]
            + [jnp.zeros((total_rows - own - 3 - early_ref.shape[1], columns), F32)],
            axis=0,
        )


def back(count, extra, rank, *values):
    _, _, _, _, queries, _, _, tokens_all, _, _, _, early = values
    rows, width = tokens_all.shape
    heads, _, size = queries.shape
    part = heads * size
    owners = early.shape[0]
    vmem = pl.BlockSpec(memory_space=pltpu.VMEM)
    return pl.pallas_call(
        functools.partial(back_body, count),
        in_specs=[pl.BlockSpec(memory_space=pltpu.SMEM)] + [vmem] * len(values),
        out_specs=[vmem, vmem],
        out_shape=[
            jax.ShapeDtypeStruct((owners, width // owners + extra, 3 * part), F32),
            jax.ShapeDtypeStruct((rows, width), BF16),
        ],
        scratch_shapes=[
            pltpu.VMEM((8, width), F32),
            pltpu.VMEM((8, 3 * part), F32),
            pltpu.VMEM((8, size), F32),
            pltpu.VMEM((width, 3 * part), F32),
            pltpu.VMEM((rows, 3 * part), BF16),
            pltpu.VMEM((size, rows), F32),
            pltpu.VMEM((size, rows), F32),
            pltpu.VMEM((rows, size), F32),
            pltpu.VMEM((rows, size), F32),
            pltpu.VMEM((rows, size), F32),
        ],
        cost_estimate=pl.CostEstimate(
            flops=14 * rows * width * part + 8 * heads * rows * rows * size,
            bytes_accessed=2 * rows * (3 * width + heads * rows + 12 * part) + 18 * width * part,
            transcendentals=0,
        ),
        name="back",
    )(rank[None], *values)


def pack_body(*refs):
    out = refs[-1]
    columns = out.shape[1]
    rows = []
    for ref in refs[:-1]:
        value = ref[...].astype(F32)[None]
        size = value.shape[1]
        if size < columns:
            rows.append(jnp.concatenate([value, jnp.zeros((1, columns - size), F32)], axis=1))
        else:
            rows += [value[:, i : i + columns] for i in range(0, size, columns)]
    rows.append(jnp.zeros((out.shape[0] - len(rows), columns), F32))
    out[...] = jnp.concatenate(rows, axis=0).astype(BF16)


def pack(vectors, columns):
    return pl.pallas_call(
        pack_body, out_shape=jax.ShapeDtypeStruct((16, columns), BF16), name="pack"
    )(*vectors)


def arrange_body(share_rows, rank_ref, p0, p1, p2, p3, o_ref):
    pieces = [p[...].astype(F32) for p in (p0, p1, p2, p3)]
    part = pieces[0].shape[1] // 3
    low, high = (rank_ref[0] & 1) == 1, (rank_ref[0] & 2) == 2
    pairs = [
        (jnp.where(low, a, b), jnp.where(low, b, a))
        for a, b in ((pieces[1], pieces[0]), (pieces[3], pieces[2]))
    ]
    total = (pieces[0] + pieces[1]) + (pieces[2] + pieces[3])
    chosen = [jnp.where(high, pairs[1][i], pairs[0][i]) for i in range(2)]
    chosen += [jnp.where(high, pairs[0][i], pairs[1][i]) for i in range(2)]
    placed = jnp.concatenate(
        [c[:, j * part : (j + 1) * part] for j in range(3) for c in chosen], axis=1
    )
    wide = jnp.concatenate([total] * 4, axis=1)
    row = lax.broadcasted_iota(jnp.int32, placed.shape, 0)
    o_ref[...] = jnp.where(row < share_rows, placed, wide).astype(BF16)


def arrange(share_rows, rank, pieces):
    rows, columns = pieces[0].shape
    vmem = pl.BlockSpec(memory_space=pltpu.VMEM)
    return pl.pallas_call(
        functools.partial(arrange_body, share_rows),
        in_specs=[pl.BlockSpec(memory_space=pltpu.SMEM)] + [vmem] * 4,
        out_specs=vmem,
        out_shape=jax.ShapeDtypeStruct((rows, 4 * columns), BF16),
        name="arrange",
    )(rank[None], *pieces)


GELU_SCALE = 0.7978845608028654
GELU_CUBE = 0.044715


def middle_body(
    m0, m1, m2, m3, x_ref, g0, g1, g2, g3, w0, w1, w2, w3, wu_ref, wd_ref, vec_ref, bias_ref,
    z_ref, m_ref, dc_ref, dd_ref, du_ref, sum_ref, g_ref,
):
    step = pl.program_id(0)

    @pl.when(step == 0)
    def _():
        dd_ref[...] = jnp.zeros_like(dd_ref)
        du_ref[...] = jnp.zeros_like(du_ref)
        sum_ref[...] = jnp.zeros_like(sum_ref)

    for r, piece in enumerate((g0, g1, g2, g3)):

        @pl.when(step == r)
        def _(piece=piece):
            g_ref[...] = piece[...]

    branch = vec_ref[0:1]
    for piece, weight in zip((m0, m1, m2, m3), (w0, w1, w2, w3)):
        branch = branch + dot(piece[...], weight[...])

    @pl.when(step == 0)
    def _():
        z_ref[...] = branch

    unit, _ = norm_parts(x_ref[...].astype(F32) + branch)
    normed = (unit * vec_ref[1:2] + vec_ref[2:3]).astype(BF16)
    inner = dot(normed, wu_ref[...]) + bias_ref[...]
    square = inner * inner
    bent = jnp.tanh(GELU_SCALE * (inner + GELU_CUBE * inner * square))
    half = 0.5 * (1.0 + bent)
    active = (inner * half).astype(BF16)
    slope = half + 0.5 * inner * (1.0 - bent * bent) * (
        GELU_SCALE * (1.0 + 3.0 * GELU_CUBE * square)
    )
    grad = g_ref[...]
    m_ref[...] = dot(active, wd_ref[...]).astype(BF16)
    dd_ref[...] += left_cross(active, grad)
    grad_inner = right_cross(grad, wd_ref[...]) * slope
    grad_low = grad_inner.astype(BF16)
    du_ref[...] += left_cross(normed, grad_low)
    grad_normed = right_cross(grad_low, wu_ref[...])
    dc_ref[...] = grad_normed.astype(BF16)
    sum_ref[0:1] += jnp.sum(grad_low.astype(F32), axis=0, keepdims=True)
    sum_ref[1:2] += jnp.sum(grad_normed * unit, axis=0, keepdims=True)
    sum_ref[2:3] += jnp.sum(grad_normed, axis=0, keepdims=True)


def middle(count, pieces, tokens_all, grads, w_proj, w_up, w_down, vectors, bias):
    rows, width = tokens_all.shape
    part = pieces[0].shape[1]
    hidden = w_up.shape[1]
    steps = rows // count

    def held(shape):
        return pl.BlockSpec(shape, lambda i: (0, 0))

    def shifted(r):
        return pl.BlockSpec((count, part), lambda i: (jnp.bitwise_xor(i, r), 0))

    block = pl.BlockSpec((count, width), lambda i: (i, 0))
    return pl.pallas_call(
        middle_body,
        grid=(steps,),
        in_specs=[shifted(r) for r in range(4)]
        + [block]
        + [held(v.shape) for v in (*grads, *w_proj, w_up, w_down)]
        + [held(vectors.shape), held(bias.shape)],
        out_specs=[
            held((count, width)),
            block,
            block,
            held((hidden, width)),
            held((width, hidden)),
            held((8, width)),
        ],
        out_shape=[
            jax.ShapeDtypeStruct((count, width), F32),
            jax.ShapeDtypeStruct((rows, width), BF16),
            jax.ShapeDtypeStruct((rows, width), BF16),
            jax.ShapeDtypeStruct((hidden, width), F32),
            jax.ShapeDtypeStruct((width, hidden), F32),
            jax.ShapeDtypeStruct((8, width), F32),
        ],
        cost_estimate=pl.CostEstimate(
            flops=14 * rows * width * hidden,
            bytes_accessed=10 * rows * width + 14 * width * hidden,
            transcendentals=rows * hidden,
        ),
        scratch_shapes=[pltpu.VMEM((count, width), BF16)],
        name="middle",
    )(*pieces, tokens_all, *grads, *w_proj, w_up, w_down, vectors, bias)


def on_device(
    dp_size,
    fs_size,
    tokens,
    cotangent,
    segment_ids,
    valid_mask,
    ln1_gain,
    ln1_bias,
    qkv_weight,
    qkv_bias,
    query_gain,
    query_bias,
    key_gain,
    proj_weight,
    proj_bias,
    ln2_gain,
    ln2_bias,
    fc1_weight,
    fc1_bias,
    fc2_weight,
    fc2_bias,
):
    count, width = tokens.shape
    rank = lax.axis_index("fsdp")
    place = lax.axis_index("dp")
    near = functools.partial(swap, axis="fsdp", size=fs_size, bit=1)
    far = functools.partial(swap, axis="fsdp", size=fs_size, bit=2)
    own_heads = HEADS // fs_size
    part = own_heads * HEAD_DIM
    hidden = fc1_weight.shape[1]
    hidden_own = hidden // fs_size
    rows_own = qkv_weight.shape[0]
    rounds = [1 << i for i in range(dp_size.bit_length() - 1)]

    def gather(value):
        second = far(value)
        return [value, near(value), second, near(second)]

    def spread(pieces):
        return [pieces[0], near(pieces[1]), far(pieces[2]), swap(pieces[3], "fsdp", fs_size, 3)]

    def collect(low, mark=None):
        low = [low[r * count : (r + 1) * count] for r in range(4)]
        other = near(jnp.concatenate([low[1], low[3]], axis=0)).astype(F32)
        first = low[0].astype(F32) + other[:count]
        sent = (low[2].astype(F32) + other[count:]).astype(BF16)
        sent = sent if mark is None else after(sent, mark)
        return first + far(sent).astype(F32), sent

    def at(r):
        return rank ^ r

    def ordered(pieces, axis):
        chosen = [lax.select_n(at(i), *[pieces[j] for j in range(4)]) for i in range(4)]
        return jnp.concatenate(chosen, axis=axis)

    small = pack(
        (ln1_gain, ln1_bias, ln2_gain, ln2_bias, proj_bias, fc2_bias, qkv_bias)
        + (query_gain, query_bias, key_gain),
        rows_own,
    )
    small_all = ordered([p[:, None] for p in gather(small)], 1).astype(F32)
    wide = small_all[:6].reshape(6, width)
    gain_one, shift_one, gain_two, shift_two, b_proj, b_down = [wide[i] for i in range(6)]
    narrow = query_gain.shape[0]
    gain_query, shift_query, gain_key = [
        small_all[i, :, :narrow].reshape(-1) for i in (9, 10, 11)
    ]
    b_qkv_all = small_all[6:9].transpose(1, 0, 2).reshape(-1)

    def own_columns(matrix, owner):
        return [
            lax.dynamic_slice_in_dim(matrix, block * width + owner * part, part, matrix.ndim - 1)
            for block in range(3)
        ]

    tokens_all = jnp.concatenate(gather(tokens), axis=0)
    w_qkv = ordered(
        spread([jnp.concatenate(own_columns(qkv_weight, at(r)), axis=1) for r in range(4)]), 0
    )

    def after(value, other):
        return lax.optimization_barrier((value, other))[0]

    up_pieces = [
        lax.dynamic_slice_in_dim(fc1_weight, at(r) * hidden_own, hidden_own, 1) for r in range(4)
    ]
    weights_valid = valid_mask.astype(F32)[:, None]
    grad_mlp_own = (cotangent.astype(F32) * weights_valid).astype(BF16)
    late = jnp.concatenate([proj_weight, grad_mlp_own, up_pieces[2]], axis=0)
    both = proj_weight.shape[0] + count
    late = far(after(late, w_qkv))
    up_pieces[3] = swap(after(up_pieces[3], w_qkv), "fsdp", fs_size, 3)
    up_pieces[1] = near(after(up_pieces[1], w_qkv))
    up_pieces[2] = late[both:]
    first = near(jnp.concatenate([proj_weight, grad_mlp_own], axis=0))
    last = near(late[:both])
    cut = proj_weight.shape[0]
    w_proj_pieces = [proj_weight, first[:cut], late[:cut], last[:cut]]
    grad_mlp_pieces = [grad_mlp_own, first[cut:], late[cut:both], last[cut:]]
    w_up = ordered(up_pieces, 0)
    ids = ordered([segment_ids[i * count : (i + 1) * count] for i in range(4)], 0)

    b_qkv = jnp.concatenate(own_columns(b_qkv_all, rank))
    vectors_one = jnp.concatenate([gain_one[None], shift_one[None]])
    head_vectors = jnp.concatenate([gain_query[None], shift_query[None], gain_key[None]])
    mixed_own, probs, raw, queries, keys, values = front(
        count, tokens_all, w_qkv, vectors_one, b_qkv[None], head_vectors, ids
    )
    vectors = jnp.concatenate([b_proj[None], gain_two[None], shift_two[None]])
    mixed_pieces = gather(mixed_own)
    branch_own, mlp_part, grad_two_part, total_down, total_up, sums_middle = middle(
        count, mixed_pieces, tokens_all, grad_mlp_pieces, w_proj_pieces, w_up, fc2_weight, vectors,
        fc1_bias.astype(F32)[None],
    )
    inputs = tokens.astype(F32)
    hidden_one = inputs + branch_own

    def held_back(other, marks, order):
        return after(other, marks[order]) if order < len(marks) and marks[order] is not None else other

    def halve(total, marks=(), tail=0):
        seen, lead = [], None
        first, second = total[:, : total.shape[1] - tail], total[:, total.shape[1] - tail :]
        for order, bit in enumerate(rounds):
            size = first.shape[1] // 2
            some = second.shape[1] // 2
            low, high = first[:, :size], first[:, size:]
            if tail:
                low = jnp.concatenate([low, second[:, :some]], axis=1)
                high = jnp.concatenate([high, second[:, some:]], axis=1)
            upper = (place & bit) != 0
            sent = jnp.where(upper, low, high).astype(BF16)
            lead = sent if order == 0 else lead
            other = held_back(swap(sent, "dp", dp_size, bit), marks, order)
            seen.append(other)
            total = jnp.where(upper, high, low).astype(F32) + other.astype(F32)
            first, second = total[:, :size], total[:, size:]
        return total, seen, lead

    def unite(share, marks=()):
        share = share.astype(BF16)[None]
        seen = []
        for order, bit in enumerate(reversed(rounds)):
            other = held_back(swap(share, "dp", dp_size, bit), marks, order)
            seen.append(other)
            upper = (place & bit) != 0
            share = jnp.where(
                upper,
                jnp.concatenate([other, share], axis=0),
                jnp.concatenate([share, other], axis=0),
            )
        return share, seen

    def to_rows(share):
        share = share.astype(BF16)
        return spread([lax.dynamic_index_in_dim(share, at(r), 0, False) for r in range(4)])

    grad_normed_two, mark_two = collect(grad_two_part)
    total_down = after(total_down, mark_two)
    sums_middle = after(sums_middle, mark_two)
    mlp_part = after(mlp_part, mark_two)
    grad_out = after(grad_mlp_own, mark_two).astype(F32)
    unit_two, scale_two = norm_parts(hidden_one)
    grad_hidden = grad_out + norm_back(grad_normed_two * gain_two, unit_two, scale_two)
    grad_branch_own = grad_hidden.astype(BF16)
    grad_branch_low = jnp.concatenate(gather(grad_branch_own), axis=0)
    total_proj = left_cross(mixed_own, grad_branch_low)
    own_sums = [sums_middle[1], sums_middle[2], jnp.sum(grad_branch_own.astype(F32), axis=0)]
    own_sums = jnp.stack(own_sums).reshape(3, fs_size, rows_own)
    bias_up = jnp.where(jnp.arange(fs_size)[:, None] == rank, sums_middle[0][None], 0.0)
    bias_down = jnp.sum(grad_out, axis=0).reshape(fs_size, rows_own)
    early_rows = jnp.concatenate(
        [own_sums[0], own_sums[1], own_sums[2], bias_up, bias_down], axis=1
    )
    early_rows = jnp.pad(early_rows, ((0, 0), (0, 9 * part - early_rows.shape[1])))
    early_rows = early_rows.reshape(fs_size, 3, 3 * part)
    total_last, grad_one_part = back(
        count, dp_size, rank, grad_branch_low, proj_weight, probs, raw, queries, keys, values,
        tokens_all, w_qkv, vectors_one, head_vectors, early_rows,
    )
    share_last, seen, lead = halve(total_last, tail=dp_size)
    grad_normed_one, _ = collect(after(grad_one_part, lead))
    unit_one, scale_one = norm_parts(inputs)
    tokens_grad = grad_hidden + norm_back(
        grad_normed_one * gain_one, unit_one, scale_one
    )

    branch_mlp = collect(mlp_part, lead)[0] + b_down
    result = hidden_one + branch_mlp
    rms_sums = jnp.stack(
        [
            jnp.sum(weights_valid * result * result),
            jnp.sum(weights_valid * branch_own * branch_own),
            jnp.sum(weights_valid * branch_mlp * branch_mlp),
            jnp.sum(weights_valid),
        ]
    )

    rms_sums = jnp.broadcast_to(rms_sums[:, None], (4, 128))
    for bit in (1, 2):
        rms_sums = rms_sums + swap(rms_sums, "fsdp", fs_size, bit)
    rms_rows = jnp.pad(rms_sums[:, 0], (0, width - 4))[None]
    rms_rows = jnp.pad(rms_rows, ((0, dp_size - 1), (0, 0)))

    count_rounds = len(rounds)
    pieces_last = to_rows(share_last)
    share_rows = rows_own // dp_size
    last, seen_back = unite(arrange(share_rows, rank, pieces_last))
    seen = [*seen, pieces_last[3], *seen_back]

    early = [grad_normed_two, grad_branch_own] + [grad_branch_low] * (count_rounds - 2)
    share_down, seen_down, _ = halve(total_down[None], early)
    grad_down, _ = unite(share_down[0], [lead, seen[0], seen[1]])
    grad_down = grad_down.astype(F32).reshape(hidden_own, width)
    total_up = after(total_up, seen_down[0])
    late = [grad_branch_own, lead] + [seen[0]] * (count_rounds - 2)
    share_up, _, _ = halve(total_up.reshape(fs_size, rows_own, hidden_own), late)
    pieces_up = to_rows(share_up)
    pieces_up[3] = after(pieces_up[3], seen[1])
    grad_up, _ = unite(ordered(pieces_up, 1), [seen[2], seen[3]])
    grad_up = grad_up.astype(F32).reshape(rows_own, hidden)
    total_proj = after(jnp.concatenate([total_proj, rms_rows], axis=0), seen[0])
    share_proj, _, _ = halve(total_proj[None], seen[1 : count_rounds + 1], tail=dp_size)
    grad_proj, _ = unite(share_proj[0], seen[count_rounds + 1 : -1])
    grad_proj = grad_proj.astype(F32)
    last = last.astype(F32)
    grad_qkv = last[:, :share_rows].reshape(rows_own, 3 * width)
    table = last[:, share_rows, : 3 * part]
    narrow = HEAD_DIM // fs_size
    flat = table[3:6].reshape(-1)
    finals = [table[0, :rows_own], table[0, rows_own : 2 * rows_own], table[1]]
    finals += [table[2, i * narrow : (i + 1) * narrow] for i in range(3)]
    finals += [flat[2 * rows_own : 3 * rows_own], flat[:rows_own], flat[rows_own : 2 * rows_own]]
    finals += [flat[3 * rows_own : 3 * rows_own + hidden_own]]
    finals += [flat[3 * rows_own + hidden_own : 4 * rows_own + hidden_own]]
    sums = grad_proj[0, share_rows, :4]
    return (
        result.astype(BF16),
        tokens_grad,
        finals[0],
        finals[1],
        grad_qkv,
        finals[2],
        finals[3],
        finals[4],
        finals[5],
        grad_proj[:, :share_rows].reshape(rows_own, width),
        finals[6],
        finals[7],
        finals[8],
        grad_up,
        finals[9],
        grad_down,
        finals[10],
        jnp.sqrt(sums[:3] / sums[3]),
    )


def solution(mesh):
    rows = P(("dp", "fsdp"), None)
    vector = P("fsdp")
    matrix = P("fsdp", None)
    device = functools.partial(on_device, mesh.shape["dp"], mesh.shape["fsdp"])

    return jax.shard_map(
        device,
        mesh=mesh,
        in_specs=(
            rows, rows, P("dp"), P(("dp", "fsdp")), vector, vector, matrix, vector, vector, vector,
            vector, matrix, vector, vector, vector, matrix, vector, matrix, vector,
        ),
        out_specs=(
            rows, rows, vector, vector, matrix, vector, vector, vector, vector, matrix, vector,
            vector, vector, matrix, vector, matrix, vector, P(),
        ),
        check_vma=False,
    )
```

```python
import functools

import jax
import jax.numpy as jnp
from jax import lax
from jax.experimental import pallas as pl
from jax.experimental.pallas import tpu as pltpu
from jax.sharding import PartitionSpec as P


HEADS = 12
HEAD_DIM = 64
EPS = 1e-06
MASKED = -1e30
F32 = jnp.float32
BF16 = jnp.bfloat16


def swap(value, axis, size, bit):
    return lax.ppermute(value, axis, [(i, i ^ bit) for i in range(size)])


def dot(first, second):
    return jnp.dot(first, second, preferred_element_type=F32)


def left_cross(first, second):
    return lax.dot_general(first, second, (((0,), (0,)), ((), ())), preferred_element_type=F32)


def right_cross(first, second):
    return lax.dot_general(first, second, (((1,), (1,)), ((), ())), preferred_element_type=F32)


def norm_parts(values):
    average = jnp.mean(values, axis=-1, keepdims=True)
    centred = values - average
    spread = jnp.mean(centred * centred, axis=-1, keepdims=True)
    scale = lax.rsqrt(spread + EPS)
    return centred * scale, scale


def norm_back(grad, unit, scale):
    return scale * (
        grad
        - jnp.mean(grad, axis=-1, keepdims=True)
        - unit * jnp.mean(grad * unit, axis=-1, keepdims=True)
    )


def block_of(step, count):
    return pl.ds(pl.multiple_of(step * count, count), count)


def front_body(
    count, x_ref, w_ref, vec_ref, bias_ref, head_ref, rows_ref, cols_ref,
    o_ref, p_ref, raw_ref, q_ref, k_ref, v_ref,
):
    heads, rows, size = q_ref.shape
    scaling = size**-0.5

    @pl.loop(0, rows // count)
    def _(step):
        at = block_of(step, count)
        unit, _ = norm_parts(x_ref[at].astype(F32))
        normed = (unit * vec_ref[0:1] + vec_ref[1:2]).astype(BF16)
        projected = dot(normed, w_ref[...]) + bias_ref[...]
        for h in range(heads):
            query, key, value = [
                projected[:, (j * heads + h) * size : (j * heads + h + 1) * size] for j in range(3)
            ]
            raw_ref[h, at] = query
            raw_ref[heads + h, at] = key
            unit, _ = norm_parts(query)
            q_ref[h, at] = ((unit * head_ref[0:1] + head_ref[1:2]) * scaling).astype(BF16)
            unit, _ = norm_parts(key)
            k_ref[h, at] = (unit * head_ref[2:3]).astype(BF16)
            v_ref[h, at] = value.astype(BF16)

    for h in range(heads):

        @pl.loop(0, rows // count)
        def _(step):
            at = block_of(step, count)
            scores = right_cross(q_ref[h, at], k_ref[h])
            scores = jnp.where(rows_ref[at] == cols_ref[...], scores, MASKED)
            top = jnp.max(scores, axis=-1, keepdims=True)
            raised = jnp.exp(scores - top)
            total = jnp.sum(raised, axis=-1, keepdims=True)
            probs = (raised * (1.0 / total)).astype(BF16)
            p_ref[h, at] = probs
            o_ref[at, h * size : (h + 1) * size] = dot(probs, v_ref[h]).astype(BF16)


def front(count, tokens_all, w_qkv, vectors, bias, head_vectors, ids):
    rows, width = tokens_all.shape
    size = head_vectors.shape[1]
    part = w_qkv.shape[1] // 3
    heads = part // size
    return pl.pallas_call(
        functools.partial(front_body, count),
        out_shape=[
            jax.ShapeDtypeStruct((rows, part), BF16),
            jax.ShapeDtypeStruct((heads, rows, rows), BF16),
            jax.ShapeDtypeStruct((2 * heads, rows, size), F32),
            jax.ShapeDtypeStruct((heads, rows, size), BF16),
            jax.ShapeDtypeStruct((heads, rows, size), BF16),
            jax.ShapeDtypeStruct((heads, rows, size), BF16),
        ],
        cost_estimate=pl.CostEstimate(
            flops=6 * rows * width * part + 4 * heads * rows * rows * size,
            bytes_accessed=2 * rows * (width + heads * rows + 8 * part) + 6 * width * part,
            transcendentals=heads * rows * rows,
        ),
        name="front",
    )(tokens_all, w_qkv, vectors, bias, head_vectors, ids[:, None], ids[None, :])


def back_body(
    count, rank_ref, z_ref, wp_ref, p_ref, raw_ref, q_ref, k_ref, v_ref, x_ref, w_ref, vec_ref,
    head_ref, early_ref, out_ref, da_ref, sum_ref, bias_ref, heads_ref, dw_ref, g_ref, dk_ref,
    dv_ref, dq_ref, dkt_ref, dvt_ref,
):
    heads, rows, size = q_ref.shape
    scaling = size**-0.5
    steps = rows // count
    sum_ref[...] = jnp.zeros_like(sum_ref)
    bias_ref[...] = jnp.zeros_like(bias_ref)
    heads_ref[...] = jnp.zeros_like(heads_ref)
    dw_ref[...] = jnp.zeros_like(dw_ref)
    for h in range(heads):
        dk_ref[...] = jnp.zeros_like(dk_ref)
        dv_ref[...] = jnp.zeros_like(dv_ref)

        @pl.loop(0, steps)
        def _(step):
            at = block_of(step, count)
            grad = right_cross(z_ref[at], wp_ref[h * size : (h + 1) * size]).astype(BF16)
            low = p_ref[h, at]
            probs = low.astype(F32)
            grad_probs = right_cross(grad, v_ref[h])
            delta = jnp.sum(probs * grad_probs, axis=-1, keepdims=True)
            grad_scores = (probs * (grad_probs - delta)).astype(BF16)
            dq_ref[at] = dot(grad_scores, k_ref[h])
            dk_ref[...] += left_cross(q_ref[h, at], grad_scores)
            dv_ref[...] += left_cross(grad, low)

        dkt_ref[...] = dk_ref[...].T
        dvt_ref[...] = dv_ref[...].T

        @pl.loop(0, steps)
        def _(step):
            at = block_of(step, count)
            grad = dq_ref[at] * scaling
            unit, scale = norm_parts(raw_ref[h, at])
            heads_ref[0:1] += jnp.sum(grad * unit, axis=0, keepdims=True)
            heads_ref[1:2] += jnp.sum(grad, axis=0, keepdims=True)
            g_ref[at, h * size : (h + 1) * size] = norm_back(
                grad * head_ref[0:1], unit, scale
            ).astype(BF16)
            grad = dkt_ref[at]
            unit, scale = norm_parts(raw_ref[heads + h, at])
            heads_ref[2:3] += jnp.sum(grad * unit, axis=0, keepdims=True)
            first = (heads + h) * size
            g_ref[at, first : first + size] = norm_back(grad * head_ref[2:3], unit, scale).astype(
                BF16
            )
            first = (2 * heads + h) * size
            g_ref[at, first : first + size] = dvt_ref[at].astype(BF16)

    @pl.loop(0, steps)
    def _(step):
        at = block_of(step, count)
        unit, _ = norm_parts(x_ref[at].astype(F32))
        normed = (unit * vec_ref[0:1] + vec_ref[1:2]).astype(BF16)
        grad = g_ref[at]
        dw_ref[...] += left_cross(normed, grad)
        bias_ref[0:1] += jnp.sum(grad.astype(F32), axis=0, keepdims=True)
        grad_normed = right_cross(grad, w_ref[...])
        da_ref[at] = grad_normed.astype(BF16)
        sum_ref[0:1] += jnp.sum(grad_normed * unit, axis=0, keepdims=True)
        sum_ref[1:2] += jnp.sum(grad_normed, axis=0, keepdims=True)


    owners, total_rows, columns = out_ref.shape
    own = dw_ref.shape[0] // owners
    part = columns // 3
    rank = rank_ref[0]
    narrow = size // owners
    for o in range(owners):
        out_ref[o, :own] = dw_ref[o * own : (o + 1) * own]
        first = jnp.concatenate(
            [sum_ref[i : i + 1, o * own : (o + 1) * own] for i in range(2)]
            + [jnp.zeros((1, columns - 2 * own), F32)],
            axis=1,
        )
        groups = []
        for j in range(3):
            group = 3 * o + j
            value = bias_ref[0:1, group // owners * part : (group // owners + 1) * part]
            groups.append(jnp.where(rank == group % owners, value, 0.0))
        gains = [heads_ref[i : i + 1, o * narrow : (o + 1) * narrow] for i in range(3)]
        third = jnp.concatenate([*gains, jnp.zeros((1, columns - 3 * narrow), F32)], axis=1)
        out_ref[o, own:] = jnp.concatenate(
            [first, jnp.concatenate(groups, axis=1), third, early_ref[o]]
            + [jnp.zeros((total_rows - own - 3 - early_ref.shape[1], columns), F32)],
            axis=0,
        )


def back(count, extra, rank, *values):
    _, _, _, _, queries, _, _, tokens_all, _, _, _, early = values
    rows, width = tokens_all.shape
    heads, _, size = queries.shape
    part = heads * size
    owners = early.shape[0]
    vmem = pl.BlockSpec(memory_space=pltpu.VMEM)
    return pl.pallas_call(
        functools.partial(back_body, count),
        in_specs=[pl.BlockSpec(memory_space=pltpu.SMEM)] + [vmem] * len(values),
        out_specs=[vmem, vmem],
        out_shape=[
            jax.ShapeDtypeStruct((owners, width // owners + extra, 3 * part), F32),
            jax.ShapeDtypeStruct((rows, width), BF16),
        ],
        scratch_shapes=[
            pltpu.VMEM((8, width), F32),
            pltpu.VMEM((8, 3 * part), F32),
            pltpu.VMEM((8, size), F32),
            pltpu.VMEM((width, 3 * part), F32),
            pltpu.VMEM((rows, 3 * part), BF16),
            pltpu.VMEM((size, rows), F32),
            pltpu.VMEM((size, rows), F32),
            pltpu.VMEM((rows, size), F32),
            pltpu.VMEM((rows, size), F32),
            pltpu.VMEM((rows, size), F32),
        ],
        cost_estimate=pl.CostEstimate(
            flops=14 * rows * width * part + 8 * heads * rows * rows * size,
            bytes_accessed=2 * rows * (3 * width + heads * rows + 12 * part) + 18 * width * part,
            transcendentals=0,
        ),
        name="back",
    )(rank[None], *values)


def pack_body(*refs):
    out = refs[-1]
    columns = out.shape[1]
    rows = []
    for ref in refs[:-1]:
        value = ref[...].astype(F32)[None]
        size = value.shape[1]
        if size < columns:
            rows.append(jnp.concatenate([value, jnp.zeros((1, columns - size), F32)], axis=1))
        else:
            rows += [value[:, i : i + columns] for i in range(0, size, columns)]
    rows.append(jnp.zeros((out.shape[0] - len(rows), columns), F32))
    out[...] = jnp.concatenate(rows, axis=0).astype(BF16)


def pack(vectors, columns):
    return pl.pallas_call(
        pack_body, out_shape=jax.ShapeDtypeStruct((16, columns), BF16), name="pack"
    )(*vectors)


def arrange_body(share_rows, rank_ref, p0, p1, p2, p3, o_ref):
    pieces = [p[...].astype(F32) for p in (p0, p1, p2, p3)]
    part = pieces[0].shape[1] // 3
    low, high = (rank_ref[0] & 1) == 1, (rank_ref[0] & 2) == 2
    pairs = [
        (jnp.where(low, a, b), jnp.where(low, b, a))
        for a, b in ((pieces[1], pieces[0]), (pieces[3], pieces[2]))
    ]
    total = (pieces[0] + pieces[1]) + (pieces[2] + pieces[3])
    chosen = [jnp.where(high, pairs[1][i], pairs[0][i]) for i in range(2)]
    chosen += [jnp.where(high, pairs[0][i], pairs[1][i]) for i in range(2)]
    placed = jnp.concatenate(
        [c[:, j * part : (j + 1) * part] for j in range(3) for c in chosen], axis=1
    )
    wide = jnp.concatenate([total] * 4, axis=1)
    row = lax.broadcasted_iota(jnp.int32, placed.shape, 0)
    o_ref[...] = jnp.where(row < share_rows, placed, wide).astype(BF16)


def arrange(share_rows, rank, pieces):
    rows, columns = pieces[0].shape
    vmem = pl.BlockSpec(memory_space=pltpu.VMEM)
    return pl.pallas_call(
        functools.partial(arrange_body, share_rows),
        in_specs=[pl.BlockSpec(memory_space=pltpu.SMEM)] + [vmem] * 4,
        out_specs=vmem,
        out_shape=jax.ShapeDtypeStruct((rows, 4 * columns), BF16),
        name="arrange",
    )(rank[None], *pieces)


GELU_SCALE = 0.7978845608028654
GELU_CUBE = 0.044715


def middle_body(
    m0, m1, m2, m3, x_ref, g0, g1, g2, g3, w0, w1, w2, w3, wu_ref, wd_ref, vec_ref, bias_ref,
    z_ref, m_ref, dc_ref, dd_ref, du_ref, sum_ref, g_ref,
):
    step = pl.program_id(0)

    @pl.when(step == 0)
    def _():
        dd_ref[...] = jnp.zeros_like(dd_ref)
        du_ref[...] = jnp.zeros_like(du_ref)
        sum_ref[...] = jnp.zeros_like(sum_ref)

    for r, piece in enumerate((g0, g1, g2, g3)):

        @pl.when(step == r)
        def _(piece=piece):
            g_ref[...] = piece[...]

    branch = vec_ref[0:1]
    for piece, weight in zip((m0, m1, m2, m3), (w0, w1, w2, w3)):
        branch = branch + dot(piece[...], weight[...])

    @pl.when(step == 0)
    def _():
        z_ref[...] = branch

    unit, _ = norm_parts(x_ref[...].astype(F32) + branch)
    normed = (unit * vec_ref[1:2] + vec_ref[2:3]).astype(BF16)
    inner = dot(normed, wu_ref[...]) + bias_ref[...]
    square = inner * inner
    bent = jnp.tanh(GELU_SCALE * (inner + GELU_CUBE * inner * square))
    half = 0.5 * (1.0 + bent)
    active = (inner * half).astype(BF16)
    slope = half + 0.5 * inner * (1.0 - bent * bent) * (
        GELU_SCALE * (1.0 + 3.0 * GELU_CUBE * square)
    )
    grad = g_ref[...]
    m_ref[...] = dot(active, wd_ref[...]).astype(BF16)
    dd_ref[...] += left_cross(active, grad)
    grad_inner = right_cross(grad, wd_ref[...]) * slope
    grad_low = grad_inner.astype(BF16)
    du_ref[...] += left_cross(normed, grad_low)
    grad_normed = right_cross(grad_low, wu_ref[...])
    dc_ref[...] = grad_normed.astype(BF16)
    sum_ref[0:1] += jnp.sum(grad_low.astype(F32), axis=0, keepdims=True)
    sum_ref[1:2] += jnp.sum(grad_normed * unit, axis=0, keepdims=True)
    sum_ref[2:3] += jnp.sum(grad_normed, axis=0, keepdims=True)


def middle(count, pieces, tokens_all, grads, w_proj, w_up, w_down, vectors, bias):
    rows, width = tokens_all.shape
    part = pieces[0].shape[1]
    hidden = w_up.shape[1]
    steps = rows // count

    def held(shape):
        return pl.BlockSpec(shape, lambda i: (0, 0))

    def shifted(r):
        return pl.BlockSpec((count, part), lambda i: (jnp.bitwise_xor(i, r), 0))

    block = pl.BlockSpec((count, width), lambda i: (i, 0))
    return pl.pallas_call(
        middle_body,
        grid=(steps,),
        in_specs=[shifted(r) for r in range(4)]
        + [block]
        + [held(v.shape) for v in (*grads, *w_proj, w_up, w_down)]
        + [held(vectors.shape), held(bias.shape)],
        out_specs=[
            held((count, width)),
            block,
            block,
            held((hidden, width)),
            held((width, hidden)),
            held((8, width)),
        ],
        out_shape=[
            jax.ShapeDtypeStruct((count, width), F32),
            jax.ShapeDtypeStruct((rows, width), BF16),
            jax.ShapeDtypeStruct((rows, width), BF16),
            jax.ShapeDtypeStruct((hidden, width), F32),
            jax.ShapeDtypeStruct((width, hidden), F32),
            jax.ShapeDtypeStruct((8, width), F32),
        ],
        cost_estimate=pl.CostEstimate(
            flops=14 * rows * width * hidden,
            bytes_accessed=10 * rows * width + 14 * width * hidden,
            transcendentals=rows * hidden,
        ),
        scratch_shapes=[pltpu.VMEM((count, width), BF16)],
        name="middle",
    )(*pieces, tokens_all, *grads, *w_proj, w_up, w_down, vectors, bias)


def on_device(
    dp_size,
    fs_size,
    tokens,
    cotangent,
    segment_ids,
    valid_mask,
    ln1_gain,
    ln1_bias,
    qkv_weight,
    qkv_bias,
    query_gain,
    query_bias,
    key_gain,
    proj_weight,
    proj_bias,
    ln2_gain,
    ln2_bias,
    fc1_weight,
    fc1_bias,
    fc2_weight,
    fc2_bias,
):
    count, width = tokens.shape
    rank = lax.axis_index("fsdp")
    place = lax.axis_index("dp")
    near = functools.partial(swap, axis="fsdp", size=fs_size, bit=1)
    far = functools.partial(swap, axis="fsdp", size=fs_size, bit=2)
    own_heads = HEADS // fs_size
    part = own_heads * HEAD_DIM
    hidden = fc1_weight.shape[1]
    hidden_own = hidden // fs_size
    rows_own = qkv_weight.shape[0]
    rounds = [1 << i for i in range(dp_size.bit_length() - 1)]

    def gather(value):
        second = far(value)
        return [value, near(value), second, near(second)]

    def spread(pieces):
        return [pieces[0], near(pieces[1]), far(pieces[2]), swap(pieces[3], "fsdp", fs_size, 3)]

    def collect(low, mark=None):
        low = [low[r * count : (r + 1) * count] for r in range(4)]
        other = near(jnp.concatenate([low[1], low[3]], axis=0)).astype(F32)
        first = low[0].astype(F32) + other[:count]
        sent = (low[2].astype(F32) + other[count:]).astype(BF16)
        sent = sent if mark is None else after(sent, mark)
        other = far(sent)
        return first + other.astype(F32), sent

    def at(r):
        return rank ^ r

    def ordered(pieces, axis):
        chosen = [lax.select_n(at(i), *[pieces[j] for j in range(4)]) for i in range(4)]
        return jnp.concatenate(chosen, axis=axis)

    small = pack(
        (ln1_gain, ln1_bias, ln2_gain, ln2_bias, proj_bias, fc2_bias, qkv_bias)
        + (query_gain, query_bias, key_gain),
        rows_own,
    )
    small_all = ordered([p[:, None] for p in gather(small)], 1).astype(F32)
    wide = small_all[:6].reshape(6, width)
    gain_one, shift_one, gain_two, shift_two, b_proj, b_down = [wide[i] for i in range(6)]
    narrow = query_gain.shape[0]
    gain_query, shift_query, gain_key = [
        small_all[i, :, :narrow].reshape(-1) for i in (9, 10, 11)
    ]
    b_qkv_all = small_all[6:9].transpose(1, 0, 2).reshape(-1)

    def own_columns(matrix, owner):
        return [
            lax.dynamic_slice_in_dim(matrix, block * width + owner * part, part, matrix.ndim - 1)
            for block in range(3)
        ]

    tokens_all = jnp.concatenate(gather(tokens), axis=0)
    w_qkv = ordered(
        spread([jnp.concatenate(own_columns(qkv_weight, at(r)), axis=1) for r in range(4)]), 0
    )

    def after(value, other):
        return lax.optimization_barrier((value, other))[0]

    w_proj_pieces = gather(after(proj_weight, w_qkv))
    up_pieces = [
        lax.dynamic_slice_in_dim(after(fc1_weight, w_qkv), at(r) * hidden_own, hidden_own, 1)
        for r in range(4)
    ]
    up_pieces[1] = near(up_pieces[1])
    up_pieces[2] = far(up_pieces[2])
    up_pieces[3] = swap(up_pieces[3], "fsdp", fs_size, 3)
    w_up = ordered(up_pieces, 0)
    weights_valid = valid_mask.astype(F32)[:, None]
    grad_mlp_own = (cotangent.astype(F32) * weights_valid).astype(BF16)
    grad_mlp_pieces = gather(after(grad_mlp_own, w_qkv))
    ids = jnp.concatenate(
        [lax.dynamic_slice_in_dim(segment_ids, at(r) * count, count) for r in range(4)]
    )

    b_qkv = jnp.concatenate(own_columns(b_qkv_all, rank))
    vectors_one = jnp.concatenate([gain_one[None], shift_one[None]])
    head_vectors = jnp.concatenate([gain_query[None], shift_query[None], gain_key[None]])
    mixed_own, probs, raw, queries, keys, values = front(
        count, tokens_all, w_qkv, vectors_one, b_qkv[None], head_vectors, ids
    )
    vectors = jnp.concatenate([b_proj[None], gain_two[None], shift_two[None]])
    mixed_pieces = gather(mixed_own)
    branch_own, mlp_part, grad_two_part, total_down, total_up, sums_middle = middle(
        count, mixed_pieces, tokens_all, grad_mlp_pieces, w_proj_pieces, w_up, fc2_weight, vectors,
        fc1_bias.astype(F32)[None],
    )
    inputs = tokens.astype(F32)
    hidden_one = inputs + branch_own

    def held_back(other, marks, order):
        return after(other, marks[order]) if order < len(marks) and marks[order] is not None else other

    def halve(total, marks=(), tail=0):
        seen, lead = [], None
        first, second = total[:, : total.shape[1] - tail], total[:, total.shape[1] - tail :]
        for order, bit in enumerate(rounds):
            size = first.shape[1] // 2
            some = second.shape[1] // 2
            low, high = first[:, :size], first[:, size:]
            if tail:
                low = jnp.concatenate([low, second[:, :some]], axis=1)
                high = jnp.concatenate([high, second[:, some:]], axis=1)
            upper = (place & bit) != 0
            sent = jnp.where(upper, low, high).astype(BF16)
            lead = sent if order == 0 else lead
            other = swap(sent, "dp", dp_size, bit)
            other = held_back(other, marks, order)
            seen.append(other)
            total = jnp.where(upper, high, low).astype(F32) + other.astype(F32)
            first, second = total[:, :size], total[:, size:]
        return total, seen, lead

    def unite(share, marks=()):
        share = share.astype(BF16)[None]
        seen = []
        for order, bit in enumerate(reversed(rounds)):
            other = swap(share, "dp", dp_size, bit)
            other = held_back(other, marks, order)
            seen.append(other)
            upper = (place & bit) != 0
            share = jnp.where(
                upper,
                jnp.concatenate([other, share], axis=0),
                jnp.concatenate([share, other], axis=0),
            )
        return share, seen

    def to_rows(share):
        share = share.astype(BF16)
        return spread([lax.dynamic_index_in_dim(share, at(r), 0, False) for r in range(4)])

    grad_normed_two, mark_two = collect(grad_two_part)
    total_down = after(total_down, mark_two)
    sums_middle = after(sums_middle, mark_two)
    grad_out = after(grad_mlp_own, mark_two).astype(F32)
    unit_two, scale_two = norm_parts(hidden_one)
    grad_hidden = grad_out + norm_back(grad_normed_two * gain_two, unit_two, scale_two)
    grad_branch_own = grad_hidden.astype(BF16)
    grad_branch_low = jnp.concatenate(gather(grad_branch_own), axis=0)
    total_proj = left_cross(mixed_own, grad_branch_low)
    own_sums = [sums_middle[1], sums_middle[2], jnp.sum(grad_branch_own.astype(F32), axis=0)]
    own_sums = jnp.stack(own_sums).reshape(3, fs_size, rows_own)
    bias_up = jnp.where(jnp.arange(fs_size)[:, None] == rank, sums_middle[0][None], 0.0)
    bias_down = jnp.sum(grad_out, axis=0).reshape(fs_size, rows_own)
    early_rows = jnp.concatenate(
        [own_sums[0], own_sums[1], own_sums[2], bias_up, bias_down], axis=1
    )
    early_rows = jnp.pad(early_rows, ((0, 0), (0, 9 * part - early_rows.shape[1])))
    early_rows = early_rows.reshape(fs_size, 3, 3 * part)
    total_last, grad_one_part = back(
        count, dp_size, rank, grad_branch_low, proj_weight, probs, raw, queries, keys, values,
        tokens_all, w_qkv, vectors_one, head_vectors, early_rows,
    )
    share_last, seen, lead = halve(total_last, tail=dp_size)
    grad_normed_one, _ = collect(after(grad_one_part, lead))
    unit_one, scale_one = norm_parts(inputs)
    tokens_grad = grad_hidden + norm_back(
        grad_normed_one * gain_one, unit_one, scale_one
    )

    count_rounds = len(rounds)
    pieces_last = to_rows(share_last)
    share_rows = rows_own // dp_size
    last, seen_back = unite(arrange(share_rows, rank, pieces_last))
    seen = [*seen, pieces_last[3], *seen_back]

    branch_mlp = collect(after(mlp_part, lead))[0] + b_down
    result = hidden_one + branch_mlp
    rms_sums = jnp.stack(
        [
            jnp.sum(weights_valid * result * result),
            jnp.sum(weights_valid * branch_own * branch_own),
            jnp.sum(weights_valid * branch_mlp * branch_mlp),
            jnp.sum(weights_valid),
        ]
    )

    rms_sums = jnp.broadcast_to(rms_sums[:, None], (4, 128))
    hops = [("fsdp", fs_size, 1), ("fsdp", fs_size, 2)] + [("dp", dp_size, bit) for bit in rounds]
    for order, (axis, size, bit) in enumerate(hops):
        other = swap(rms_sums, axis, size, bit)
        rms_sums = rms_sums + after(other, seen[min(order + 1, len(seen) - 2)])
    sums = rms_sums[:, 0]

    early = [grad_branch_own, grad_branch_own] + [grad_branch_low] * (count_rounds - 2)
    share_down, seen_down, _ = halve(total_down[None], early)
    grad_down, _ = unite(share_down[0], [seen[0], seen[0], seen[1]])
    grad_down = grad_down.astype(F32).reshape(hidden_own, width)
    total_up = after(total_up, seen_down[0])
    late = [grad_branch_own, lead] + [seen[0]] * (count_rounds - 2)
    share_up, _, _ = halve(total_up.reshape(fs_size, rows_own, hidden_own), late)
    pieces_up = to_rows(share_up)
    grad_up, _ = unite(ordered(pieces_up, 1), [seen[1], seen[2], seen[count_rounds]])
    grad_up = grad_up.astype(F32).reshape(rows_own, hidden)
    share_proj, _, _ = halve(total_proj[None], seen[:count_rounds])
    grad_proj, _ = unite(share_proj[0], seen[count_rounds:])
    grad_proj = grad_proj.astype(F32).reshape(rows_own, width)
    last = last.astype(F32)
    grad_qkv = last[:, :share_rows].reshape(rows_own, 3 * width)
    table = last[:, share_rows, : 3 * part]
    narrow = HEAD_DIM // fs_size
    flat = table[3:6].reshape(-1)
    finals = [table[0, :rows_own], table[0, rows_own : 2 * rows_own], table[1]]
    finals += [table[2, i * narrow : (i + 1) * narrow] for i in range(3)]
    finals += [flat[2 * rows_own : 3 * rows_own], flat[:rows_own], flat[rows_own : 2 * rows_own]]
    finals += [flat[3 * rows_own : 3 * rows_own + hidden_own]]
    finals += [flat[3 * rows_own + hidden_own : 4 * rows_own + hidden_own]]
    return (
        result.astype(BF16),
        tokens_grad,
        finals[0],
        finals[1],
        grad_qkv,
        finals[2],
        finals[3],
        finals[4],
        finals[5],
        grad_proj,
        finals[6],
        finals[7],
        finals[8],
        grad_up,
        finals[9],
        grad_down,
        finals[10],
        jnp.sqrt(sums[:3] / sums[3]),
    )


def solution(mesh):
    rows = P(("dp", "fsdp"), None)
    vector = P("fsdp")
    matrix = P("fsdp", None)
    device = functools.partial(on_device, mesh.shape["dp"], mesh.shape["fsdp"])

    return jax.shard_map(
        device,
        mesh=mesh,
        in_specs=(
            rows, rows, P("dp"), P(("dp", "fsdp")), vector, vector, matrix, vector, vector, vector,
            vector, matrix, vector, vector, vector, matrix, vector, matrix, vector,
        ),
        out_specs=(
            rows, rows, vector, vector, matrix, vector, vector, vector, vector, matrix, vector,
            vector, vector, matrix, vector, matrix, vector, P(),
        ),
        check_vma=False,
    )
```

```python
import functools

import jax
import jax.numpy as jnp
from jax import lax
from jax.experimental import pallas as pl
from jax.experimental.pallas import tpu as pltpu
from jax.sharding import PartitionSpec as P


HEADS = 12
HEAD_DIM = 64
EPS = 1e-06
MASKED = -1e30
F32 = jnp.float32
BF16 = jnp.bfloat16


def swap(value, axis, size, bit):
    return lax.ppermute(value, axis, [(i, i ^ bit) for i in range(size)])


def dot(first, second):
    return jnp.dot(first, second, preferred_element_type=F32)


def left_cross(first, second):
    return lax.dot_general(first, second, (((0,), (0,)), ((), ())), preferred_element_type=F32)


def right_cross(first, second):
    return lax.dot_general(first, second, (((1,), (1,)), ((), ())), preferred_element_type=F32)


def norm_parts(values):
    average = jnp.mean(values, axis=-1, keepdims=True)
    centred = values - average
    spread = jnp.mean(centred * centred, axis=-1, keepdims=True)
    scale = lax.rsqrt(spread + EPS)
    return centred * scale, scale


def norm_back(grad, unit, scale):
    return scale * (
        grad
        - jnp.mean(grad, axis=-1, keepdims=True)
        - unit * jnp.mean(grad * unit, axis=-1, keepdims=True)
    )


def block_of(step, count):
    return pl.ds(pl.multiple_of(step * count, count), count)


def front_body(
    count, x_ref, w_ref, vec_ref, bias_ref, head_ref, rows_ref, cols_ref,
    o_ref, p_ref, raw_ref, q_ref, k_ref, v_ref,
):
    heads, rows, size = q_ref.shape
    scaling = size**-0.5

    @pl.loop(0, rows // count)
    def _(step):
        at = block_of(step, count)
        unit, _ = norm_parts(x_ref[at].astype(F32))
        normed = (unit * vec_ref[0:1] + vec_ref[1:2]).astype(BF16)
        projected = dot(normed, w_ref[...]) + bias_ref[...]
        for h in range(heads):
            query, key, value = [
                projected[:, (j * heads + h) * size : (j * heads + h + 1) * size] for j in range(3)
            ]
            raw_ref[h, at] = query
            raw_ref[heads + h, at] = key
            unit, _ = norm_parts(query)
            q_ref[h, at] = ((unit * head_ref[0:1] + head_ref[1:2]) * scaling).astype(BF16)
            unit, _ = norm_parts(key)
            k_ref[h, at] = (unit * head_ref[2:3]).astype(BF16)
            v_ref[h, at] = value.astype(BF16)

    for h in range(heads):

        @pl.loop(0, rows // count)
        def _(step):
            at = block_of(step, count)
            scores = right_cross(q_ref[h, at], k_ref[h])
            scores = jnp.where(rows_ref[at] == cols_ref[...], scores, MASKED)
            top = jnp.max(scores, axis=-1, keepdims=True)
            raised = jnp.exp(scores - top)
            total = jnp.sum(raised, axis=-1, keepdims=True)
            probs = (raised * (1.0 / total)).astype(BF16)
            p_ref[h, at] = probs
            o_ref[at, h * size : (h + 1) * size] = dot(probs, v_ref[h]).astype(BF16)


def front(count, tokens_all, w_qkv, vectors, bias, head_vectors, ids):
    rows, width = tokens_all.shape
    size = head_vectors.shape[1]
    part = w_qkv.shape[1] // 3
    heads = part // size
    return pl.pallas_call(
        functools.partial(front_body, count),
        out_shape=[
            jax.ShapeDtypeStruct((rows, part), BF16),
            jax.ShapeDtypeStruct((heads, rows, rows), BF16),
            jax.ShapeDtypeStruct((2 * heads, rows, size), F32),
            jax.ShapeDtypeStruct((heads, rows, size), BF16),
            jax.ShapeDtypeStruct((heads, rows, size), BF16),
            jax.ShapeDtypeStruct((heads, rows, size), BF16),
        ],
        cost_estimate=pl.CostEstimate(
            flops=6 * rows * width * part + 4 * heads * rows * rows * size,
            bytes_accessed=2 * rows * (width + heads * rows + 8 * part) + 6 * width * part,
            transcendentals=heads * rows * rows,
        ),
        name="front",
    )(tokens_all, w_qkv, vectors, bias, head_vectors, ids[:, None], ids[None, :])


def back_body(
    count, rank_ref, z_ref, wp_ref, p_ref, raw_ref, q_ref, k_ref, v_ref, x_ref, w_ref, vec_ref,
    head_ref, early_ref, out_ref, da_ref, sum_ref, bias_ref, heads_ref, dw_ref, g_ref, dk_ref,
    dv_ref, dq_ref, dkt_ref, dvt_ref,
):
    heads, rows, size = q_ref.shape
    scaling = size**-0.5
    steps = rows // count
    sum_ref[...] = jnp.zeros_like(sum_ref)
    bias_ref[...] = jnp.zeros_like(bias_ref)
    heads_ref[...] = jnp.zeros_like(heads_ref)
    dw_ref[...] = jnp.zeros_like(dw_ref)
    for h in range(heads):
        dk_ref[...] = jnp.zeros_like(dk_ref)
        dv_ref[...] = jnp.zeros_like(dv_ref)

        @pl.loop(0, steps)
        def _(step):
            at = block_of(step, count)
            grad = right_cross(z_ref[at], wp_ref[h * size : (h + 1) * size]).astype(BF16)
            low = p_ref[h, at]
            probs = low.astype(F32)
            grad_probs = right_cross(grad, v_ref[h])
            delta = jnp.sum(probs * grad_probs, axis=-1, keepdims=True)
            grad_scores = (probs * (grad_probs - delta)).astype(BF16)
            dq_ref[at] = dot(grad_scores, k_ref[h])
            dk_ref[...] += left_cross(q_ref[h, at], grad_scores)
            dv_ref[...] += left_cross(grad, low)

        dkt_ref[...] = dk_ref[...].T
        dvt_ref[...] = dv_ref[...].T

        @pl.loop(0, steps)
        def _(step):
            at = block_of(step, count)
            grad = dq_ref[at] * scaling
            unit, scale = norm_parts(raw_ref[h, at])
            heads_ref[0:1] += jnp.sum(grad * unit, axis=0, keepdims=True)
            heads_ref[1:2] += jnp.sum(grad, axis=0, keepdims=True)
            g_ref[at, h * size : (h + 1) * size] = norm_back(
                grad * head_ref[0:1], unit, scale
            ).astype(BF16)
            grad = dkt_ref[at]
            unit, scale = norm_parts(raw_ref[heads + h, at])
            heads_ref[2:3] += jnp.sum(grad * unit, axis=0, keepdims=True)
            first = (heads + h) * size
            g_ref[at, first : first + size] = norm_back(grad * head_ref[2:3], unit, scale).astype(
                BF16
            )
            first = (2 * heads + h) * size
            g_ref[at, first : first + size] = dvt_ref[at].astype(BF16)

    @pl.loop(0, steps)
    def _(step):
        at = block_of(step, count)
        unit, _ = norm_parts(x_ref[at].astype(F32))
        normed = (unit * vec_ref[0:1] + vec_ref[1:2]).astype(BF16)
        grad = g_ref[at]
        dw_ref[...] += left_cross(normed, grad)
        bias_ref[0:1] += jnp.sum(grad.astype(F32), axis=0, keepdims=True)
        grad_normed = right_cross(grad, w_ref[...])
        da_ref[at] = grad_normed.astype(BF16)
        sum_ref[0:1] += jnp.sum(grad_normed * unit, axis=0, keepdims=True)
        sum_ref[1:2] += jnp.sum(grad_normed, axis=0, keepdims=True)


    owners, total_rows, columns = out_ref.shape
    own = dw_ref.shape[0] // owners
    part = columns // 3
    rank = rank_ref[0]
    narrow = size // owners
    for o in range(owners):
        out_ref[o, :own] = dw_ref[o * own : (o + 1) * own]
        first = jnp.concatenate(
            [sum_ref[i : i + 1, o * own : (o + 1) * own] for i in range(2)]
            + [jnp.zeros((1, columns - 2 * own), F32)],
            axis=1,
        )
        groups = []
        for j in range(3):
            group = 3 * o + j
            value = bias_ref[0:1, group // owners * part : (group // owners + 1) * part]
            groups.append(jnp.where(rank == group % owners, value, 0.0))
        gains = [heads_ref[i : i + 1, o * narrow : (o + 1) * narrow] for i in range(3)]
        third = jnp.concatenate([*gains, jnp.zeros((1, columns - 3 * narrow), F32)], axis=1)
        out_ref[o, own:] = jnp.concatenate(
            [first, jnp.concatenate(groups, axis=1), third, early_ref[o]]
            + [jnp.zeros((total_rows - own - 3 - early_ref.shape[1], columns), F32)],
            axis=0,
        )


def back(count, extra, rank, *values):
    _, _, _, _, queries, _, _, tokens_all, _, _, _, early = values
    rows, width = tokens_all.shape
    heads, _, size = queries.shape
    part = heads * size
    owners = early.shape[0]
    vmem = pl.BlockSpec(memory_space=pltpu.VMEM)
    return pl.pallas_call(
        functools.partial(back_body, count),
        in_specs=[pl.BlockSpec(memory_space=pltpu.SMEM)] + [vmem] * len(values),
        out_specs=[vmem, vmem],
        out_shape=[
            jax.ShapeDtypeStruct((owners, width // owners + extra, 3 * part), F32),
            jax.ShapeDtypeStruct((rows, width), BF16),
        ],
        scratch_shapes=[
            pltpu.VMEM((8, width), F32),
            pltpu.VMEM((8, 3 * part), F32),
            pltpu.VMEM((8, size), F32),
            pltpu.VMEM((width, 3 * part), F32),
            pltpu.VMEM((rows, 3 * part), BF16),
            pltpu.VMEM((size, rows), F32),
            pltpu.VMEM((size, rows), F32),
            pltpu.VMEM((rows, size), F32),
            pltpu.VMEM((rows, size), F32),
            pltpu.VMEM((rows, size), F32),
        ],
        cost_estimate=pl.CostEstimate(
            flops=14 * rows * width * part + 8 * heads * rows * rows * size,
            bytes_accessed=2 * rows * (3 * width + heads * rows + 12 * part) + 18 * width * part,
            transcendentals=0,
        ),
        name="back",
    )(rank[None], *values)


def pack_body(*refs):
    out = refs[-1]
    columns = out.shape[1]
    rows = []
    for ref in refs[:-1]:
        value = ref[...].astype(F32)[None]
        size = value.shape[1]
        if size < columns:
            rows.append(jnp.concatenate([value, jnp.zeros((1, columns - size), F32)], axis=1))
        else:
            rows += [value[:, i : i + columns] for i in range(0, size, columns)]
    rows.append(jnp.zeros((out.shape[0] - len(rows), columns), F32))
    out[...] = jnp.concatenate(rows, axis=0).astype(BF16)


def pack(vectors, columns):
    return pl.pallas_call(
        pack_body, out_shape=jax.ShapeDtypeStruct((16, columns), BF16), name="pack"
    )(*vectors)


def arrange_body(share_rows, rank_ref, p0, p1, p2, p3, o_ref):
    pieces = [p[...].astype(F32) for p in (p0, p1, p2, p3)]
    part = pieces[0].shape[1] // 3
    low, high = (rank_ref[0] & 1) == 1, (rank_ref[0] & 2) == 2
    pairs = [
        (jnp.where(low, a, b), jnp.where(low, b, a))
        for a, b in ((pieces[1], pieces[0]), (pieces[3], pieces[2]))
    ]
    total = (pieces[0] + pieces[1]) + (pieces[2] + pieces[3])
    chosen = [jnp.where(high, pairs[1][i], pairs[0][i]) for i in range(2)]
    chosen += [jnp.where(high, pairs[0][i], pairs[1][i]) for i in range(2)]
    placed = jnp.concatenate(
        [c[:, j * part : (j + 1) * part] for j in range(3) for c in chosen], axis=1
    )
    wide = jnp.concatenate([total] * 4, axis=1)
    row = lax.broadcasted_iota(jnp.int32, placed.shape, 0)
    o_ref[...] = jnp.where(row < share_rows, placed, wide).astype(BF16)


def arrange(share_rows, rank, pieces):
    rows, columns = pieces[0].shape
    vmem = pl.BlockSpec(memory_space=pltpu.VMEM)
    return pl.pallas_call(
        functools.partial(arrange_body, share_rows),
        in_specs=[pl.BlockSpec(memory_space=pltpu.SMEM)] + [vmem] * 4,
        out_specs=vmem,
        out_shape=jax.ShapeDtypeStruct((rows, 4 * columns), BF16),
        name="arrange",
    )(rank[None], *pieces)


GELU_SCALE = 0.7978845608028654
GELU_CUBE = 0.044715


def middle_body(
    m0, m1, m2, m3, x_ref, g0, g1, g2, g3, w0, w1, w2, w3, wu_ref, wd_ref, vec_ref, bias_ref,
    z_ref, m_ref, dc_ref, dd_ref, du_ref, sum_ref, g_ref,
):
    step = pl.program_id(0)

    @pl.when(step == 0)
    def _():
        dd_ref[...] = jnp.zeros_like(dd_ref)
        du_ref[...] = jnp.zeros_like(du_ref)
        sum_ref[...] = jnp.zeros_like(sum_ref)

    for r, piece in enumerate((g0, g1, g2, g3)):

        @pl.when(step == r)
        def _(piece=piece):
            g_ref[...] = piece[...]

    branch = vec_ref[0:1]
    for piece, weight in zip((m0, m1, m2, m3), (w0, w1, w2, w3)):
        branch = branch + dot(piece[...], weight[...])

    @pl.when(step == 0)
    def _():
        z_ref[...] = branch

    unit, _ = norm_parts(x_ref[...].astype(F32) + branch)
    normed = (unit * vec_ref[1:2] + vec_ref[2:3]).astype(BF16)
    inner = dot(normed, wu_ref[...]) + bias_ref[...]
    square = inner * inner
    bent = jnp.tanh(GELU_SCALE * (inner + GELU_CUBE * inner * square))
    half = 0.5 * (1.0 + bent)
    active = (inner * half).astype(BF16)
    slope = half + 0.5 * inner * (1.0 - bent * bent) * (
        GELU_SCALE * (1.0 + 3.0 * GELU_CUBE * square)
    )
    grad = g_ref[...]
    m_ref[...] = dot(active, wd_ref[...]).astype(BF16)
    dd_ref[...] += left_cross(active, grad)
    grad_inner = right_cross(grad, wd_ref[...]) * slope
    grad_low = grad_inner.astype(BF16)
    du_ref[...] += left_cross(normed, grad_low)
    grad_normed = right_cross(grad_low, wu_ref[...])
    dc_ref[...] = grad_normed.astype(BF16)
    sum_ref[0:1] += jnp.sum(grad_low.astype(F32), axis=0, keepdims=True)
    sum_ref[1:2] += jnp.sum(grad_normed * unit, axis=0, keepdims=True)
    sum_ref[2:3] += jnp.sum(grad_normed, axis=0, keepdims=True)


def middle(count, pieces, tokens_all, grads, w_proj, w_up, w_down, vectors, bias):
    rows, width = tokens_all.shape
    part = pieces[0].shape[1]
    hidden = w_up.shape[1]
    steps = rows // count

    def held(shape):
        return pl.BlockSpec(shape, lambda i: (0, 0))

    def shifted(r):
        return pl.BlockSpec((count, part), lambda i: (jnp.bitwise_xor(i, r), 0))

    block = pl.BlockSpec((count, width), lambda i: (i, 0))
    return pl.pallas_call(
        middle_body,
        grid=(steps,),
        in_specs=[shifted(r) for r in range(4)]
        + [block]
        + [held(v.shape) for v in (*grads, *w_proj, w_up, w_down)]
        + [held(vectors.shape), held(bias.shape)],
        out_specs=[
            held((count, width)),
            block,
            block,
            held((hidden, width)),
            held((width, hidden)),
            held((8, width)),
        ],
        out_shape=[
            jax.ShapeDtypeStruct((count, width), F32),
            jax.ShapeDtypeStruct((rows, width), BF16),
            jax.ShapeDtypeStruct((rows, width), BF16),
            jax.ShapeDtypeStruct((hidden, width), F32),
            jax.ShapeDtypeStruct((width, hidden), F32),
            jax.ShapeDtypeStruct((8, width), F32),
        ],
        cost_estimate=pl.CostEstimate(
            flops=14 * rows * width * hidden,
            bytes_accessed=10 * rows * width + 14 * width * hidden,
            transcendentals=rows * hidden,
        ),
        scratch_shapes=[pltpu.VMEM((count, width), BF16)],
        name="middle",
    )(*pieces, tokens_all, *grads, *w_proj, w_up, w_down, vectors, bias)


def on_device(
    dp_size,
    fs_size,
    tokens,
    cotangent,
    segment_ids,
    valid_mask,
    ln1_gain,
    ln1_bias,
    qkv_weight,
    qkv_bias,
    query_gain,
    query_bias,
    key_gain,
    proj_weight,
    proj_bias,
    ln2_gain,
    ln2_bias,
    fc1_weight,
    fc1_bias,
    fc2_weight,
    fc2_bias,
):
    count, width = tokens.shape
    rank = lax.axis_index("fsdp")
    place = lax.axis_index("dp")
    near = functools.partial(swap, axis="fsdp", size=fs_size, bit=1)
    far = functools.partial(swap, axis="fsdp", size=fs_size, bit=2)
    own_heads = HEADS // fs_size
    part = own_heads * HEAD_DIM
    hidden = fc1_weight.shape[1]
    hidden_own = hidden // fs_size
    rows_own = qkv_weight.shape[0]
    rounds = [1 << i for i in range(dp_size.bit_length() - 1)]

    def gather(value):
        second = far(value)
        return [value, near(value), second, near(second)]

    def spread(pieces):
        return [pieces[0], near(pieces[1]), far(pieces[2]), swap(pieces[3], "fsdp", fs_size, 3)]

    def collect(low, mark=None, hold=None):
        low = [low[r * count : (r + 1) * count] for r in range(4)]
        other = near(jnp.concatenate([low[1], low[3]], axis=0)).astype(F32)
        first = low[0].astype(F32) + other[:count]
        sent = (low[2].astype(F32) + other[count:]).astype(BF16)
        sent = sent if mark is None else after(sent, mark)
        other = far(sent)
        other = other if hold is None else after(other, hold)
        return first + other.astype(F32), sent

    def at(r):
        return rank ^ r

    def ordered(pieces, axis):
        chosen = [lax.select_n(at(i), *[pieces[j] for j in range(4)]) for i in range(4)]
        return jnp.concatenate(chosen, axis=axis)

    small = pack(
        (ln1_gain, ln1_bias, ln2_gain, ln2_bias, proj_bias, fc2_bias, qkv_bias)
        + (query_gain, query_bias, key_gain),
        rows_own,
    )
    small_all = ordered([p[:, None] for p in gather(small)], 1).astype(F32)
    wide = small_all[:6].reshape(6, width)
    gain_one, shift_one, gain_two, shift_two, b_proj, b_down = [wide[i] for i in range(6)]
    narrow = query_gain.shape[0]
    gain_query, shift_query, gain_key = [
        small_all[i, :, :narrow].reshape(-1) for i in (9, 10, 11)
    ]
    b_qkv_all = small_all[6:9].transpose(1, 0, 2).reshape(-1)

    def own_columns(matrix, owner):
        return [
            lax.dynamic_slice_in_dim(matrix, block * width + owner * part, part, matrix.ndim - 1)
            for block in range(3)
        ]

    tokens_all = jnp.concatenate(gather(tokens), axis=0)
    w_qkv = ordered(
        spread([jnp.concatenate(own_columns(qkv_weight, at(r)), axis=1) for r in range(4)]), 0
    )

    def after(value, other):
        return lax.optimization_barrier((value, other))[0]

    w_proj_pieces = gather(after(proj_weight, w_qkv))
    up_pieces = [
        lax.dynamic_slice_in_dim(after(fc1_weight, w_qkv), at(r) * hidden_own, hidden_own, 1)
        for r in range(4)
    ]
    up_pieces[1] = near(up_pieces[1])
    up_pieces[2] = far(up_pieces[2])
    up_pieces[3] = swap(up_pieces[3], "fsdp", fs_size, 3)
    w_up = ordered(up_pieces, 0)
    weights_valid = valid_mask.astype(F32)[:, None]
    grad_mlp_own = (cotangent.astype(F32) * weights_valid).astype(BF16)
    grad_mlp_pieces = gather(after(grad_mlp_own, w_qkv))
    ids = jnp.concatenate(
        [lax.dynamic_slice_in_dim(segment_ids, at(r) * count, count) for r in range(4)]
    )

    b_qkv = jnp.concatenate(own_columns(b_qkv_all, rank))
    vectors_one = jnp.concatenate([gain_one[None], shift_one[None]])
    head_vectors = jnp.concatenate([gain_query[None], shift_query[None], gain_key[None]])
    mixed_own, probs, raw, queries, keys, values = front(
        count, tokens_all, w_qkv, vectors_one, b_qkv[None], head_vectors, ids
    )
    vectors = jnp.concatenate([b_proj[None], gain_two[None], shift_two[None]])
    mixed_pieces = gather(mixed_own)
    branch_own, mlp_part, grad_two_part, total_down, total_up, sums_middle = middle(
        count, mixed_pieces, tokens_all, grad_mlp_pieces, w_proj_pieces, w_up, fc2_weight, vectors,
        fc1_bias.astype(F32)[None],
    )
    inputs = tokens.astype(F32)
    hidden_one = inputs + branch_own

    def held_back(other, marks, order):
        return after(other, marks[order]) if order < len(marks) and marks[order] is not None else other

    def halve(total, marks=(), tail=0):
        seen, lead = [], None
        first, second = total[:, : total.shape[1] - tail], total[:, total.shape[1] - tail :]
        for order, bit in enumerate(rounds):
            size = first.shape[1] // 2
            some = second.shape[1] // 2
            low, high = first[:, :size], first[:, size:]
            if tail:
                low = jnp.concatenate([low, second[:, :some]], axis=1)
                high = jnp.concatenate([high, second[:, some:]], axis=1)
            upper = (place & bit) != 0
            sent = jnp.where(upper, low, high).astype(BF16)
            lead = sent if order == 0 else lead
            other = swap(sent, "dp", dp_size, bit)
            other = held_back(other, marks, order)
            seen.append(other)
            total = jnp.where(upper, high, low).astype(F32) + other.astype(F32)
            first, second = total[:, :size], total[:, size:]
        return total, seen, lead

    def unite(share, marks=()):
        share = share.astype(BF16)[None]
        seen = []
        for order, bit in enumerate(reversed(rounds)):
            other = swap(share, "dp", dp_size, bit)
            other = held_back(other, marks, order)
            seen.append(other)
            upper = (place & bit) != 0
            share = jnp.where(
                upper,
                jnp.concatenate([other, share], axis=0),
                jnp.concatenate([share, other], axis=0),
            )
        return share, seen

    def to_rows(share):
        share = share.astype(BF16)
        return spread([lax.dynamic_index_in_dim(share, at(r), 0, False) for r in range(4)])

    grad_normed_two, mark_two = collect(grad_two_part)
    total_down = after(total_down, mark_two)
    sums_middle = after(sums_middle, mark_two)
    grad_out = after(grad_mlp_own, mark_two).astype(F32)
    unit_two, scale_two = norm_parts(hidden_one)
    grad_hidden = grad_out + norm_back(grad_normed_two * gain_two, unit_two, scale_two)
    grad_branch_own = grad_hidden.astype(BF16)
    grad_branch_low = jnp.concatenate(gather(grad_branch_own), axis=0)
    total_proj = left_cross(mixed_own, grad_branch_low)
    own_sums = [sums_middle[1], sums_middle[2], jnp.sum(grad_branch_own.astype(F32), axis=0)]
    own_sums = jnp.stack(own_sums).reshape(3, fs_size, rows_own)
    bias_up = jnp.where(jnp.arange(fs_size)[:, None] == rank, sums_middle[0][None], 0.0)
    bias_down = jnp.sum(grad_out, axis=0).reshape(fs_size, rows_own)
    early_rows = jnp.concatenate(
        [own_sums[0], own_sums[1], own_sums[2], bias_up, bias_down], axis=1
    )
    early_rows = jnp.pad(early_rows, ((0, 0), (0, 9 * part - early_rows.shape[1])))
    early_rows = early_rows.reshape(fs_size, 3, 3 * part)
    total_last, grad_one_part = back(
        count, dp_size, rank, grad_branch_low, proj_weight, probs, raw, queries, keys, values,
        tokens_all, w_qkv, vectors_one, head_vectors, early_rows,
    )
    share_last, seen, lead = halve(total_last, tail=dp_size)
    grad_normed_one, _ = collect(after(grad_one_part, lead), hold=seen[2])
    unit_one, scale_one = norm_parts(inputs)
    tokens_grad = grad_hidden + norm_back(
        grad_normed_one * gain_one, unit_one, scale_one
    )

    count_rounds = len(rounds)
    pieces_last = to_rows(share_last)
    share_rows = rows_own // dp_size
    last, seen_back = unite(arrange(share_rows, rank, pieces_last))
    seen = [*seen, pieces_last[3], *seen_back]

    branch_mlp = collect(after(mlp_part, lead), hold=seen[2])[0] + b_down
    result = hidden_one + branch_mlp
    rms_sums = jnp.stack(
        [
            jnp.sum(weights_valid * result * result),
            jnp.sum(weights_valid * branch_own * branch_own),
            jnp.sum(weights_valid * branch_mlp * branch_mlp),
            jnp.sum(weights_valid),
        ]
    )

    rms_sums = jnp.broadcast_to(rms_sums[:, None], (4, 128))
    hops = [("fsdp", fs_size, 1), ("fsdp", fs_size, 2)] + [("dp", dp_size, bit) for bit in rounds]
    for order, (axis, size, bit) in enumerate(hops):
        other = swap(rms_sums, axis, size, bit)
        rms_sums = rms_sums + (after(other, seen[-2]) if order == 1 else other)
    sums = rms_sums[:, 0]

    early = [grad_branch_own, grad_branch_own] + [grad_branch_low] * (count_rounds - 2)
    share_down, seen_down, _ = halve(total_down[None], early)
    grad_down, _ = unite(share_down[0], [seen[0], seen[1]])
    grad_down = grad_down.astype(F32).reshape(hidden_own, width)
    total_up = after(total_up, seen_down[0])
    late = [lead, seen[0]] + [seen[1]] * (count_rounds - 2)
    share_up, _, _ = halve(total_up.reshape(fs_size, rows_own, hidden_own), late)
    pieces_up = to_rows(share_up)
    grad_up, _ = unite(ordered(pieces_up, 1), [seen[count_rounds], seen[count_rounds + 1]])
    grad_up = grad_up.astype(F32).reshape(rows_own, hidden)
    share_proj, _, _ = halve(total_proj[None], seen[:count_rounds])
    grad_proj, _ = unite(share_proj[0], seen[count_rounds:])
    grad_proj = grad_proj.astype(F32).reshape(rows_own, width)
    last = last.astype(F32)
    grad_qkv = last[:, :share_rows].reshape(rows_own, 3 * width)
    table = last[:, share_rows, : 3 * part]
    narrow = HEAD_DIM // fs_size
    flat = table[3:6].reshape(-1)
    finals = [table[0, :rows_own], table[0, rows_own : 2 * rows_own], table[1]]
    finals += [table[2, i * narrow : (i + 1) * narrow] for i in range(3)]
    finals += [flat[2 * rows_own : 3 * rows_own], flat[:rows_own], flat[rows_own : 2 * rows_own]]
    finals += [flat[3 * rows_own : 3 * rows_own + hidden_own]]
    finals += [flat[3 * rows_own + hidden_own : 4 * rows_own + hidden_own]]
    return (
        result.astype(BF16),
        tokens_grad,
        finals[0],
        finals[1],
        grad_qkv,
        finals[2],
        finals[3],
        finals[4],
        finals[5],
        grad_proj,
        finals[6],
        finals[7],
        finals[8],
        grad_up,
        finals[9],
        grad_down,
        finals[10],
        jnp.sqrt(sums[:3] / sums[3]),
    )


def solution(mesh):
    rows = P(("dp", "fsdp"), None)
    vector = P("fsdp")
    matrix = P("fsdp", None)
    device = functools.partial(on_device, mesh.shape["dp"], mesh.shape["fsdp"])

    return jax.shard_map(
        device,
        mesh=mesh,
        in_specs=(
            rows, rows, P("dp"), P(("dp", "fsdp")), vector, vector, matrix, vector, vector, vector,
            vector, matrix, vector, vector, vector, matrix, vector, matrix, vector,
        ),
        out_specs=(
            rows, rows, vector, vector, matrix, vector, vector, vector, vector, matrix, vector,
            vector, vector, matrix, vector, matrix, vector, P(),
        ),
        check_vma=False,
    )
```

```python
import functools

import jax
import jax.numpy as jnp
from jax import lax
from jax.experimental import pallas as pl
from jax.experimental.pallas import tpu as pltpu
from jax.sharding import PartitionSpec as P


HEADS = 12
HEAD_DIM = 64
EPS = 1e-06
MASKED = -1e30
F32 = jnp.float32
BF16 = jnp.bfloat16


def swap(value, axis, size, bit):
    return lax.ppermute(value, axis, [(i, i ^ bit) for i in range(size)])


def dot(first, second):
    return jnp.dot(first, second, preferred_element_type=F32)


def left_cross(first, second):
    return lax.dot_general(first, second, (((0,), (0,)), ((), ())), preferred_element_type=F32)


def right_cross(first, second):
    return lax.dot_general(first, second, (((1,), (1,)), ((), ())), preferred_element_type=F32)


def norm_parts(values):
    average = jnp.mean(values, axis=-1, keepdims=True)
    centred = values - average
    spread = jnp.mean(centred * centred, axis=-1, keepdims=True)
    scale = lax.rsqrt(spread + EPS)
    return centred * scale, scale


def norm_back(grad, unit, scale):
    return scale * (
        grad
        - jnp.mean(grad, axis=-1, keepdims=True)
        - unit * jnp.mean(grad * unit, axis=-1, keepdims=True)
    )


def block_of(step, count):
    return pl.ds(pl.multiple_of(step * count, count), count)


def front_body(
    count, x_ref, w_ref, vec_ref, bias_ref, head_ref, rows_ref, cols_ref,
    o_ref, p_ref, raw_ref, q_ref, k_ref, v_ref,
):
    heads, rows, size = q_ref.shape
    scaling = size**-0.5

    @pl.loop(0, rows // count)
    def _(step):
        at = block_of(step, count)
        unit, _ = norm_parts(x_ref[at].astype(F32))
        normed = (unit * vec_ref[0:1] + vec_ref[1:2]).astype(BF16)
        projected = dot(normed, w_ref[...]) + bias_ref[...]
        for h in range(heads):
            query, key, value = [
                projected[:, (j * heads + h) * size : (j * heads + h + 1) * size] for j in range(3)
            ]
            raw_ref[h, at] = query
            raw_ref[heads + h, at] = key
            unit, _ = norm_parts(query)
            q_ref[h, at] = ((unit * head_ref[0:1] + head_ref[1:2]) * scaling).astype(BF16)
            unit, _ = norm_parts(key)
            k_ref[h, at] = (unit * head_ref[2:3]).astype(BF16)
            v_ref[h, at] = value.astype(BF16)

    for h in range(heads):

        @pl.loop(0, rows // count)
        def _(step):
            at = block_of(step, count)
            scores = right_cross(q_ref[h, at], k_ref[h])
            scores = jnp.where(rows_ref[at] == cols_ref[...], scores, MASKED)
            top = jnp.max(scores, axis=-1, keepdims=True)
            raised = jnp.exp(scores - top)
            total = jnp.sum(raised, axis=-1, keepdims=True)
            probs = (raised * (1.0 / total)).astype(BF16)
            p_ref[h, at] = probs
            o_ref[at, h * size : (h + 1) * size] = dot(probs, v_ref[h]).astype(BF16)


def front(count, tokens_all, w_qkv, vectors, bias, head_vectors, ids):
    rows, width = tokens_all.shape
    size = head_vectors.shape[1]
    part = w_qkv.shape[1] // 3
    heads = part // size
    return pl.pallas_call(
        functools.partial(front_body, count),
        out_shape=[
            jax.ShapeDtypeStruct((rows, part), BF16),
            jax.ShapeDtypeStruct((heads, rows, rows), BF16),
            jax.ShapeDtypeStruct((2 * heads, rows, size), F32),
            jax.ShapeDtypeStruct((heads, rows, size), BF16),
            jax.ShapeDtypeStruct((heads, rows, size), BF16),
            jax.ShapeDtypeStruct((heads, rows, size), BF16),
        ],
        cost_estimate=pl.CostEstimate(
            flops=6 * rows * width * part + 4 * heads * rows * rows * size,
            bytes_accessed=2 * rows * (width + heads * rows + 8 * part) + 6 * width * part,
            transcendentals=heads * rows * rows,
        ),
        name="front",
    )(tokens_all, w_qkv, vectors, bias, head_vectors, ids[:, None], ids[None, :])


def back_body(
    count, rank_ref, z_ref, wp_ref, p_ref, raw_ref, q_ref, k_ref, v_ref, x_ref, w_ref, vec_ref,
    head_ref, early_ref, out_ref, da_ref, sum_ref, bias_ref, heads_ref, dw_ref, g_ref, dk_ref,
    dv_ref, dq_ref, dkt_ref, dvt_ref,
):
    heads, rows, size = q_ref.shape
    scaling = size**-0.5
    steps = rows // count
    sum_ref[...] = jnp.zeros_like(sum_ref)
    bias_ref[...] = jnp.zeros_like(bias_ref)
    heads_ref[...] = jnp.zeros_like(heads_ref)
    dw_ref[...] = jnp.zeros_like(dw_ref)
    for h in range(heads):
        dk_ref[...] = jnp.zeros_like(dk_ref)
        dv_ref[...] = jnp.zeros_like(dv_ref)

        @pl.loop(0, steps)
        def _(step):
            at = block_of(step, count)
            grad = right_cross(z_ref[at], wp_ref[h * size : (h + 1) * size]).astype(BF16)
            low = p_ref[h, at]
            probs = low.astype(F32)
            grad_probs = right_cross(grad, v_ref[h])
            delta = jnp.sum(probs * grad_probs, axis=-1, keepdims=True)
            grad_scores = (probs * (grad_probs - delta)).astype(BF16)
            dq_ref[at] = dot(grad_scores, k_ref[h])
            dk_ref[...] += left_cross(q_ref[h, at], grad_scores)
            dv_ref[...] += left_cross(grad, low)

        dkt_ref[...] = dk_ref[...].T
        dvt_ref[...] = dv_ref[...].T

        @pl.loop(0, steps)
        def _(step):
            at = block_of(step, count)
            grad = dq_ref[at] * scaling
            unit, scale = norm_parts(raw_ref[h, at])
            heads_ref[0:1] += jnp.sum(grad * unit, axis=0, keepdims=True)
            heads_ref[1:2] += jnp.sum(grad, axis=0, keepdims=True)
            g_ref[at, h * size : (h + 1) * size] = norm_back(
                grad * head_ref[0:1], unit, scale
            ).astype(BF16)
            grad = dkt_ref[at]
            unit, scale = norm_parts(raw_ref[heads + h, at])
            heads_ref[2:3] += jnp.sum(grad * unit, axis=0, keepdims=True)
            first = (heads + h) * size
            g_ref[at, first : first + size] = norm_back(grad * head_ref[2:3], unit, scale).astype(
                BF16
            )
            first = (2 * heads + h) * size
            g_ref[at, first : first + size] = dvt_ref[at].astype(BF16)

    @pl.loop(0, steps)
    def _(step):
        at = block_of(step, count)
        unit, _ = norm_parts(x_ref[at].astype(F32))
        normed = (unit * vec_ref[0:1] + vec_ref[1:2]).astype(BF16)
        grad = g_ref[at]
        dw_ref[...] += left_cross(normed, grad)
        bias_ref[0:1] += jnp.sum(grad.astype(F32), axis=0, keepdims=True)
        grad_normed = right_cross(grad, w_ref[...])
        da_ref[at] = grad_normed.astype(BF16)
        sum_ref[0:1] += jnp.sum(grad_normed * unit, axis=0, keepdims=True)
        sum_ref[1:2] += jnp.sum(grad_normed, axis=0, keepdims=True)


    owners, total_rows, columns = out_ref.shape
    own = dw_ref.shape[0] // owners
    part = columns // 3
    rank = rank_ref[0]
    narrow = size // owners
    for o in range(owners):
        out_ref[o, :own] = dw_ref[o * own : (o + 1) * own]
        first = jnp.concatenate(
            [sum_ref[i : i + 1, o * own : (o + 1) * own] for i in range(2)]
            + [jnp.zeros((1, columns - 2 * own), F32)],
            axis=1,
        )
        groups = []
        for j in range(3):
            group = 3 * o + j
            value = bias_ref[0:1, group // owners * part : (group // owners + 1) * part]
            groups.append(jnp.where(rank == group % owners, value, 0.0))
        gains = [heads_ref[i : i + 1, o * narrow : (o + 1) * narrow] for i in range(3)]
        third = jnp.concatenate([*gains, jnp.zeros((1, columns - 3 * narrow), F32)], axis=1)
        out_ref[o, own:] = jnp.concatenate(
            [first, jnp.concatenate(groups, axis=1), third, early_ref[o]]
            + [jnp.zeros((total_rows - own - 3 - early_ref.shape[1], columns), F32)],
            axis=0,
        )


def back(count, extra, rank, *values):
    _, _, _, _, queries, _, _, tokens_all, _, _, _, early = values
    rows, width = tokens_all.shape
    heads, _, size = queries.shape
    part = heads * size
    owners = early.shape[0]
    vmem = pl.BlockSpec(memory_space=pltpu.VMEM)
    return pl.pallas_call(
        functools.partial(back_body, count),
        in_specs=[pl.BlockSpec(memory_space=pltpu.SMEM)] + [vmem] * len(values),
        out_specs=[vmem, vmem],
        out_shape=[
            jax.ShapeDtypeStruct((owners, width // owners + extra, 3 * part), F32),
            jax.ShapeDtypeStruct((rows, width), BF16),
        ],
        scratch_shapes=[
            pltpu.VMEM((8, width), F32),
            pltpu.VMEM((8, 3 * part), F32),
            pltpu.VMEM((8, size), F32),
            pltpu.VMEM((width, 3 * part), F32),
            pltpu.VMEM((rows, 3 * part), BF16),
            pltpu.VMEM((size, rows), F32),
            pltpu.VMEM((size, rows), F32),
            pltpu.VMEM((rows, size), F32),
            pltpu.VMEM((rows, size), F32),
            pltpu.VMEM((rows, size), F32),
        ],
        cost_estimate=pl.CostEstimate(
            flops=14 * rows * width * part + 8 * heads * rows * rows * size,
            bytes_accessed=2 * rows * (3 * width + heads * rows + 12 * part) + 18 * width * part,
            transcendentals=0,
        ),
        name="back",
    )(rank[None], *values)


def pack_body(*refs):
    out = refs[-1]
    columns = out.shape[1]
    rows = []
    for ref in refs[:-1]:
        value = ref[...].astype(F32)[None]
        size = value.shape[1]
        if size < columns:
            rows.append(jnp.concatenate([value, jnp.zeros((1, columns - size), F32)], axis=1))
        else:
            rows += [value[:, i : i + columns] for i in range(0, size, columns)]
    rows.append(jnp.zeros((out.shape[0] - len(rows), columns), F32))
    out[...] = jnp.concatenate(rows, axis=0).astype(BF16)


def pack(vectors, columns):
    return pl.pallas_call(
        pack_body, out_shape=jax.ShapeDtypeStruct((16, columns), BF16), name="pack"
    )(*vectors)


def arrange_body(share_rows, rank_ref, p0, p1, p2, p3, o_ref):
    pieces = [p[...].astype(F32) for p in (p0, p1, p2, p3)]
    part = pieces[0].shape[1] // 3
    low, high = (rank_ref[0] & 1) == 1, (rank_ref[0] & 2) == 2
    pairs = [
        (jnp.where(low, a, b), jnp.where(low, b, a))
        for a, b in ((pieces[1], pieces[0]), (pieces[3], pieces[2]))
    ]
    total = (pieces[0] + pieces[1]) + (pieces[2] + pieces[3])
    chosen = [jnp.where(high, pairs[1][i], pairs[0][i]) for i in range(2)]
    chosen += [jnp.where(high, pairs[0][i], pairs[1][i]) for i in range(2)]
    placed = jnp.concatenate(
        [c[:, j * part : (j + 1) * part] for j in range(3) for c in chosen], axis=1
    )
    wide = jnp.concatenate([total] * 4, axis=1)
    row = lax.broadcasted_iota(jnp.int32, placed.shape, 0)
    o_ref[...] = jnp.where(row < share_rows, placed, wide).astype(BF16)


def arrange(share_rows, rank, pieces):
    rows, columns = pieces[0].shape
    vmem = pl.BlockSpec(memory_space=pltpu.VMEM)
    return pl.pallas_call(
        functools.partial(arrange_body, share_rows),
        in_specs=[pl.BlockSpec(memory_space=pltpu.SMEM)] + [vmem] * 4,
        out_specs=vmem,
        out_shape=jax.ShapeDtypeStruct((rows, 4 * columns), BF16),
        name="arrange",
    )(rank[None], *pieces)


GELU_SCALE = 0.7978845608028654
GELU_CUBE = 0.044715


def middle_body(
    m0, m1, m2, m3, x_ref, g0, g1, g2, g3, w0, w1, w2, w3, wu_ref, wd_ref, vec_ref, bias_ref,
    z_ref, m_ref, dc_ref, dd_ref, du_ref, sum_ref, g_ref,
):
    step = pl.program_id(0)

    @pl.when(step == 0)
    def _():
        dd_ref[...] = jnp.zeros_like(dd_ref)
        du_ref[...] = jnp.zeros_like(du_ref)
        sum_ref[...] = jnp.zeros_like(sum_ref)

    for r, piece in enumerate((g0, g1, g2, g3)):

        @pl.when(step == r)
        def _(piece=piece):
            g_ref[...] = piece[...]

    branch = vec_ref[0:1]
    for piece, weight in zip((m0, m1, m2, m3), (w0, w1, w2, w3)):
        branch = branch + dot(piece[...], weight[...])

    @pl.when(step == 0)
    def _():
        z_ref[...] = branch

    unit, _ = norm_parts(x_ref[...].astype(F32) + branch)
    normed = (unit * vec_ref[1:2] + vec_ref[2:3]).astype(BF16)
    inner = dot(normed, wu_ref[...]) + bias_ref[...]
    square = inner * inner
    bent = jnp.tanh(GELU_SCALE * (inner + GELU_CUBE * inner * square))
    half = 0.5 * (1.0 + bent)
    active = (inner * half).astype(BF16)
    slope = half + 0.5 * inner * (1.0 - bent * bent) * (
        GELU_SCALE * (1.0 + 3.0 * GELU_CUBE * square)
    )
    grad = g_ref[...]
    m_ref[...] = dot(active, wd_ref[...]).astype(BF16)
    dd_ref[...] += left_cross(active, grad)
    grad_inner = right_cross(grad, wd_ref[...]) * slope
    grad_low = grad_inner.astype(BF16)
    du_ref[...] += left_cross(normed, grad_low)
    grad_normed = right_cross(grad_low, wu_ref[...])
    dc_ref[...] = grad_normed.astype(BF16)
    sum_ref[0:1] += jnp.sum(grad_low.astype(F32), axis=0, keepdims=True)
    sum_ref[1:2] += jnp.sum(grad_normed * unit, axis=0, keepdims=True)
    sum_ref[2:3] += jnp.sum(grad_normed, axis=0, keepdims=True)


def middle(count, pieces, tokens_all, grads, w_proj, w_up, w_down, vectors, bias):
    rows, width = tokens_all.shape
    part = pieces[0].shape[1]
    hidden = w_up.shape[1]
    steps = rows // count

    def held(shape):
        return pl.BlockSpec(shape, lambda i: (0, 0))

    def shifted(r):
        return pl.BlockSpec((count, part), lambda i: (jnp.bitwise_xor(i, r), 0))

    block = pl.BlockSpec((count, width), lambda i: (i, 0))
    return pl.pallas_call(
        middle_body,
        grid=(steps,),
        in_specs=[shifted(r) for r in range(4)]
        + [block]
        + [held(v.shape) for v in (*grads, *w_proj, w_up, w_down)]
        + [held(vectors.shape), held(bias.shape)],
        out_specs=[
            held((count, width)),
            block,
            block,
            held((hidden, width)),
            held((width, hidden)),
            held((8, width)),
        ],
        out_shape=[
            jax.ShapeDtypeStruct((count, width), F32),
            jax.ShapeDtypeStruct((rows, width), BF16),
            jax.ShapeDtypeStruct((rows, width), BF16),
            jax.ShapeDtypeStruct((hidden, width), F32),
            jax.ShapeDtypeStruct((width, hidden), F32),
            jax.ShapeDtypeStruct((8, width), F32),
        ],
        cost_estimate=pl.CostEstimate(
            flops=14 * rows * width * hidden,
            bytes_accessed=10 * rows * width + 14 * width * hidden,
            transcendentals=rows * hidden,
        ),
        scratch_shapes=[pltpu.VMEM((count, width), BF16)],
        name="middle",
    )(*pieces, tokens_all, *grads, *w_proj, w_up, w_down, vectors, bias)


def on_device(
    dp_size,
    fs_size,
    tokens,
    cotangent,
    segment_ids,
    valid_mask,
    ln1_gain,
    ln1_bias,
    qkv_weight,
    qkv_bias,
    query_gain,
    query_bias,
    key_gain,
    proj_weight,
    proj_bias,
    ln2_gain,
    ln2_bias,
    fc1_weight,
    fc1_bias,
    fc2_weight,
    fc2_bias,
):
    count, width = tokens.shape
    rank = lax.axis_index("fsdp")
    place = lax.axis_index("dp")
    near = functools.partial(swap, axis="fsdp", size=fs_size, bit=1)
    far = functools.partial(swap, axis="fsdp", size=fs_size, bit=2)
    own_heads = HEADS // fs_size
    part = own_heads * HEAD_DIM
    hidden = fc1_weight.shape[1]
    hidden_own = hidden // fs_size
    rows_own = qkv_weight.shape[0]
    rounds = [1 << i for i in range(dp_size.bit_length() - 1)]

    def gather(value):
        second = far(value)
        return [value, near(value), second, near(second)]

    def spread(pieces):
        return [pieces[0], near(pieces[1]), far(pieces[2]), swap(pieces[3], "fsdp", fs_size, 3)]

    def collect(low, mark=None):
        low = [low[r * count : (r + 1) * count] for r in range(4)]
        other = near(jnp.concatenate([low[1], low[3]], axis=0)).astype(F32)
        first = low[0].astype(F32) + other[:count]
        sent = (low[2].astype(F32) + other[count:]).astype(BF16)
        sent = sent if mark is None else after(sent, mark)
        other = far(sent)
        return first + other.astype(F32), sent

    def at(r):
        return rank ^ r

    def ordered(pieces, axis):
        chosen = [lax.select_n(at(i), *[pieces[j] for j in range(4)]) for i in range(4)]
        return jnp.concatenate(chosen, axis=axis)

    small = pack(
        (ln1_gain, ln1_bias, ln2_gain, ln2_bias, proj_bias, fc2_bias, qkv_bias)
        + (query_gain, query_bias, key_gain),
        rows_own,
    )
    small_all = ordered([p[:, None] for p in gather(small)], 1).astype(F32)
    wide = small_all[:6].reshape(6, width)
    gain_one, shift_one, gain_two, shift_two, b_proj, b_down = [wide[i] for i in range(6)]
    narrow = query_gain.shape[0]
    gain_query, shift_query, gain_key = [
        small_all[i, :, :narrow].reshape(-1) for i in (9, 10, 11)
    ]
    b_qkv_all = small_all[6:9].transpose(1, 0, 2).reshape(-1)

    def own_columns(matrix, owner):
        return [
            lax.dynamic_slice_in_dim(matrix, block * width + owner * part, part, matrix.ndim - 1)
            for block in range(3)
        ]

    tokens_all = jnp.concatenate(gather(tokens), axis=0)
    w_qkv = ordered(
        spread([jnp.concatenate(own_columns(qkv_weight, at(r)), axis=1) for r in range(4)]), 0
    )

    def after(value, other):
        return lax.optimization_barrier((value, other))[0]

    w_proj_pieces = gather(after(proj_weight, w_qkv))
    up_pieces = [
        lax.dynamic_slice_in_dim(after(fc1_weight, w_qkv), at(r) * hidden_own, hidden_own, 1)
        for r in range(4)
    ]
    up_pieces[1] = near(up_pieces[1])
    up_pieces[2] = far(up_pieces[2])
    up_pieces[3] = swap(up_pieces[3], "fsdp", fs_size, 3)
    w_up = ordered(up_pieces, 0)
    weights_valid = valid_mask.astype(F32)[:, None]
    grad_mlp_own = (cotangent.astype(F32) * weights_valid).astype(BF16)
    grad_mlp_pieces = gather(after(grad_mlp_own, w_qkv))
    ids = jnp.concatenate(
        [lax.dynamic_slice_in_dim(segment_ids, at(r) * count, count) for r in range(4)]
    )

    b_qkv = jnp.concatenate(own_columns(b_qkv_all, rank))
    vectors_one = jnp.concatenate([gain_one[None], shift_one[None]])
    head_vectors = jnp.concatenate([gain_query[None], shift_query[None], gain_key[None]])
    mixed_own, probs, raw, queries, keys, values = front(
        count, tokens_all, w_qkv, vectors_one, b_qkv[None], head_vectors, ids
    )
    vectors = jnp.concatenate([b_proj[None], gain_two[None], shift_two[None]])
    mixed_pieces = gather(mixed_own)
    branch_own, mlp_part, grad_two_part, total_down, total_up, sums_middle = middle(
        count, mixed_pieces, tokens_all, grad_mlp_pieces, w_proj_pieces, w_up, fc2_weight, vectors,
        fc1_bias.astype(F32)[None],
    )
    inputs = tokens.astype(F32)
    hidden_one = inputs + branch_own

    def held_back(other, marks, order):
        return after(other, marks[order]) if order < len(marks) and marks[order] is not None else other

    def halve(total, marks=(), tail=0):
        seen, lead = [], None
        first, second = total[:, : total.shape[1] - tail], total[:, total.shape[1] - tail :]
        for order, bit in enumerate(rounds):
            size = first.shape[1] // 2
            some = second.shape[1] // 2
            low, high = first[:, :size], first[:, size:]
            if tail:
                low = jnp.concatenate([low, second[:, :some]], axis=1)
                high = jnp.concatenate([high, second[:, some:]], axis=1)
            upper = (place & bit) != 0
            sent = jnp.where(upper, low, high).astype(BF16)
            lead = sent if order == 0 else lead
            other = swap(sent, "dp", dp_size, bit)
            other = held_back(other, marks, order)
            seen.append(other)
            total = jnp.where(upper, high, low).astype(F32) + other.astype(F32)
            first, second = total[:, :size], total[:, size:]
        return total, seen, lead

    def unite(share, marks=()):
        share = share.astype(BF16)[None]
        seen = []
        for order, bit in enumerate(reversed(rounds)):
            other = swap(share, "dp", dp_size, bit)
            other = held_back(other, marks, order)
            seen.append(other)
            upper = (place & bit) != 0
            share = jnp.where(
                upper,
                jnp.concatenate([other, share], axis=0),
                jnp.concatenate([share, other], axis=0),
            )
        return share, seen

    def to_rows(share):
        share = share.astype(BF16)
        return spread([lax.dynamic_index_in_dim(share, at(r), 0, False) for r in range(4)])

    grad_normed_two, mark_two = collect(grad_two_part)
    total_down = after(total_down, mark_two)
    sums_middle = after(sums_middle, mark_two)
    mlp_part = after(mlp_part, mark_two)
    grad_out = after(grad_mlp_own, mark_two).astype(F32)
    unit_two, scale_two = norm_parts(hidden_one)
    grad_hidden = grad_out + norm_back(grad_normed_two * gain_two, unit_two, scale_two)
    grad_branch_own = grad_hidden.astype(BF16)
    grad_branch_low = jnp.concatenate(gather(grad_branch_own), axis=0)
    total_proj = left_cross(mixed_own, grad_branch_low)
    branch_mlp = collect(mlp_part, grad_branch_own)[0] + b_down
    result = hidden_one + branch_mlp
    rms_sums = jnp.stack(
        [
            jnp.sum(weights_valid * result * result),
            jnp.sum(weights_valid * branch_own * branch_own),
            jnp.sum(weights_valid * branch_mlp * branch_mlp),
            jnp.sum(weights_valid),
        ]
    )

    own_sums = [sums_middle[1], sums_middle[2], jnp.sum(grad_branch_own.astype(F32), axis=0)]
    own_sums = jnp.stack(own_sums).reshape(3, fs_size, rows_own)
    bias_up = jnp.where(jnp.arange(fs_size)[:, None] == rank, sums_middle[0][None], 0.0)
    bias_down = jnp.sum(grad_out, axis=0).reshape(fs_size, rows_own)
    early_rows = jnp.concatenate(
        [own_sums[0], own_sums[1], own_sums[2], bias_up, bias_down]
        + [jnp.broadcast_to(rms_sums[None], (fs_size, 4))],
        axis=1,
    )
    early_rows = jnp.pad(early_rows, ((0, 0), (0, 9 * part - early_rows.shape[1])))
    early_rows = early_rows.reshape(fs_size, 3, 3 * part)
    total_last, grad_one_part = back(
        count, dp_size, rank, grad_branch_low, proj_weight, probs, raw, queries, keys, values,
        tokens_all, w_qkv, vectors_one, head_vectors, early_rows,
    )
    share_last, seen, lead = halve(total_last, tail=dp_size)
    grad_normed_one, _ = collect(after(grad_one_part, lead))
    unit_one, scale_one = norm_parts(inputs)
    tokens_grad = grad_hidden + norm_back(
        grad_normed_one * gain_one, unit_one, scale_one
    )

    count_rounds = len(rounds)
    pieces_last = to_rows(share_last)
    share_rows = rows_own // dp_size
    last, seen_back = unite(arrange(share_rows, rank, pieces_last))
    seen = [*seen, pieces_last[3], *seen_back]

    early = [grad_branch_own, grad_branch_own] + [grad_branch_low] * (count_rounds - 2)
    share_down, seen_down, _ = halve(total_down[None], early)
    grad_down, _ = unite(share_down[0], [lead, seen[0], seen[1]])
    grad_down = grad_down.astype(F32).reshape(hidden_own, width)
    total_up = after(total_up, seen_down[0])
    late = [grad_branch_own] + [lead] * (count_rounds - 1)
    share_up, _, _ = halve(total_up.reshape(fs_size, rows_own, hidden_own), late)
    grad_up, _ = unite(ordered(to_rows(share_up), 1), [seen[1], seen[2], seen[count_rounds]])
    grad_up = grad_up.astype(F32).reshape(rows_own, hidden)
    share_proj, _, _ = halve(total_proj[None], seen[:count_rounds])
    grad_proj, _ = unite(share_proj[0], seen[count_rounds:])
    grad_proj = grad_proj.astype(F32).reshape(rows_own, width)
    last = last.astype(F32)
    grad_qkv = last[:, :share_rows].reshape(rows_own, 3 * width)
    table = last[:, share_rows, : 3 * part]
    narrow = HEAD_DIM // fs_size
    flat = table[3:6].reshape(-1)
    finals = [table[0, :rows_own], table[0, rows_own : 2 * rows_own], table[1]]
    finals += [table[2, i * narrow : (i + 1) * narrow] for i in range(3)]
    finals += [flat[2 * rows_own : 3 * rows_own], flat[:rows_own], flat[rows_own : 2 * rows_own]]
    finals += [flat[3 * rows_own : 3 * rows_own + hidden_own]]
    finals += [flat[3 * rows_own + hidden_own : 4 * rows_own + hidden_own]]
    sums = flat[4 * rows_own + hidden_own :]
    return (
        result.astype(BF16),
        tokens_grad,
        finals[0],
        finals[1],
        grad_qkv,
        finals[2],
        finals[3],
        finals[4],
        finals[5],
        grad_proj,
        finals[6],
        finals[7],
        finals[8],
        grad_up,
        finals[9],
        grad_down,
        finals[10],
        jnp.sqrt(sums[:3] / sums[3]),
    )


def solution(mesh):
    rows = P(("dp", "fsdp"), None)
    vector = P("fsdp")
    matrix = P("fsdp", None)
    device = functools.partial(on_device, mesh.shape["dp"], mesh.shape["fsdp"])

    return jax.shard_map(
        device,
        mesh=mesh,
        in_specs=(
            rows, rows, P("dp"), P(("dp", "fsdp")), vector, vector, matrix, vector, vector, vector,
            vector, matrix, vector, vector, vector, matrix, vector, matrix, vector,
        ),
        out_specs=(
            rows, rows, vector, vector, matrix, vector, vector, vector, vector, matrix, vector,
            vector, vector, matrix, vector, matrix, vector, P(),
        ),
        check_vma=False,
    )
```
